256 devices in a mesh: seq: 8 (over z), chan: 32 (over y, x, core).
Axes of the slice: x: 4, y: 4, z: 8, core: 2. Of those that a mesh axis runs over, the one named last changes fastest.
Arguments:
- tokens: bfloat16 [8192, 4096], P('seq', 'chan'), may hold values from -8 to 8
- norm_gain: float32 [4096], replicated, may hold values from 0.5 to 1.5
- gate_proj: bfloat16 [4096, 8192], P(None, 'chan'), may hold values from -0.09375 to 0.09375
- inner_proj: bfloat16 [4096, 8192], P(None, 'chan'), may hold values from -0.09375 to 0.09375
- state_proj: bfloat16 [4096, 384], P('chan'), may hold values from -0.11816406 to 0.11816406
- conv_inner: float32 [4, 8192], P(None, 'chan'), may hold values from -3 to 3
- conv_state: float32 [4, 256], replicated, may hold values from -3 to 3
- log_rate: float32 [128], P('chan'), may hold values from -1 to 0
- rate_bias: float32 [128], P('chan'), may hold values from -16 to -2
- skip_gain: float32 [128], P('chan'), may hold values from 0.2 to 4
- gate_gain: float32 [8192], P('chan'), may hold values from 0.5 to 1.5
- out_proj: bfloat16 [8192, 4096], P('chan'), may hold values from -0.125 to 0.125
Outputs:
- layer_out: bfloat16 [8192, 4096], P('seq', 'chan')
The draws below stay inside these ranges and needn't reach their ends.
All inputs are finite; a program needn't handle non-finite values.
Results may differ from the reference program's by a relative error of at most 0.012.
Values may be sent and summed in bfloat16 or wider, within the bound.
No kernel may reach another device: no remote copies, remote signals or barrier semaphores. Data moves between devices by JAX's collectives and lax.ppermute only.
A program may use at most 128 MiB of HBM per device.

```python
import jax
import jax.numpy as jnp
from jax import lax

D = 4096
H = 128
P_SIZE = 64
N = 128
K = 4
Q = 256
DI = 8192
TOKENS = 8192


def layout_plan(key):
    base_key = jax.random.fold_in(key, 4211)
    direction = jnp.clip(jax.random.normal(jax.random.fold_in(base_key, 1), (D,), jnp.float32), -6.0, 6.0)
    spot_count = max(4, TOKENS // 512)
    spot_rows = jax.random.randint(jax.random.fold_in(base_key, 2), (spot_count,), 0, TOKENS)
    spot_power = jax.random.uniform(jax.random.fold_in(base_key, 5), (spot_count,), jnp.float32, 0.8, 1.0)
    mixing = jax.random.uniform(jax.random.fold_in(base_key, 3), (H,), jnp.float32)
    memory = 30.0 * jnp.exp(mixing * jnp.log(jnp.float32(2 * TOKENS)))
    rate_logs = jax.random.uniform(jax.random.fold_in(base_key, 4), (H,), jnp.float32, -1.0, 0.0)
    offset = -jnp.log(1.65 * jnp.exp(rate_logs) * memory)
    return (direction, spot_rows, spot_power, rate_logs, offset)


def draw_tokens(key, part):
    direction, spot_rows, spot_power, rate_logs, offset = layout_plan(key)
    grid_key = jax.random.fold_in(key, 11)
    noise_draw = jnp.clip(jax.random.normal(grid_key, (TOKENS, D), jnp.float32), -6.0, 6.0)
    hits = jnp.arange(TOKENS)[:, None] == spot_rows[None, :]
    marked = jnp.any(hits, axis=1)
    power = jnp.max(jnp.where(hits, spot_power[None, :], 0.0), axis=1)
    result = jnp.where(marked[:, None], power[:, None] * direction[None, :] + 0.3 * noise_draw, noise_draw)
    return result.astype(jnp.bfloat16)


def draw_state_proj(key, part):
    direction, spot_rows, spot_power, rate_logs, offset = layout_plan(key)
    noise_draw = jnp.clip(jax.random.normal(jax.random.fold_in(key, 12), (D, 2 * N + H), jnp.float32), -6.0, 6.0)
    noise_draw = noise_draw / jnp.sqrt(jnp.float32(D))
    push_cols = jnp.concatenate([jnp.zeros((2 * N,), jnp.float32), -offset])
    return (noise_draw + direction[:, None] * push_cols[None, :] / D).astype(jnp.bfloat16)


def draw_log_rate(key, part):
    direction, spot_rows, spot_power, rate_logs, offset = layout_plan(key)
    return rate_logs


def draw_rate_bias(key, part):
    direction, spot_rows, spot_power, rate_logs, offset = layout_plan(key)
    return offset


def draw_skip_gain(key, part):
    base_key = jax.random.fold_in(key, 13)
    height = jnp.arange(H, dtype=jnp.float32) / H
    spread = jnp.exp(jax.random.uniform(base_key, (H,), jnp.float32, -0.35, 0.35))
    return (0.5 + 2.0 * height) * spread


def spiked(values, own_key, source, target, shards_of, factor):
    owner, partner = [(jnp.arange(values.shape[position]) // (values.shape[position] // shards_of)).reshape([-1 if axis == position else 1 for axis in range(values.ndim)]) for position in (source, target)]
    chosen = jax.random.permutation(own_key, shards_of)[partner]
    strong = (owner == chosen) | (owner == (partner + shards_of // 2) % shards_of)
    return jnp.where(strong, factor * values, values)


def block_scale(key, dims, cuts, least, largest):
    def one(position, parts):
        heights = jax.random.uniform(jax.random.fold_in(jax.random.fold_in(key, 6), position), (parts,), jnp.float32, least / len(cuts), largest / len(cuts))
        return jnp.repeat(jnp.exp(heights), dims[position] // parts).reshape((-1,) + (1,) * (len(dims) - position - 1))

    factor_of = one(*cuts[0])
    for cut in cuts[1:]:
        factor_of = factor_of * one(*cut)
    return factor_of


def normal_values(key, shape, scale, limit, shards=(), kind=jnp.bfloat16):
    factor_of = block_scale(key, shape, shards, -0.22, 0.18) if shards else 1.0
    values = jax.random.normal(key, shape, jnp.float32) * scale * factor_of
    return jnp.minimum(jnp.maximum(values, -limit), limit).astype(kind)


def noise_with(own_key, dims, scale, bound, cuts, heavy, held_as=jnp.bfloat16):
    values = scale * jax.random.normal(own_key, dims, jnp.float32)
    if cuts:
        values = values * block_scale(own_key, dims, cuts, -0.22, 0.18)
    return jnp.clip(spiked(values, jax.random.fold_in(own_key, 3), *heavy), -bound, bound).astype(held_as)


def setup_inputs(seed: int = 0) -> dict:
    key_list = jax.random.split(jax.random.key(seed), 13)
    return {
        "tokens": draw_tokens(jax.random.fold_in(key_list[12], 71), 0),
        "norm_gain": jnp.clip(1.0 + 0.1 * jax.random.normal(key_list[1], (D,), jnp.float32), 0.5, 1.5),
        "gate_proj": normal_values(key_list[2], (D, DI), D ** -0.5, 0.09375, ((1, 32),)),
        "inner_proj": normal_values(key_list[3], (D, DI), D ** -0.5, 0.09375, ((1, 32),)),
        "state_proj": draw_state_proj(jax.random.fold_in(key_list[12], 71), 0),
        "conv_inner": normal_values(key_list[5], (K, DI), K ** -0.5, 3.0, ((1, 32),), jnp.float32),
        "conv_state": normal_values(key_list[6], (K, 2 * N), K ** -0.5, 3.0, (), jnp.float32),
        "log_rate": draw_log_rate(jax.random.fold_in(key_list[12], 71), 0),
        "rate_bias": draw_rate_bias(jax.random.fold_in(key_list[12], 71), 0),
        "skip_gain": draw_skip_gain(jax.random.fold_in(key_list[12], 71), 0),
        "gate_gain": jnp.clip(1.0 + 0.1 * jax.random.normal(key_list[10], (DI,), jnp.float32), 0.5, 1.5),
        "out_proj": noise_with(key_list[11], (DI, D), DI ** -0.5, 0.125, ((0, 32),), (0, 1, 32, 2.75)),
    }


precise = lax.Precision.HIGHEST

def causal_mix(fresh_rows, weights):
    length = fresh_rows.shape[0]
    padded = jnp.concatenate([jnp.zeros((K - 1, fresh_rows.shape[1]), fresh_rows.dtype), fresh_rows], axis=0)
    summed = jnp.zeros(fresh_rows.shape, jnp.float32)
    for offset in range(K):
        summed = summed + weights[offset] * padded[offset:offset + length].astype(jnp.float32)
    return jax.nn.silu(summed)

def block_step(state, pieces):
    values, in_map, out_map, step_size, decay_log = pieces
    within = jnp.cumsum(decay_log, axis=0)
    log_gaps = within[:, None, :] - within[None, :, :]
    lower_mask = jnp.arange(Q)[:, None] >= jnp.arange(Q)[None, :]
    fading = jnp.exp(jnp.where(lower_mask[:, :, None], log_gaps, -jnp.inf))
    scores = jnp.dot(out_map, in_map.T, precision=precise)
    mixing = scores[:, :, None] * fading * step_size[None, :, :]
    inside = jnp.einsum('tsh,shp->thp', mixing, values, precision=precise)
    carried = jnp.einsum('tn,hnp->thp', out_map, state, precision=precise) * jnp.exp(within)[:, :, None]
    tail_weight = jnp.exp(within[-1:] - within) * step_size
    fresh_state = jnp.einsum('sn,shp->hnp', in_map, values * tail_weight[:, :, None], precision=precise)
    state = jnp.exp(within[-1])[:, None, None] * state + fresh_state
    return (state, inside + carried)

def reference(tokens, norm_gain, gate_proj, inner_proj, state_proj, conv_inner, conv_state, log_rate, rate_bias, skip_gain, gate_gain, out_proj):
    widened = tokens.astype(jnp.float32)
    inverse = lax.rsqrt(lax.optimization_barrier(jnp.mean(widened * widened, axis=1, keepdims=True)) + 1e-05)
    normed = (widened * inverse * norm_gain).astype(jnp.bfloat16)
    gate_raw = jnp.dot(normed, gate_proj, preferred_element_type=jnp.float32).astype(jnp.bfloat16)
    inner_raw = jnp.dot(normed, inner_proj, preferred_element_type=jnp.float32).astype(jnp.bfloat16)
    projected = jnp.dot(normed, state_proj, preferred_element_type=jnp.float32)
    state_raw = projected[:, :2 * N]
    raw_rate = projected[:, 2 * N:]
    inner_conv = causal_mix(inner_raw, conv_inner)
    state_conv = causal_mix(state_raw, conv_state)
    step_size = jax.nn.softplus(raw_rate + rate_bias)
    decay_log = -jnp.exp(log_rate) * step_size
    blocks = TOKENS // Q
    pieces = (inner_conv.reshape(blocks, Q, H, P_SIZE), state_conv[:, :N].reshape(blocks, Q, N), state_conv[:, N:].reshape(blocks, Q, N), step_size.reshape(blocks, Q, H), decay_log.reshape(blocks, Q, H))
    start_state = jnp.zeros((H, N, P_SIZE), jnp.float32)
    final_state, ssd_parts = lax.scan(block_step, start_state, pieces)
    skip_wide = jnp.repeat(skip_gain, P_SIZE)
    ssd_out = ssd_parts.reshape(TOKENS, DI) + skip_wide * inner_conv
    gated_out = ssd_out * jax.nn.silu(gate_raw.astype(jnp.float32))
    norm_scale = lax.rsqrt(lax.optimization_barrier(jnp.mean(gated_out * gated_out, axis=1, keepdims=True)) + 1e-05)
    shaped = (gated_out * norm_scale * gate_gain).astype(jnp.bfloat16)
    added = jnp.dot(shaped, out_proj, preferred_element_type=jnp.float32)
    return (widened + added).astype(jnp.bfloat16)
```

```python
import jax
import jax.numpy as jnp
from jax import lax
from jax.experimental import pallas as pl
from jax.experimental.pallas import tpu as pltpu
from jax.sharding import PartitionSpec as P

D = 4096
DI = 8192
N = 128
P_SIZE = 64
K = 4
Q = 256
ROWS = 1024
HALF = 512
CHUNKS = 4
HEADS = 4
CH = 256
EPS = 1e-05
F32 = jnp.float32
BF16 = jnp.bfloat16
HIGH = lax.Precision.HIGHEST


def plane_move(value, dy, dx, dc=0):
    pairs = []
    for y in range(4):
        for x in range(4):
            for c in range(2):
                pairs.append(((y * 4 + x) * 2 + c, ((y + dy) % 4 * 4 + (x + dx) % 4) * 2 + (c ^ dc)))
    return lax.ppermute(value, "chan", pairs)


def swap(value):
    return plane_move(value, 0, 0, 1)


def later(value, steps):
    return lax.ppermute(value, "seq", [(i, i + steps) for i in range(8 - steps)])


def kernel(body, outs, name, n_in, smem=0, scratch=(), flops=0):
    return pl.pallas_call(
        body,
        out_shape=outs,
        in_specs=[pl.BlockSpec(memory_space=pltpu.SMEM)] * smem + [pl.BlockSpec(memory_space=pltpu.VMEM)] * (n_in - smem),
        out_specs=jax.tree.map(lambda _: pl.BlockSpec(memory_space=pltpu.VMEM), outs),
        scratch_shapes=list(scratch),
        name=name,
        compiler_params=pltpu.CompilerParams(vmem_limit_bytes=56 * 1024 * 1024),
        cost_estimate=pl.CostEstimate(flops=flops, transcendentals=0, bytes_accessed=1 << 20),
    )


def shape(dims, kind=F32):
    return jax.ShapeDtypeStruct(dims, kind)


def dot(a, b, precision=None):
    return jnp.dot(a, b, preferred_element_type=F32, precision=precision)


def project_body(first):
    def body(pos, r0, r1, r2, r3, s0, s1, s2, s3, wg, wi, wr, own_gi, snd_gi, own_st, snd_st, ssq):
        mine, other = (r0, r1, r2, r3), (s0, s1, s2, s3)
        y, x, ci = pos[0], pos[1], pos[2]
        for s in range(4):
            ids = []
            for t in range(4):
                dy, dx = (s, t) if first else (t, s)
                ids.append(((y - dy) & 3) * 4 + ((x - dx) & 3))
            lhs = jnp.concatenate([mine[s][t, :HALF] for t in range(4)], axis=1)

            def rhs(ref, lo, hi):
                return jnp.concatenate([ref[i, :, lo:hi] for i in ids], axis=0)

            parts = [dot(lhs, rhs(wg, 0, CH)), dot(lhs, rhs(wi, 0, CH))]
            away = [dot(lhs, rhs(wr, 0, CH)), dot(lhs, rhs(wr, CH, 2 * CH))]
            cols = []
            for cb in range(3):
                col = []
                for t in range(4):
                    a = mine[s][t, HALF + 64 * cb : HALF + 64 * cb + 64]
                    b = other[t][s, HALF + 64 * cb : HALF + 64 * cb + 64]
                    col += [a, b] if first else [b, a]
                cols.append(jnp.concatenate(col, axis=0))
            state = [dot(lhs, jnp.concatenate(cols[:2], axis=1)), dot(lhs, cols[2])]
            squares = None
            for t in range(4):
                v = mine[s][t, :HALF].astype(F32)
                squares = v * v if squares is None else squares + v * v
            if s == 0:
                own_gi[:, :CH] = parts[0]
                own_gi[:, CH:] = parts[1]
                ssq[:, :CH] = away[0]
                ssq[:, CH : 2 * CH] = away[1]
                own_st[:, : 2 * N] = state[0]
                own_st[:, 2 * N :] = state[1]
                ssq[:, 2 * CH :] = squares
            else:
                own_gi[:, :CH] += parts[0]
                own_gi[:, CH:] += parts[1]
                ssq[:, :CH] += away[0]
                ssq[:, CH : 2 * CH] += away[1]
                own_st[:, : 2 * N] += state[0]
                own_st[:, 2 * N :] += state[1]
                ssq[:, 2 * CH :] += squares
        snd_gi[...] = ssq[:, : 2 * CH].astype(BF16)
        total = jnp.sum(ssq[:, 2 * CH :], axis=1, keepdims=True)
        rates = own_st[:, 2 * N :]
        lane = lax.broadcasted_iota(jnp.int32, (HALF, N), 1)
        start = ci * HEADS
        away_start = (ci ^ 1) * HEADS
        own_rate = pltpu.roll(rates, (N - start) & (N - 1), 1)
        away_rate = pltpu.roll(rates, (N - away_start) & (N - 1), 1)
        own_st[:, 2 * N :] = jnp.where(lane < HEADS, own_rate, total)
        snd_st[:, : 2 * N] = own_st[:, : 2 * N]
        snd_st[:, 2 * N :] = jnp.where(lane < HEADS, away_rate, total)

    return body


def project(first, pos, mine, other, wg, wi, wr):
    outs = (
        shape((HALF, 2 * CH)),
        shape((HALF, 2 * CH), BF16),
        shape((HALF, 3 * N)),
        shape((HALF, 3 * N)),
    )
    call = kernel(
        project_body(first), outs, "project", 12, 1, (pltpu.VMEM((HALF, 2 * CH + N), F32),), 2 * HALF * 2048 * 1408
    )
    return call(pos, *mine, *other, wg, wi, wr)


def join_body(gi_a, rgi_a, st_a, rst_a, gi_b, rgi_b, st_b, rst_b, gate, inner, state, rate):
    for h, (gi, rgi, st, rst) in enumerate(((gi_a, rgi_a, st_a, rst_a), (gi_b, rgi_b, st_b, rst_b))):
        rows = slice(h * HALF, (h + 1) * HALF)
        tail = st[:, 2 * N :] + rst[:, 2 * N :]
        inverse = lax.rsqrt(tail[:, HEADS : HEADS + 1] / D + EPS)
        gate[rows] = ((gi[:, :CH] + rgi[:, :CH].astype(F32)) * inverse).astype(BF16)
        inner[rows] = ((gi[:, CH:] + rgi[:, CH:].astype(F32)) * inverse).astype(BF16)
        state[rows] = (st[:, : 2 * N] + rst[:, : 2 * N]) * inverse
        rate[rows] = tail * inverse


def join(*parts):
    outs = (shape((ROWS, CH), BF16), shape((ROWS, CH), BF16), shape((ROWS, 2 * N)), shape((ROWS, N)))
    return kernel(join_body, outs, "join", 8)(*parts)


def silu(v):
    return v / (1.0 + jnp.exp(-v))


def widen(columns, rows):
    return jnp.concatenate(
        [jnp.broadcast_to(columns[:, h : h + 1], (rows, P_SIZE)) for h in range(HEADS)], axis=1
    )


def scan_body(
    rim, inner, state, rate, conv_inner, conv_state, bias, decay,
    values, in_map, out_map, within, until, step, entering, packet,
    pad_i, pad_s,
):
    pad_i[:8] = rim[:, :CH]
    pad_s[:8] = rim[:, CH:]
    pad_i[8:] = inner[...].astype(F32)
    pad_s[8:] = state[...]
    lane = lax.broadcasted_iota(jnp.int32, (Q, N), 1)
    row = lax.broadcasted_iota(jnp.int32, (Q, Q), 0)
    col = lax.broadcasted_iota(jnp.int32, (Q, Q), 1)
    lower = (row >= col).astype(F32)
    carry = jnp.zeros((N, CH), F32)
    passed = jnp.zeros((1, N), F32)
    for c in range(CHUNKS):
        base = c * Q
        rows = slice(base, base + Q)
        vi = jnp.zeros((Q, CH), F32)
        vs = jnp.zeros((Q, CH), F32)
        for k in range(K):
            vi = vi + conv_inner[k : k + 1] * pad_i[base + 5 + k : base + 5 + k + Q]
            vs = vs + conv_state[k : k + 1] * pad_s[base + 5 + k : base + 5 + k + Q]
        vi = silu(vi)
        vs = silu(vs)
        values[rows] = vi
        b = vs[:, :N].astype(BF16)
        in_map[rows] = b
        out_map[rows] = vs[:, N:].astype(BF16)
        v = rate[rows] + bias[...]
        soft = jnp.maximum(v, 0.0) + jnp.log1p(jnp.exp(-jnp.abs(v)))
        steps = jnp.where(lane < HEADS, soft, 0.0)
        step[rows] = steps
        logs = steps * decay[...]
        w = dot(lower, logs, HIGH)
        within[rows] = w
        until[rows] = w + passed
        last = w[Q - 1 : Q]
        tail = jnp.exp(last - w) * steps
        scaled = (vi * widen(tail, Q)).astype(BF16)
        block = lax.dot_general(b, scaled, (((0,), (0,)), ((), ())), preferred_element_type=F32)
        entering[c] = carry.astype(BF16)
        carry = widen(jnp.exp(last), 1) * carry + block
        passed = passed + last
    total = widen(passed, 1)
    high = total.astype(BF16)
    low = (total - high.astype(F32)).astype(BF16)
    packet[:N] = carry.astype(BF16)
    packet[N:] = jnp.concatenate([high, low, jnp.zeros((14, CH), BF16)], axis=0)


def scan(*parts):
    outs = (
        shape((ROWS, CH)),
        shape((ROWS, N), BF16),
        shape((ROWS, N), BF16),
        shape((ROWS, N)),
        shape((ROWS, N)),
        shape((ROWS, N)),
        shape((CHUNKS, N, CH), BF16),
        shape((N + 16, CH), BF16),
    )
    scratch = (pltpu.VMEM((ROWS + 8, CH), F32), pltpu.VMEM((ROWS + 8, CH), F32))
    return kernel(scan_body, outs, "scan", 8, 0, scratch)(*parts)


def inside_body(values, in_map, out_map, within, step, entering, skip, result):
    row = lax.broadcasted_iota(jnp.int32, (Q, Q), 0)
    col = lax.broadcasted_iota(jnp.int32, (Q, Q), 1)
    lower = row >= col
    for c in range(CHUNKS):
        rows = slice(c * Q, (c + 1) * Q)
        b, out, w, vi = in_map[rows], out_map[rows], within[rows], values[rows]
        scores = lax.dot_general(out, b, (((1,), (1,)), ((), ())), preferred_element_type=F32)
        flat = w.T
        stepped = (vi * widen(step[rows], Q)).astype(BF16)
        parts = []
        for h in range(HEADS):
            gap = w[:, h : h + 1] - flat[h : h + 1]
            mixing = (scores * jnp.exp(jnp.where(lower, gap, -jnp.inf))).astype(BF16)
            parts.append(dot(mixing, stepped[:, h * P_SIZE : (h + 1) * P_SIZE]))
        local = jnp.concatenate(parts, axis=1)
        local = local + dot(out, entering[c]) * widen(jnp.exp(w), Q)
        result[rows] = local + skip[...] * vi


def inside(*parts):
    return kernel(inside_body, shape((ROWS, CH)), "inside", 7)(*parts)


def as_rows(column):
    eye = lax.broadcasted_iota(jnp.int32, (N, N), 0) == lax.broadcasted_iota(jnp.int32, (N, N), 1)
    parts = []
    for i in range(4):
        part = jnp.where(eye, jnp.broadcast_to(column[i * N : (i + 1) * N], (N, N)), 0.0)
        parts.append(jnp.sum(part, axis=0, keepdims=True))
    return jnp.concatenate(parts, axis=0)


def as_column(rows):
    eye = lax.broadcasted_iota(jnp.int32, (N, N), 0) == lax.broadcasted_iota(jnp.int32, (N, N), 1)
    parts = []
    for i in range(4):
        part = jnp.where(eye, jnp.broadcast_to(rows[i : i + 1], (N, N)), 0.0)
        parts.append(jnp.sum(part, axis=1, keepdims=True))
    return jnp.concatenate(parts, axis=0)


def gated_body(p1, p2, p3, p4, p5, p6, p7, local, out_map, until, gate, gate_gain, shaped, energy):
    carried = jnp.zeros((N, CH), F32)
    log = jnp.zeros((1, CH), F32)
    for p in (p1, p2, p3, p4, p5, p6, p7):
        carried = carried + jnp.exp(log) * p[:N].astype(F32)
        tail = p[N:].astype(F32)
        log = log + (tail[0:1] + tail[1:2])
    carried = carried.astype(BF16)
    for h in range(2):
        squares = []
        for c in (2 * h, 2 * h + 1):
            rows = slice(c * Q, (c + 1) * Q)
            out = local[rows] + dot(out_map[rows], carried) * widen(jnp.exp(until[rows]), Q)
            out = out * silu(gate[rows].astype(F32))
            shaped[rows] = (out * gate_gain[...]).astype(BF16)
            squares.append(jnp.sum(out * out, axis=1, keepdims=True))
        energy[4 * h : 4 * h + 4] = as_rows(jnp.concatenate(squares, axis=0))


def gated(*parts):
    return kernel(gated_body, (shape((ROWS, CH), BF16), shape((8, N))), "gated", 12)(*parts)


def split_rows(energy):
    high = energy.astype(BF16)
    low = (energy - high.astype(F32)).astype(BF16)
    return jnp.concatenate([high, low, jnp.zeros((8, N), BF16)], axis=0)


def spread_body(half):
    def body(pos, own, away, e_own, e_away, wk, wr, o0, o1, o2, o3):
        y, x = pos[0], pos[1]
        rows = slice(half * HALF, (half + 1) * HALF)
        a, b = own[rows], away[rows]
        tail = split_rows(e_own[4 * half : 4 * half + 4] + e_away[4 * half : 4 * half + 4])
        for s, out in enumerate((o0, o1, o2, o3)):
            ids = []
            for t in range(4):
                dy, dx = (t, s) if half == 0 else (s, t)
                ids.append(((y + dy) & 3) * 4 + ((x + dx) & 3))
            for t in range(0, 4, 2):
                w0 = jnp.concatenate([wk[ids[t]], wk[ids[t + 1]]], axis=1)
                w1 = jnp.concatenate([wr[ids[t]], wr[ids[t + 1]]], axis=1)
                block = dot(a, w0) + dot(b, w1)
                out[t, :HALF] = block[:, :N].astype(BF16)
                out[t + 1, :HALF] = block[:, N:].astype(BF16)
            for t in range(4):
                out[t, HALF:] = tail

    return body


def spread(half, *parts):
    outs = (shape((4, HALF + 16, N), BF16),) * 4
    return kernel(spread_body(half), outs, "spread", 7, 1, (), 2 * HALF * 512 * 2048)(*parts)


def half_sum_body(v0, v1, v2, v3, q0, q1, q2, q3):
    for t, q in enumerate((q0, q1, q2, q3)):
        q[:HALF] = sum(v[t, :HALF].astype(F32) for v in (v0, v1, v2, v3)).astype(q.dtype)
        e = sum(v[t, HALF:].astype(F32) for v in (v0, v1, v2, v3))
        e = e[:4] + e[4:8]
        if q.dtype == BF16:
            q[HALF:] = split_rows(e)
        else:
            q[HALF:] = jnp.concatenate([e, jnp.zeros((12, N), F32)], axis=0)


def half_sum(*parts):
    outs = (shape((HALF + 16, N)),) + (shape((HALF + 16, N), BF16),) * 3
    return kernel(half_sum_body, outs, "half_sum", 4)(*parts)


def finish_body(tokens, a0, a1, a2, a3, b0, b1, b2, b3, out):
    for h, (v0, v1, v2, v3) in enumerate(((a0, a1, a2, a3), (b0, b1, b2, b3))):
        rows = slice(h * HALF, (h + 1) * HALF)
        total = v0[:HALF] + v1[:HALF].astype(F32) + v2[:HALF].astype(F32) + v3[:HALF].astype(F32)
        e = v0[HALF:] + v1[HALF:].astype(F32) + v2[HALF:].astype(F32) + v3[HALF:].astype(F32)
        scale = lax.rsqrt(as_column(e[:4] + e[4:8]) / DI + EPS)
        out[rows] = (tokens[rows].astype(F32) + total * scale).astype(BF16)


def finish(*parts):
    return kernel(finish_body, shape((ROWS, N), BF16), "finish", 9)(*parts)


def gather(half, first):
    def go(value, steps, along_x):
        return plane_move(value, 0, steps, 0) if along_x else plane_move(value, steps, 0, 0)

    near = jnp.stack([half, go(half, 1, first), go(half, 2, first), go(half, -1, first)])
    return [near, go(near, 1, not first), go(near, 2, not first), go(near, -1, not first)]


def local(
    tokens,
    norm_gain,
    gate_proj,
    inner_proj,
    state_proj,
    conv_inner,
    conv_state,
    log_rate,
    rate_bias,
    skip_gain,
    gate_gain,
    out_proj,
):
    ci = lax.axis_index("chan")
    core = ci & 1
    y, x = ci >> 3, (ci >> 1) & 3
    pos = jnp.stack([y, x, ci]).astype(jnp.int32)

    own_gain = lax.dynamic_slice_in_dim(norm_gain, ci * N, N)
    state_w = (state_proj.astype(F32) * own_gain[:, None]).astype(BF16)
    state_w = state_w.reshape(2, 64, 3, N).transpose(0, 2, 1, 3).reshape(2, 192, N)
    half_a = jnp.concatenate([tokens[:HALF], state_w[0]], axis=0)
    half_b = jnp.concatenate([tokens[HALF:], state_w[1]], axis=0)
    all_a = gather(half_a, True)
    all_b = gather(half_b, False)

    gain = norm_gain.reshape(16, 2, N, 1)

    def pick(weight, which):
        part = lax.dynamic_index_in_dim(weight.reshape(16, 2, N, CH), which, 1, keepdims=False)
        scale = lax.dynamic_index_in_dim(gain, which, 1, keepdims=False)
        return (part.astype(F32) * scale).astype(BF16)

    keep_g, keep_i = pick(gate_proj, core), pick(inner_proj, core)
    away = jnp.concatenate([pick(gate_proj, 1 - core), pick(inner_proj, 1 - core)], axis=2)
    got = swap(away)
    out_w = out_proj.reshape(CH, 16, 2, N)
    keep_w = lax.dynamic_index_in_dim(out_w, core, 2, keepdims=False).transpose(1, 0, 2)
    got_w = swap(lax.dynamic_index_in_dim(out_w, 1 - core, 2, keepdims=False).transpose(1, 0, 2))

    gi_a, sgi_a, st_a, sst_a = project(True, pos, all_a, all_b, keep_g, keep_i, got)
    rgi_a, rst_a = swap(sgi_a), swap(sst_a)
    gi_b, sgi_b, st_b, sst_b = project(False, pos, all_b, all_a, keep_g, keep_i, got)
    rgi_b, rst_b = swap(sgi_b), swap(sst_b)

    edge = gi_b[-8:, CH:] + rgi_b[-8:, CH:].astype(F32)
    edge_st = st_b[-8:] + rst_b[-8:]
    edge_scale = lax.rsqrt(edge_st[:, 2 * N + HEADS : 2 * N + HEADS + 1] / D + EPS)
    edge = (edge * edge_scale).astype(BF16).astype(F32)
    rim = later(jnp.concatenate([edge, edge_st[:, : 2 * N] * edge_scale], axis=1), 1)

    gate, inner, state, rate = join(gi_a, rgi_a, st_a, rst_a, gi_b, rgi_b, st_b, rst_b)

    bias = jnp.pad(rate_bias, (0, N - HEADS))[None]
    decay = jnp.pad(-jnp.exp(log_rate), (0, N - HEADS))[None]
    values, in_map, out_map, within, until, step, entering, packet = scan(
        rim, inner, state, rate, conv_inner, conv_state, bias, decay
    )
    packets = [later(packet, s) for s in range(1, 8)]
    skip = jnp.repeat(skip_gain, P_SIZE)[None]
    result = inside(values, in_map, out_map, within, step, entering, skip)
    shaped, energy = gated(*packets, result, out_map, until, gate, gate_gain[None])

    away_shaped, away_energy = swap(shaped), swap(energy)
    blocks_a = spread(0, pos, shaped, away_shaped, energy, away_energy, keep_w, got_w)
    sums_a = [blocks_a[0]] + [plane_move(blocks_a[s], 0, s) for s in range(1, 4)]
    blocks_b = spread(1, pos, shaped, away_shaped, energy, away_energy, keep_w, got_w)
    sums_b = [blocks_b[0]] + [plane_move(blocks_b[s], s, 0) for s in range(1, 4)]
    q_a = half_sum(*sums_a)
    last_a = [q_a[0]] + [plane_move(q_a[t], t, 0) for t in range(1, 4)]
    q_b = half_sum(*sums_b)
    last_b = [q_b[0]] + [plane_move(q_b[t], 0, t) for t in range(1, 4)]
    return finish(tokens, *last_a, *last_b)


def solution(mesh):
    return jax.shard_map(
        local,
        mesh=mesh,
        in_specs=(
            P("seq", "chan"),
            P(),
            P(None, "chan"),
            P(None, "chan"),
            P("chan", None),
            P(None, "chan"),
            P(),
            P("chan"),
            P("chan"),
            P("chan"),
            P("chan"),
            P("chan", None),
        ),
        out_specs=P("seq", "chan"),
        check_vma=False,
    )
```

```python
import jax
import jax.numpy as jnp
from jax import lax
from jax.experimental import pallas as pl
from jax.experimental.pallas import tpu as pltpu
from jax.sharding import PartitionSpec as P


D = 4096
DI = 8192
N = 128
P_SIZE = 64
K = 4
Q = 256
ROWS = 1024
HALF = 512
CHUNKS = 4
HEADS = 4
CH = 256
EPS = 1e-05
F32 = jnp.float32
BF16 = jnp.bfloat16
HIGH = lax.Precision.HIGHEST


def plane_move(value, steps, phase):
    pairs = []
    for y in range(4):
        for x in range(4):
            for c in range(2):
                dy, dx = (0, steps) if c == phase else (steps, 0)
                pairs.append(((y * 4 + x) * 2 + c, ((y + dy) % 4 * 4 + (x + dx) % 4) * 2 + c))
    return lax.ppermute(value, "chan", pairs)


def swap(value):
    return lax.ppermute(value, "chan", [(i, i ^ 1) for i in range(32)])


def later(value, steps):
    return lax.ppermute(value, "seq", [(i, i + steps) for i in range(8 - steps)])


def kernel(body, outs, n_in, smem=0, scratch=(), flops=0, place=True):
    inner = pl.pallas_call(
        body,
        out_shape=jax.tree.map(lambda o: pltpu.VMEM(o.shape, o.dtype), outs) if place else outs,
        in_specs=[pl.BlockSpec(memory_space=pltpu.SMEM)] * smem + [pl.BlockSpec(memory_space=pltpu.VMEM)] * (n_in - smem),
        out_specs=jax.tree.map(lambda _: pl.BlockSpec(memory_space=pltpu.VMEM), outs),
        scratch_shapes=list(scratch),
        compiler_params=pltpu.CompilerParams(vmem_limit_bytes=16 * 1024 * 1024),
        cost_estimate=pl.CostEstimate(flops=flops, transcendentals=0, bytes_accessed=1 << 20),
    )

    def call(*args):
        placed = [pltpu.with_memory_space_constraint(a, pltpu.VMEM) for a in args[smem:]]
        return inner(*args[:smem], *placed)

    return call


def shape(dims, kind=F32):
    return jax.ShapeDtypeStruct(dims, kind)


def dot(a, b, precision=None):
    return jnp.dot(a, b, preferred_element_type=F32, precision=precision)


def eye(n):
    return lax.broadcasted_iota(jnp.int32, (n, n), 0) == lax.broadcasted_iota(jnp.int32, (n, n), 1)


def stand(row):
    return jnp.sum(jnp.where(eye(N), jnp.broadcast_to(row, (N, N)), 0.0), axis=1, keepdims=True)


def lay(column):
    return jnp.sum(jnp.where(eye(N), jnp.broadcast_to(column, (N, N)), 0.0), axis=0, keepdims=True)


def as_rows(column):
    return jnp.concatenate([lay(column[i * N : (i + 1) * N]) for i in range(4)], axis=0)


def as_column(rows):
    return jnp.concatenate([stand(rows[i : i + 1]) for i in range(4)], axis=0)


def half(index):
    return pl.ds(pl.multiple_of(index * HALF, HALF), HALF)


BLOCK = 2 * HALF + 3 * N


def block_body(pos, tokens, away, state_w, gain, out):
    c, ci = pos[2], pos[3]
    out[half(c)] = tokens[half(c)]
    out[half(1 - c)] = away[...]
    scaled = (state_w[...].astype(F32) * stand(gain[pl.ds(ci, 1)])).astype(BF16)
    for b in range(3):
        out[2 * HALF + b * N : 2 * HALF + (b + 1) * N] = scaled[:, b * N : (b + 1) * N]


def scale_body(gate, inner, gain, out):
    def step(i, _):
        rows = pl.ds(pl.multiple_of(i * N, N), N)
        column = stand(gain[pl.ds(i, 1)])
        out[rows, :CH] = (gate[rows].astype(F32) * column).astype(BF16)
        out[rows, CH:] = (inner[rows].astype(F32) * column).astype(BF16)
        return 0

    lax.fori_loop(0, 2 * 16, step, 0)


def mark_body(ref, out):
    out[...] = ref[0, :16]


def mark(piece):
    return kernel(mark_body, shape((16, N), BF16), 1)(piece)


def pick_body(count):
    def body(*refs):
        for i, ref in enumerate(refs[:count]):
            refs[-1][2 * i] = ref[0, 2 * HALF :]
            refs[-1][2 * i + 1] = ref[1, 2 * HALF :]

    return body


def pick(*pieces, marks=()):
    count = len(pieces)
    out = shape((2 * count, 3 * N, N), BF16)
    return kernel(pick_body(count), out, count + len(marks))(*pieces, *marks)


def owner(pos, s, t):
    first = pos[2] == 0
    dy = jnp.where(first, s, t)
    dx = jnp.where(first, t, s)
    return ((pos[0] - dy) & 3) * 4 + ((pos[1] - dx) & 3)


STEP = 256


def add_slots(pos, slots, keep, got, acc, squares, fresh):
    def rows_of(r, _):
        rows = pl.ds(pl.multiple_of(r * STEP, STEP), STEP)
        low = pl.ds(pl.multiple_of(r * STEP, STEP), STEP)
        high = pl.ds(pl.multiple_of(HALF + r * STEP, STEP), STEP)
        square = None if fresh else squares[rows]
        for n, (s, pieces) in enumerate(slots):
            parts = []
            for t in range(4):
                ref = pieces[t // 2]
                parts += [ref[t % 2, low], ref[t % 2, high]]
            for v in parts:
                v = v.astype(F32)
                square = v * v if square is None else square + v * v
            lhs = jnp.concatenate(parts, axis=1)
            ids = [pl.ds(pl.multiple_of(owner(pos, s, t) * 2 * N, 2 * N), 2 * N) for t in range(4)]
            for w, ref in enumerate((keep, got)):
                for b in range(2):
                    cols = slice(w * 2 * CH + b * CH, w * 2 * CH + (b + 1) * CH)
                    rhs = jnp.concatenate([ref[i, b * CH : (b + 1) * CH] for i in ids], axis=0)
                    part = dot(lhs, rhs)
                    if fresh and n == 0:
                        acc[rows, cols] = part
                    else:
                        acc[rows, cols] += part
        squares[rows] = square
        return 0

    lax.fori_loop(0, HALF // STEP, rows_of, 0)


def most_body(pos, a0, a1, b0, b1, d0, d1, keep, got, acc, squares):
    add_slots(pos, ((0, (a0, a1)), (1, (b0, b1)), (3, (d0, d1))), keep, got, acc, squares, True)


def most(pos, *parts):
    outs = (shape((HALF, 4 * CH)), shape((HALF, N)))
    return kernel(most_body, outs, 9, 1, (), 2 * HALF * 3072 * 1024)(pos, *parts)


def rest_body(pos, c0, c1, keep, got, acc_in, squares_in, own, send, scale, acc, squares):
    acc[...] = acc_in[...]
    squares[...] = squares_in[...]
    add_slots(pos, ((2, (c0, c1)),), keep, got, acc, squares, False)
    inverse = lax.rsqrt(jnp.sum(squares[...], axis=1, keepdims=True) / D + EPS)
    own[...] = (acc[:, : 2 * CH] * inverse).astype(BF16)
    send[...] = (acc[:, 2 * CH :] * inverse).astype(BF16)
    scale[...] = jnp.broadcast_to(inverse, (HALF, N))


def rest(pos, *parts):
    outs = (shape((HALF, 2 * CH), BF16), shape((HALF, 2 * CH), BF16), shape((HALF, N)))
    scratch = (pltpu.VMEM((HALF, 4 * CH), F32), pltpu.VMEM((HALF, N), F32))
    return kernel(rest_body, outs, 7, 1, scratch, 2 * HALF * 1024 * 1024)(pos, *parts)


def state_body(pos, a0, a1, b0, b1, d0, d1, c0, c1, most_own, most_got, last_own, last_got, scale, out):
    c, ci = pos[2], pos[3]
    pieces = (a0, a1, b0, b1, d0, d1, c0, c1)
    order = (0, 1, 3, 2)

    def rows_of(r, _):
        rows = pl.ds(pl.multiple_of(r * STEP, STEP), STEP)
        mine = pl.ds(pl.multiple_of(c * HALF + r * STEP, STEP), STEP)
        other = pl.ds(pl.multiple_of((1 - c) * HALF + r * STEP, STEP), STEP)
        total = [None, None]
        for g in range(4):
            lhs, w = [], [[], [], []]
            for k in range(4):
                i = 4 * g + k
                ref = pieces[i // 2]
                lhs += [ref[i % 2, mine], ref[i % 2, other]]
                j = 4 * order.index(k) + order[g]
                for b in range(3):
                    cut = slice(b * N, (b + 1) * N)
                    w[b].append(most_own[i, cut] if i < 12 else last_own[i - 12, cut])
                    w[b].append(most_got[j, cut] if j < 12 else last_got[j - 12, cut])
            lhs = jnp.concatenate(lhs, axis=1)
            w = [jnp.concatenate(v, axis=0) for v in w]
            for j, v in enumerate((dot(lhs, jnp.concatenate(w[:2], axis=1)), dot(lhs, w[2]))):
                total[j] = v if total[j] is None else total[j] + v
        inverse = scale[rows]
        out[rows, :N] = total[0][:, :N] * inverse
        out[rows, N : 2 * N] = total[0][:, N:] * inverse
        rates = total[1] * inverse
        lane = lax.broadcasted_iota(jnp.int32, (STEP, N), 1)
        own_rate = pltpu.roll(rates, (N - ci * HEADS) & (N - 1), 1)
        away_rate = pltpu.roll(rates, (N + HEADS - (ci ^ 1) * HEADS) & (N - 1), 1)
        out[rows, 2 * N :] = jnp.where(lane < HEADS, own_rate, away_rate)
        return 0

    lax.fori_loop(0, HALF // STEP, rows_of, 0)


def state_of(pos, *parts):
    return kernel(state_body, shape((HALF, 3 * N)), 14, 1, (), 2 * HALF * 4096 * 384)(pos, *parts)


def silu(v):
    return v / (1.0 + jnp.exp(-v))


def widen(columns, rows):
    return jnp.concatenate(
        [jnp.broadcast_to(columns[:, h : h + 1], (rows, P_SIZE)) for h in range(HEADS)], axis=1
    )


def scan_body(
    pos, rim, own_gi, got_gi, own_st, got_st, conv_inner, conv_state, small,
    values, in_map, out_map, within, until, step, entering, packet,
    pad_i, pad_s, rate, carry, passed,
):
    c = pos[2]
    pad_i[:8] = rim[:, :CH]
    pad_s[:8] = rim[:, CH:]
    for which, gi, st in ((c, own_gi, own_st), (1 - c, got_gi, got_st)):
        rows = pl.ds(pl.multiple_of(8 + which * HALF, 8), HALF)
        pad_i[rows] = gi[:, CH:].astype(F32)
        pad_s[rows] = st[:, : 2 * N]
        tail = st[:, 2 * N :]
        rate[half(which)] = tail if st is own_st else pltpu.roll(tail, N - HEADS, 1)
    lane = lax.broadcasted_iota(jnp.int32, (Q, N), 1)
    lower = (
        lax.broadcasted_iota(jnp.int32, (Q, Q), 0) >= lax.broadcasted_iota(jnp.int32, (Q, Q), 1)
    ).astype(F32)
    carry[...] = jnp.zeros((N, CH), F32)
    passed[...] = jnp.zeros((8, N), F32)

    def chunk(i, _):
        rows = pl.ds(pl.multiple_of(i * Q, Q), Q)
        window = pl.ds(pl.multiple_of(i * Q, Q), Q + 8)
        wi, ws = pad_i[window], pad_s[window]
        vi = jnp.zeros((Q, CH), F32)
        vs = jnp.zeros((Q, CH), F32)
        for k in range(K):
            vi = vi + conv_inner[k : k + 1] * wi[5 + k : 5 + k + Q]
            vs = vs + conv_state[k : k + 1] * ws[5 + k : 5 + k + Q]
        vi = silu(vi)
        vs = silu(vs)
        values[rows] = vi
        b = vs[:, :N].astype(BF16)
        in_map[rows] = b
        out_map[rows] = vs[:, N:].astype(BF16)
        v = rate[rows] + small[0:1]
        soft = jnp.maximum(v, 0.0) + jnp.log1p(jnp.exp(-jnp.abs(v)))
        steps = jnp.where(lane < HEADS, soft, 0.0)
        step[rows] = steps
        w = dot(lower, steps * small[1:2], HIGH)
        within[rows] = w
        before = passed[:1]
        until[rows] = w + before
        last = w[Q - 1 : Q]
        scaled = (vi * widen(jnp.exp(last - w) * steps, Q)).astype(BF16)
        block = lax.dot_general(b, scaled, (((0,), (0,)), ((), ())), preferred_element_type=F32)
        old = carry[...]
        entering[i] = old.astype(BF16)
        carry[...] = widen(jnp.exp(last), 1) * old + block
        passed[:1] = before + last
        return 0

    lax.fori_loop(0, CHUNKS, chunk, 0)
    total = widen(passed[:1], 1)
    high = total.astype(BF16)
    low = (total - high.astype(F32)).astype(BF16)
    packet[:N] = carry[...].astype(BF16)
    packet[N:] = jnp.concatenate([high, low, jnp.zeros((14, CH), BF16)], axis=0)


def scan(pos, *parts):
    outs = (
        shape((ROWS, CH)),
        shape((ROWS, N), BF16),
        shape((ROWS, N), BF16),
        shape((ROWS, N)),
        shape((ROWS, N)),
        shape((ROWS, N)),
        shape((CHUNKS, N, CH), BF16),
        shape((N + 16, CH), BF16),
    )
    scratch = (
        pltpu.VMEM((ROWS + 8, CH), F32),
        pltpu.VMEM((ROWS + 8, CH), F32),
        pltpu.VMEM((ROWS, N), F32),
        pltpu.VMEM((N, CH), F32),
        pltpu.VMEM((8, N), F32),
    )
    return kernel(scan_body, outs, 9, 1, scratch)(pos, *parts)


def inside_body(pos, own_gi, got_gi, values, in_map, out_map, within, step, entering, small, result, opened, gate):
    c = pos[2]
    skip = widen(small[2:3], 1)
    gate[half(c)] = own_gi[:, :CH]
    gate[half(1 - c)] = got_gi[:, :CH]
    lower = lax.broadcasted_iota(jnp.int32, (Q, Q), 0) >= lax.broadcasted_iota(jnp.int32, (Q, Q), 1)

    def chunk(i, _):
        rows = pl.ds(pl.multiple_of(i * Q, Q), Q)
        opened[rows] = silu(gate[rows].astype(F32))
        b, out, w, vi = in_map[rows], out_map[rows], within[rows], values[rows]
        scores = lax.dot_general(out, b, (((1,), (1,)), ((), ())), preferred_element_type=F32)
        flat = w.T
        stepped = (vi * widen(step[rows], Q)).astype(BF16)
        parts = []
        for h in range(HEADS):
            gap = w[:, h : h + 1] - flat[h : h + 1]
            mixing = (scores * jnp.exp(jnp.where(lower, gap, -jnp.inf))).astype(BF16)
            parts.append(dot(mixing, stepped[:, h * P_SIZE : (h + 1) * P_SIZE]))
        local = jnp.concatenate(parts, axis=1)
        local = local + dot(out, entering[i]) * widen(jnp.exp(w), Q)
        result[rows] = local + skip * vi
        return 0

    lax.fori_loop(0, CHUNKS, chunk, 0)


def inside(pos, *parts):
    outs = (shape((ROWS, CH)), shape((ROWS, CH)))
    scratch = (pltpu.VMEM((ROWS, CH), BF16),)
    return kernel(inside_body, outs, 10, 1, scratch)(pos, *parts)


def split(energy):
    high = energy.astype(BF16)
    return high, (energy - high.astype(F32)).astype(BF16)


def gated_body(pos, p1, p2, p3, p4, p5, p6, p7, local, out_map, until, opened, gate_gain, own, send, energy):
    c = pos[2]
    carried = jnp.zeros((N, CH), F32)
    log = jnp.zeros((1, CH), F32)
    for p in (p1, p2, p3, p4, p5, p6, p7):
        carried = carried + jnp.exp(log) * p[:N].astype(F32)
        tail = p[N:].astype(F32)
        log = log + (tail[0:1] + tail[1:2])
    carried = carried.astype(BF16)
    for which, to in ((1 - c, send), (c, own)):
        rows = half(which)
        out = local[rows] + dot(out_map[rows], carried) * widen(jnp.exp(until[rows]), HALF)
        out = out * opened[rows]
        to[:HALF] = (out * gate_gain[...]).astype(BF16)
        e = as_rows(jnp.sum(out * out, axis=1, keepdims=True))
        if to is own:
            energy[...] = jnp.concatenate([e, jnp.zeros((4, N), F32)], axis=0)
        else:
            e = jnp.concatenate(split(e), axis=1)
            to[HALF:] = jnp.concatenate([e, jnp.zeros((12, CH), BF16)], axis=0)


def gated(pos, *parts):
    outs = (shape((HALF, CH), BF16), shape((HALF + 16, CH), BF16), shape((8, N)))
    return kernel(gated_body, outs, 13, 1)(pos, *parts)


TALL = 2 * HALF + 16


def energy_rows(energy):
    return jnp.concatenate([*split(energy), jnp.zeros((8, N), BF16)], axis=0)


def spread_body(s):
    def body(pos, own, got, energy, w_own, w_got, out):
        tail = got[HALF:].astype(F32)
        tail = energy_rows(energy[:4] + (tail[:4, :N] + tail[:4, N:]))
        lhs = jnp.concatenate([own[...], got[:HALF]], axis=1)
        first = pos[2] == 0

        def block(t, _):
            dy = jnp.where(first, t, s)
            dx = jnp.where(first, s, t)
            chip = ((pos[0] + dy) & 3) * 4 + ((pos[1] + dx) & 3)
            cols = pl.ds(pl.multiple_of(chip * 2 * N, 2 * N), 2 * N)
            part = dot(lhs, jnp.concatenate([w_own[:, cols], w_got[:, cols]], axis=0))
            out[t, :HALF] = part[:, :N].astype(BF16)
            out[t, HALF : 2 * HALF] = part[:, N:].astype(BF16)
            out[t, 2 * HALF :] = tail
            return 0

        lax.fori_loop(0, 4, block, 0)

    return body


def spread(s, pos, *parts):
    out = shape((4, TALL, N), BF16)
    return kernel(spread_body(s), out, 6, 1, (), 2 * HALF * 512 * 1024)(pos, *parts)


def half_sum_body(v0, v1, v2, v3, q0, q1, q2, q3):
    for t, q in enumerate((q0, q1, q2, q3)):
        q[: 2 * HALF] = sum(v[t, : 2 * HALF].astype(F32) for v in (v0, v1, v2, v3)).astype(q.dtype)
        e = sum(v[t, 2 * HALF :].astype(F32) for v in (v0, v1, v2, v3))
        e = e[:4] + e[4:8]
        if q.dtype == BF16:
            q[2 * HALF :] = energy_rows(e)
        else:
            q[2 * HALF :] = jnp.concatenate([e, jnp.zeros((12, N), F32)], axis=0)


def half_sum(*parts):
    outs = (shape((TALL, N)),) + (shape((TALL, N), BF16),) * 3
    return kernel(half_sum_body, outs, 4)(*parts)


def total_body(pos, v0, v1, v2, v3, own, send):
    c = pos[2]
    e = v0[2 * HALF :] + v1[2 * HALF :].astype(F32) + v2[2 * HALF :].astype(F32) + v3[2 * HALF :].astype(F32)
    scale = lax.rsqrt(as_column(e[:4] + e[4:8]) / DI + EPS)
    for which, to in ((1 - c, send), (c, own)):
        rows = half(which)
        to[...] = (v0[rows] + v1[rows].astype(F32) + v2[rows].astype(F32) + v3[rows].astype(F32)) * scale


def total(pos, *parts):
    return kernel(total_body, (shape((HALF, N)), shape((HALF, N))), 5, 1)(pos, *parts)


def finish_body(pos, tokens, own, got, out):
    c = pos[2]
    for which, part in ((c, own), (1 - c, got)):
        rows = half(which)
        out[rows] = (tokens[rows].astype(F32) + part[...]).astype(BF16)


def finish(pos, *parts):
    return kernel(finish_body, shape((ROWS, N), BF16), 4, 1, place=False)(pos, *parts)


def local(
    tokens,
    norm_gain,
    gate_proj,
    inner_proj,
    state_proj,
    conv_inner,
    conv_state,
    log_rate,
    rate_bias,
    skip_gain,
    gate_gain,
    out_proj,
):
    ci = lax.axis_index("chan")
    core = ci & 1
    pos = jnp.stack([ci >> 3, (ci >> 1) & 3, core, ci]).astype(jnp.int32)
    gain = norm_gain.reshape(32, N)

    small = jnp.pad(jnp.stack([rate_bias, -jnp.exp(log_rate), skip_gain]), ((0, 5), (0, N - HEADS)))

    away_tokens = swap(lax.dynamic_slice_in_dim(tokens, (1 - core) * HALF, HALF, 0))
    block = kernel(block_body, shape((BLOCK, N), BF16), 5, 1)(pos, tokens, away_tokens, state_proj, gain)

    steps = [block] + [plane_move(block, k, 0) for k in (1, 2, -1)]
    a0, a1 = jnp.stack(steps[:2]), jnp.stack(steps[2:])
    near_mark = mark(a0)
    b0, d1 = plane_move(a0, 1, 1), plane_move(a1, -1, 1)
    b1, d0 = plane_move(a1, 1, 1), plane_move(a0, -1, 1)
    far_mark = mark(b0)
    c0, c1 = plane_move(b0, 1, 1), plane_move(d1, -1, 1)

    keep = kernel(scale_body, shape((D, 2 * CH), BF16), 3)(gate_proj, inner_proj, gain)
    got = swap(keep)
    got_w = swap(out_proj)

    most_own = pick(a0, a1, b0, b1, d0, d1, marks=(near_mark, far_mark))
    most_got = swap(most_own)
    acc, squares = most(pos, a0, a1, b0, b1, d0, d1, keep, got)
    last_own = pick(c0, c1)
    last_got = swap(last_own)
    own_gi, send_gi, scale = rest(pos, c0, c1, keep, got, acc, squares)
    got_gi = swap(send_gi)
    own_st = state_of(pos, a0, a1, b0, b1, d0, d1, c0, c1, most_own, most_got, last_own, last_got, scale)
    got_st = swap(own_st)

    edge = jnp.where(core == 1, own_gi[-8:, CH:], got_gi[-8:, CH:]).astype(F32)
    edge_st = jnp.where(core == 1, own_st[-8:, : 2 * N], got_st[-8:, : 2 * N])
    rim = later(jnp.concatenate([edge, edge_st], axis=1), 1)

    values, in_map, out_map, within, until, step, entering, packet = scan(
        pos, rim, own_gi, got_gi, own_st, got_st, conv_inner, conv_state, small
    )
    packets = [later(packet, s) for s in range(1, 8)]
    result, opened = inside(pos, own_gi, got_gi, values, in_map, out_map, within, step, entering, small)
    own_g, send_g, energy = gated(pos, *packets, result, out_map, until, opened, gate_gain[None])

    got_g = swap(send_g)
    parts = [None] * 4
    for s in (2, 1, 3, 0):
        parts[s] = spread(s, pos, own_g, got_g, energy, out_proj, got_w)
    sums = [parts[0]] + [plane_move(parts[s], s, 0) for s in (1, 2, 3)]
    q = half_sum(*sums)
    last = [q[0]] + [plane_move(q[t], t, 1) for t in (1, 2, 3)]
    own, send = total(pos, *last)
    return finish(pos, tokens, own, swap(send))


def solution(mesh):
    return jax.shard_map(
        local,
        mesh=mesh,
        in_specs=(
            P("seq", "chan"),
            P(),
            P(None, "chan"),
            P(None, "chan"),
            P("chan", None),
            P(None, "chan"),
            P(),
            P("chan"),
            P("chan"),
            P("chan"),
            P("chan"),
            P("chan", None),
        ),
        out_specs=P("seq", "chan"),
        check_vma=False,
    )
```

```python
import jax
import jax.numpy as jnp
from jax import lax
from jax.experimental import pallas as pl
from jax.experimental.pallas import tpu as pltpu
from jax.sharding import PartitionSpec as P


D = 4096
DI = 8192
N = 128
P_SIZE = 64
K = 4
Q = 256
ROWS = 1024
HALF = 512
CHUNKS = 4
HEADS = 4
CH = 256
EPS = 1e-05
F32 = jnp.float32
BF16 = jnp.bfloat16
HIGH = lax.Precision.HIGHEST


def plane_move(value, steps, phase):
    pairs = []
    for y in range(4):
        for x in range(4):
            for c in range(2):
                dy, dx = (0, steps) if c == phase else (steps, 0)
                pairs.append(((y * 4 + x) * 2 + c, ((y + dy) % 4 * 4 + (x + dx) % 4) * 2 + c))
    return lax.ppermute(value, "chan", pairs)


def swap(value):
    return lax.ppermute(value, "chan", [(i, i ^ 1) for i in range(32)])


def later(value, steps):
    return lax.ppermute(value, "seq", [(i, i + steps) for i in range(8 - steps)])


def kernel(body, outs, n_in, smem=0, scratch=(), flops=0, place=True, inputs=pltpu.VMEM):
    inner = pl.pallas_call(
        body,
        out_shape=jax.tree.map(lambda o: pltpu.VMEM(o.shape, o.dtype), outs) if place else outs,
        in_specs=[pl.BlockSpec(memory_space=pltpu.SMEM)] * smem + [pl.BlockSpec(memory_space=pltpu.VMEM)] * (n_in - smem),
        out_specs=jax.tree.map(lambda _: pl.BlockSpec(memory_space=pltpu.VMEM), outs),
        scratch_shapes=list(scratch),
        compiler_params=pltpu.CompilerParams(vmem_limit_bytes=16 * 1024 * 1024),
        cost_estimate=pl.CostEstimate(flops=flops, transcendentals=0, bytes_accessed=1 << 20),
    )

    def call(*args):
        placed = [pltpu.with_memory_space_constraint(a, inputs) for a in args[smem:]]
        return inner(*args[:smem], *placed)

    return call


def shape(dims, kind=F32):
    return jax.ShapeDtypeStruct(dims, kind)


def dot(a, b, precision=None):
    return jnp.dot(a, b, preferred_element_type=F32, precision=precision)


def eye(n):
    return lax.broadcasted_iota(jnp.int32, (n, n), 0) == lax.broadcasted_iota(jnp.int32, (n, n), 1)


def stand(row):
    return jnp.sum(jnp.where(eye(N), jnp.broadcast_to(row, (N, N)), 0.0), axis=1, keepdims=True)


def lay(column):
    return jnp.sum(jnp.where(eye(N), jnp.broadcast_to(column, (N, N)), 0.0), axis=0, keepdims=True)


def as_rows(column):
    return jnp.concatenate([lay(column[i * N : (i + 1) * N]) for i in range(4)], axis=0)


def as_column(rows):
    return jnp.concatenate([stand(rows[i : i + 1]) for i in range(4)], axis=0)


def half(index):
    return pl.ds(pl.multiple_of(index * HALF, HALF), HALF)


BLOCK = 2 * HALF + 3 * N


def block_body(pos, tokens, away, state_w, gain, out):
    c, ci = pos[2], pos[3]
    out[half(c)] = tokens[half(c)]
    out[half(1 - c)] = away[half(c)]
    scaled = (state_w[...].astype(F32) * stand(gain[pl.ds(ci, 1)])).astype(BF16)
    for b in range(3):
        out[2 * HALF + b * N : 2 * HALF + (b + 1) * N] = scaled[:, b * N : (b + 1) * N]


def scale_body(gate, inner, gain, out):
    def step(i, _):
        rows = pl.ds(pl.multiple_of(i * N, N), N)
        column = stand(gain[pl.ds(i, 1)])
        out[rows, :CH] = (gate[rows].astype(F32) * column).astype(BF16)
        out[rows, CH:] = (inner[rows].astype(F32) * column).astype(BF16)
        return 0

    lax.fori_loop(0, 2 * 16, step, 0)


def mark_body(ref, out):
    out[...] = ref[0, :16]


def mark(piece):
    return kernel(mark_body, shape((16, N), BF16), 1)(piece)


def pick_body(count):
    def body(*refs):
        for i, ref in enumerate(refs[:count]):
            refs[-1][2 * i] = ref[0, 2 * HALF :]
            refs[-1][2 * i + 1] = ref[1, 2 * HALF :]

    return body


def pick(*pieces, marks=()):
    count = len(pieces)
    out = shape((2 * count, 3 * N, N), BF16)
    return kernel(pick_body(count), out, count + len(marks))(*pieces, *marks)


def owner(pos, s, t):
    first = pos[2] == 0
    dy = jnp.where(first, s, t)
    dx = jnp.where(first, t, s)
    return ((pos[0] - dy) & 3) * 4 + ((pos[1] - dx) & 3)


STEP = 256


def add_slots(pos, slots, keep, got, acc, squares, fresh):
    def rows_of(r, _):
        rows = pl.ds(pl.multiple_of(r * STEP, STEP), STEP)
        low = pl.ds(pl.multiple_of(r * STEP, STEP), STEP)
        high = pl.ds(pl.multiple_of(HALF + r * STEP, STEP), STEP)
        square = None if fresh else squares[rows]
        for n, (s, pieces) in enumerate(slots):
            parts = []
            for t in range(4):
                ref = pieces[t // 2]
                parts += [ref[t % 2, low], ref[t % 2, high]]
            for v in parts:
                v = v.astype(F32)
                square = v * v if square is None else square + v * v
            lhs = jnp.concatenate(parts, axis=1)
            ids = [pl.ds(pl.multiple_of(owner(pos, s, t) * 2 * N, 2 * N), 2 * N) for t in range(4)]
            for w, ref in enumerate((keep, got)):
                for b in range(2):
                    cols = slice(w * 2 * CH + b * CH, w * 2 * CH + (b + 1) * CH)
                    rhs = jnp.concatenate([ref[i, b * CH : (b + 1) * CH] for i in ids], axis=0)
                    part = dot(lhs, rhs)
                    if fresh and n == 0:
                        acc[rows, cols] = part
                    else:
                        acc[rows, cols] += part
        squares[rows] = square
        return 0

    lax.fori_loop(0, HALF // STEP, rows_of, 0)


def most_body(pos, a0, a1, b0, b1, d0, d1, keep, got, acc, squares):
    add_slots(pos, ((0, (a0, a1)), (1, (b0, b1)), (3, (d0, d1))), keep, got, acc, squares, True)


def most(pos, *parts):
    outs = (shape((HALF, 4 * CH)), shape((HALF, N)))
    return kernel(most_body, outs, 9, 1, (), 2 * HALF * 3072 * 1024)(pos, *parts)


def rest_body(pos, c0, c1, keep, got, acc, squares, own, send, scale):
    pieces = (c0, c1)

    def rows_of(r, _):
        rows = pl.ds(pl.multiple_of(r * STEP, STEP), STEP)
        high = pl.ds(pl.multiple_of(HALF + r * STEP, STEP), STEP)
        square = squares[rows]
        parts = []
        for t in range(4):
            parts += [pieces[t // 2][t % 2, rows], pieces[t // 2][t % 2, high]]
        for v in parts:
            v = v.astype(F32)
            square = square + v * v
        inverse = lax.rsqrt(jnp.sum(square, axis=1, keepdims=True) / D + EPS)
        scale[rows] = jnp.broadcast_to(inverse, (STEP, N))
        lhs = jnp.concatenate(parts, axis=1)
        ids = [pl.ds(pl.multiple_of(owner(pos, 2, t) * 2 * N, 2 * N), 2 * N) for t in range(4)]
        for w, (ref, out) in enumerate(((keep, own), (got, send))):
            for b in range(2):
                cols = slice(b * CH, (b + 1) * CH)
                rhs = jnp.concatenate([ref[i, cols] for i in ids], axis=0)
                part = acc[rows, w * 2 * CH + b * CH : w * 2 * CH + (b + 1) * CH] + dot(lhs, rhs)
                out[rows, cols] = (part * inverse).astype(BF16)
        return 0

    lax.fori_loop(0, HALF // STEP, rows_of, 0)


def rest(pos, *parts):
    outs = (shape((HALF, 2 * CH), BF16), shape((HALF, 2 * CH), BF16), shape((HALF, N)))
    return kernel(rest_body, outs, 7, 1, (), 2 * HALF * 1024 * 1024)(pos, *parts)


ORDER = (0, 1, 3, 2)


def state_sum(pos, pieces, most_own, most_got, last_own, last_got, slots, finish):
    c = pos[2]

    def rows_of(r, _):
        mine = pl.ds(pl.multiple_of(c * HALF + r * STEP, STEP), STEP)
        other = pl.ds(pl.multiple_of((1 - c) * HALF + r * STEP, STEP), STEP)
        lhs, w = [], [[], [], []]
        for g, k in slots:
            i = 4 * g + k
            lhs += [pieces[i // 2][i % 2, mine], pieces[i // 2][i % 2, other]]
            j = 4 * ORDER.index(k) + ORDER[g]
            for b in range(3):
                cut = slice(b * N, (b + 1) * N)
                w[b].append(most_own[i, cut] if i < 12 else last_own[i - 12, cut])
                w[b].append(most_got[j, cut] if j < 12 else last_got[j - 12, cut])
        lhs = jnp.concatenate(lhs, axis=1)
        w = [jnp.concatenate(v, axis=0) for v in w]
        finish(r, dot(lhs, jnp.concatenate(w[:2], axis=1)), dot(lhs, w[2]))
        return 0

    lax.fori_loop(0, HALF // STEP, rows_of, 0)


EARLY = [(g, k) for g in range(3) for k in (0, 1, 3)]
LATE = [(g, 2) for g in range(3)] + [(3, k) for k in range(4)]


def state_most_body(pos, a0, a1, b0, b1, d0, d1, most_own, most_got, out):
    def finish(r, left, right):
        rows = pl.ds(pl.multiple_of(r * STEP, STEP), STEP)
        out[rows, : 2 * N] = left
        out[rows, 2 * N :] = right

    state_sum(pos, (a0, a1, b0, b1, d0, d1), most_own, most_got, None, None, EARLY, finish)


def state_most(pos, *parts):
    call = kernel(state_most_body, shape((HALF, 3 * N)), 9, 1, (), 2 * HALF * 2304 * 384)
    return call(pos, *parts)


def state_body(pos, a1, b1, d1, c0, c1, most_own, most_got, last_own, last_got, acc, scale, out):
    ci = pos[3]

    def finish(r, left, right):
        rows = pl.ds(pl.multiple_of(r * STEP, STEP), STEP)
        inverse = scale[rows]
        out[rows, :N] = (acc[rows, :N] + left[:, :N]) * inverse
        out[rows, N : 2 * N] = (acc[rows, N : 2 * N] + left[:, N:]) * inverse
        rates = (acc[rows, 2 * N :] + right) * inverse
        lane = lax.broadcasted_iota(jnp.int32, (STEP, N), 1)
        own_rate = pltpu.roll(rates, (N - ci * HEADS) & (N - 1), 1)
        away_rate = pltpu.roll(rates, (N + HEADS - (ci ^ 1) * HEADS) & (N - 1), 1)
        out[rows, 2 * N :] = jnp.where(lane < HEADS, own_rate, away_rate)

    state_sum(pos, (None, a1, None, b1, None, d1, c0, c1), most_own, most_got, last_own, last_got, LATE, finish)


def state_rest(pos, *parts):
    return kernel(state_body, shape((HALF, 3 * N)), 12, 1, (), 2 * HALF * 1792 * 384)(pos, *parts)


def silu(v):
    return v / (1.0 + jnp.exp(-v))


def widen(columns, rows):
    return jnp.concatenate(
        [jnp.broadcast_to(columns[:, h : h + 1], (rows, P_SIZE)) for h in range(HEADS)], axis=1
    )


def scan_body(
    pos, rim, own_gi, got_gi, own_st, got_st, conv_inner, conv_state, small,
    values, in_map, out_map, within, until, step, entering, packet,
    pad_i, pad_s, rate, carry, passed,
):
    c = pos[2]
    pad_i[:8] = rim[:, :CH]
    pad_s[:8] = rim[:, CH:]
    for which, gi, st in ((c, own_gi, own_st), (1 - c, got_gi, got_st)):
        rows = pl.ds(pl.multiple_of(8 + which * HALF, 8), HALF)
        pad_i[rows] = gi[:, CH:].astype(F32)
        pad_s[rows] = st[:, : 2 * N]
        tail = st[:, 2 * N :]
        rate[half(which)] = tail if st is own_st else pltpu.roll(tail, N - HEADS, 1)
    lane = lax.broadcasted_iota(jnp.int32, (Q, N), 1)
    lower = (
        lax.broadcasted_iota(jnp.int32, (Q, Q), 0) >= lax.broadcasted_iota(jnp.int32, (Q, Q), 1)
    ).astype(F32)
    carry[...] = jnp.zeros((N, CH), F32)
    passed[...] = jnp.zeros((8, N), F32)

    def chunk(i, _):
        rows = pl.ds(pl.multiple_of(i * Q, Q), Q)
        window = pl.ds(pl.multiple_of(i * Q, Q), Q + 8)
        wi, ws = pad_i[window], pad_s[window]
        vi = jnp.zeros((Q, CH), F32)
        vs = jnp.zeros((Q, CH), F32)
        for k in range(K):
            vi = vi + conv_inner[k : k + 1] * wi[5 + k : 5 + k + Q]
            vs = vs + conv_state[k : k + 1] * ws[5 + k : 5 + k + Q]
        vi = silu(vi)
        vs = silu(vs)
        values[rows] = vi
        b = vs[:, :N].astype(BF16)
        in_map[rows] = b
        out_map[rows] = vs[:, N:].astype(BF16)
        v = rate[rows] + small[0:1]
        soft = jnp.maximum(v, 0.0) + jnp.log1p(jnp.exp(-jnp.abs(v)))
        steps = jnp.where(lane < HEADS, soft, 0.0)
        step[rows] = steps
        w = dot(lower, steps * small[1:2], HIGH)
        within[rows] = w
        before = passed[:1]
        until[rows] = w + before
        last = w[Q - 1 : Q]
        scaled = (vi * widen(jnp.exp(last - w) * steps, Q)).astype(BF16)
        block = lax.dot_general(b, scaled, (((0,), (0,)), ((), ())), preferred_element_type=F32)
        old = carry[...]
        entering[i] = old.astype(BF16)
        carry[...] = widen(jnp.exp(last), 1) * old + block
        passed[:1] = before + last
        return 0

    lax.fori_loop(0, CHUNKS, chunk, 0)
    total = widen(passed[:1], 1)
    high = total.astype(BF16)
    low = (total - high.astype(F32)).astype(BF16)
    packet[:N] = carry[...].astype(BF16)
    packet[N:] = jnp.concatenate([high, low, jnp.zeros((14, CH), BF16)], axis=0)


def scan(pos, *parts):
    outs = (
        shape((ROWS, CH)),
        shape((ROWS, N), BF16),
        shape((ROWS, N), BF16),
        shape((ROWS, N)),
        shape((ROWS, N)),
        shape((ROWS, N)),
        shape((CHUNKS, N, CH), BF16),
        shape((N + 16, CH), BF16),
    )
    scratch = (
        pltpu.VMEM((ROWS + 8, CH), F32),
        pltpu.VMEM((ROWS + 8, CH), F32),
        pltpu.VMEM((ROWS, N), F32),
        pltpu.VMEM((N, CH), F32),
        pltpu.VMEM((8, N), F32),
    )
    return kernel(scan_body, outs, 9, 1, scratch)(pos, *parts)


def inside_body(pos, own_gi, got_gi, values, in_map, out_map, within, step, entering, small, result, opened, gate):
    c = pos[2]
    skip = widen(small[2:3], 1)
    gate[half(c)] = own_gi[:, :CH]
    gate[half(1 - c)] = got_gi[:, :CH]
    lower = lax.broadcasted_iota(jnp.int32, (Q, Q), 0) >= lax.broadcasted_iota(jnp.int32, (Q, Q), 1)

    def chunk(i, _):
        rows = pl.ds(pl.multiple_of(i * Q, Q), Q)
        opened[rows] = silu(gate[rows].astype(F32))
        b, out, w, vi = in_map[rows], out_map[rows], within[rows], values[rows]
        scores = lax.dot_general(out, b, (((1,), (1,)), ((), ())), preferred_element_type=F32)
        flat = w.T
        stepped = (vi * widen(step[rows], Q)).astype(BF16)
        parts = []
        for h in range(HEADS):
            gap = w[:, h : h + 1] - flat[h : h + 1]
            mixing = (scores * jnp.exp(jnp.where(lower, gap, -jnp.inf))).astype(BF16)
            parts.append(dot(mixing, stepped[:, h * P_SIZE : (h + 1) * P_SIZE]))
        local = jnp.concatenate(parts, axis=1)
        local = local + dot(out, entering[i]) * widen(jnp.exp(w), Q)
        result[rows] = local + skip * vi
        return 0

    lax.fori_loop(0, CHUNKS, chunk, 0)


def inside(pos, *parts):
    outs = (shape((ROWS, CH)), shape((ROWS, CH)))
    scratch = (pltpu.VMEM((ROWS, CH), BF16),)
    return kernel(inside_body, outs, 10, 1, scratch)(pos, *parts)


def split(energy):
    high = energy.astype(BF16)
    return high, (energy - high.astype(F32)).astype(BF16)


def gated_body(pos, p1, p2, p3, p4, p5, p6, p7, local, out_map, until, opened, gate_gain, own, send, energy):
    c = pos[2]
    carried = jnp.zeros((N, CH), F32)
    log = jnp.zeros((1, CH), F32)
    for p in (p1, p2, p3, p4, p5, p6, p7):
        carried = carried + jnp.exp(log) * p[:N].astype(F32)
        tail = p[N:].astype(F32)
        log = log + (tail[0:1] + tail[1:2])
    carried = carried.astype(BF16)
    for which, to in ((1 - c, send), (c, own)):
        rows = half(which)
        out = local[rows] + dot(out_map[rows], carried) * widen(jnp.exp(until[rows]), HALF)
        out = out * opened[rows]
        to[:HALF] = (out * gate_gain[...]).astype(BF16)
        e = as_rows(jnp.sum(out * out, axis=1, keepdims=True))
        if to is own:
            energy[...] = jnp.concatenate([e, jnp.zeros((4, N), F32)], axis=0)
        else:
            e = jnp.concatenate(split(e), axis=1)
            to[HALF:] = jnp.concatenate([e, jnp.zeros((12, CH), BF16)], axis=0)


def gated(pos, *parts):
    outs = (shape((HALF, CH), BF16), shape((HALF + 16, CH), BF16), shape((8, N)))
    return kernel(gated_body, outs, 13, 1)(pos, *parts)


TALL = 2 * HALF + 16


def energy_rows(energy):
    return jnp.concatenate([*split(energy), jnp.zeros((8, N), BF16)], axis=0)


def stack_body(own, got, out):
    out[:CH] = own[...]
    out[CH:] = got[...]


def pair_energy(got, energy):
    tail = got[HALF:].astype(F32)
    return energy[:4] + (tail[:4, :N] + tail[:4, N:])


def product(pos, own, got, weights, s, t):
    first = pos[2] == 0
    dy = jnp.where(first, t, s)
    dx = jnp.where(first, s, t)
    chip = ((pos[0] + dy) & 3) * 4 + ((pos[1] + dx) & 3)
    cols = pl.ds(pl.multiple_of(chip * 2 * N, 2 * N), 2 * N)
    return dot(jnp.concatenate([own[...], got[:HALF]], axis=1), weights[:, cols])


def spread_body(specs, adds):
    def body(pos, own, got, energy, weights, *refs):
        extra, outs = refs[:adds], refs[adds:]
        for n, (s, pair) in enumerate(specs):
            tail = pair_energy(got, energy)
            if adds:
                rows = extra[n][0, 2 * HALF :].astype(F32)
                tail = tail + (rows[:4] + rows[4:8])
            tail = energy_rows(tail)
            for k, t in enumerate(pair):
                part = product(pos, own, got, weights, s, t)
                for side in range(2):
                    rows = slice(side * HALF, (side + 1) * HALF)
                    value = part[:, side * N : (side + 1) * N]
                    if adds:
                        value = value + extra[n][k, rows].astype(F32)
                    outs[n][k, rows] = value.astype(BF16)
                outs[n][k, 2 * HALF :] = tail

    return body


def spread(pos, specs, parts, extra=()):
    outs = tuple(shape((2, TALL, N), BF16) for _ in specs)
    count = len(extra)
    flops = 2 * HALF * 512 * 512 * len(specs)
    return kernel(spread_body(specs, count), outs, 5 + count, 1, (), flops)(pos, *parts, *extra)


def keep_body(pos, own, got, energy, weights, out, tail):
    for t in range(4):
        part = product(pos, own, got, weights, 0, t)
        out[t, :HALF] = part[:, :N]
        out[t, HALF:] = part[:, N:]
    tail[...] = jnp.concatenate([pair_energy(got, energy), jnp.zeros((4, N), F32)], axis=0)


def half_sum_body(own, tail, u_plus, d_minus, d_plus, u_minus, q0, q1, q2, q3):
    for t, q in enumerate((q0, q1, q2, q3)):
        x, y = ((u_plus, d_minus), (d_plus, u_minus))[t // 2]
        k = t % 2
        value = own[t] + x[k, : 2 * HALF].astype(F32) + y[k, : 2 * HALF].astype(F32)
        q[: 2 * HALF] = value.astype(q.dtype)
        e = x[k, 2 * HALF :].astype(F32) + y[k, 2 * HALF :].astype(F32)
        e = tail[:4] + (e[:4] + e[4:8])
        if q.dtype == BF16:
            q[2 * HALF :] = energy_rows(e)
        else:
            q[2 * HALF :] = jnp.concatenate([e, jnp.zeros((12, N), F32)], axis=0)


def half_sum(*parts):
    outs = (shape((TALL, N)),) + (shape((TALL, N), BF16),) * 3
    return kernel(half_sum_body, outs, 6)(*parts)


def total_body(pos, v0, v1, v2, v3, own, send):
    c = pos[2]
    e = v0[2 * HALF :] + v1[2 * HALF :].astype(F32) + v2[2 * HALF :].astype(F32) + v3[2 * HALF :].astype(F32)
    scale = lax.rsqrt(as_column(e[:4] + e[4:8]) / DI + EPS)
    for which, to in ((1 - c, send), (c, own)):
        rows = half(which)
        to[...] = (v0[rows] + v1[rows].astype(F32) + v2[rows].astype(F32) + v3[rows].astype(F32)) * scale


def total(pos, *parts):
    return kernel(total_body, (shape((HALF, N)), shape((HALF, N))), 5, 1)(pos, *parts)


def finish_body(pos, tokens, own, got, out):
    c = pos[2]
    for which, part in ((c, own), (1 - c, got)):
        rows = half(which)
        out[rows] = (tokens[rows].astype(F32) + part[...]).astype(BF16)


def finish(pos, *parts):
    return kernel(finish_body, shape((ROWS, N), BF16), 4, 1, place=False)(pos, *parts)


def local(
    tokens,
    norm_gain,
    gate_proj,
    inner_proj,
    state_proj,
    conv_inner,
    conv_state,
    log_rate,
    rate_bias,
    skip_gain,
    gate_gain,
    out_proj,
):
    ci = lax.axis_index("chan")
    core = ci & 1
    pos = jnp.stack([ci >> 3, (ci >> 1) & 3, core, ci]).astype(jnp.int32)
    gain = norm_gain.reshape(32, N)

    small = jnp.pad(jnp.stack([rate_bias, -jnp.exp(log_rate), skip_gain]), ((0, 5), (0, N - HEADS)))

    away_tokens = swap(tokens)
    make_block = kernel(block_body, shape((BLOCK, N), BF16), 5, 1, inputs=pltpu.HBM)
    block = make_block(pos, tokens, away_tokens, state_proj, gain)

    near1, near3 = plane_move(block, 1, 0), plane_move(block, -1, 0)
    near_low = plane_move(near1[: BLOCK // 2], 1, 0)
    near_high = plane_move(near3[BLOCK // 2 :], -1, 0)
    a0 = jnp.stack([block, near1])
    a1 = jnp.concatenate([near_low, near_high, near3], axis=0).reshape(2, BLOCK, N)
    near_mark = mark(a0)
    b0, d1 = plane_move(a0, 1, 1), plane_move(a1, -1, 1)
    b1, d0 = plane_move(a1, 1, 1), plane_move(a0, -1, 1)
    far_mark = mark(b0)
    c0, c1 = plane_move(b0, 1, 1), plane_move(d1, -1, 1)

    keep = kernel(scale_body, shape((D, 2 * CH), BF16), 3)(gate_proj, inner_proj, gain)
    got = swap(keep)
    got_w = swap(out_proj)

    most_own = pick(a0, a1, b0, b1, d0, d1, marks=(near_mark, far_mark))
    most_got = swap(most_own)
    acc, squares = most(pos, a0, a1, b0, b1, d0, d1, keep, got)
    acc_st = state_most(pos, a0, a1, b0, b1, d0, d1, most_own, most_got)
    w_all = kernel(stack_body, shape((2 * CH, D), BF16), 2)(out_proj, got_w)
    last_own = pick(c0, c1)
    last_got = swap(last_own)
    own_gi, send_gi, scale = rest(pos, c0, c1, keep, got, acc, squares)
    got_gi = swap(send_gi)
    own_st = state_rest(pos, a1, b1, d1, c0, c1, most_own, most_got, last_own, last_got, acc_st, scale)
    got_st = swap(own_st)

    edge = jnp.where(core == 1, own_gi[-8:, CH:], got_gi[-8:, CH:]).astype(F32)
    edge_st = jnp.where(core == 1, own_st[-8:, : 2 * N], got_st[-8:, : 2 * N])
    rim = later(jnp.concatenate([edge, edge_st], axis=1), 1)

    values, in_map, out_map, within, until, step, entering, packet = scan(
        pos, rim, own_gi, got_gi, own_st, got_st, conv_inner, conv_state, small
    )
    packets = {s: later(packet, s) for s in (3, 7, 2, 6, 1, 5)}
    packets[4] = later(packets[3], 1)
    packets = [packets[s] for s in range(1, 8)]
    result, opened = inside(pos, own_gi, got_gi, values, in_map, out_map, within, step, entering, small)
    own_g, send_g, energy = gated(pos, *packets, result, out_map, until, opened, gate_gain[None])

    got_g = swap(send_g)
    parts = (own_g, got_g, energy, w_all)
    far_low, far_high = spread(pos, ((2, (0, 1)), (2, (2, 3))), parts)
    t_plus, t_minus = plane_move(far_low, 1, 0), plane_move(far_high, -1, 0)
    near_plus, near_minus = spread(pos, ((1, (2, 3)), (3, (0, 1))), parts)
    d_plus, d_minus = plane_move(near_plus, 1, 0), plane_move(near_minus, -1, 0)
    keep_outs = (shape((4, 2 * HALF, N)), shape((8, N)))
    kept, tail = kernel(keep_body, keep_outs, 5, 1, (), 2 * HALF * 512 * 1024)(pos, *parts)
    (on_plus,) = spread(pos, ((1, (0, 1)),), parts, (t_plus,))
    u_plus = plane_move(on_plus, 1, 0)
    (on_minus,) = spread(pos, ((3, (2, 3)),), parts, (t_minus,))
    u_minus = plane_move(on_minus, -1, 0)
    q = half_sum(kept, tail, u_plus, d_minus, d_plus, u_minus)
    last = [q[0]] + [plane_move(q[t], t, 1) for t in (1, 2, 3)]
    own, send = total(pos, *last)
    return finish(pos, tokens, own, swap(send))


def solution(mesh):
    return jax.shard_map(
        local,
        mesh=mesh,
        in_specs=(
            P("seq", "chan"),
            P(),
            P(None, "chan"),
            P(None, "chan"),
            P("chan", None),
            P(None, "chan"),
            P(),
            P("chan"),
            P("chan"),
            P("chan"),
            P("chan"),
            P("chan", None),
        ),
        out_specs=P("seq", "chan"),
        check_vma=False,
    )
```

```python
import jax
import jax.numpy as jnp
from jax import lax
from jax.experimental import pallas as pl
from jax.experimental.pallas import tpu as pltpu
from jax.sharding import PartitionSpec as P


D = 4096
DI = 8192
N = 128
P_SIZE = 64
K = 4
Q = 256
ROWS = 1024
HALF = 512
CHUNKS = 4
HEADS = 4
CH = 256
EPS = 1e-05
F32 = jnp.float32
BF16 = jnp.bfloat16
HIGH = lax.Precision.HIGHEST


def plane_move(value, steps, phase):
    pairs = []
    for y in range(4):
        for x in range(4):
            for c in range(2):
                dy, dx = (0, steps) if c == phase else (steps, 0)
                pairs.append(((y * 4 + x) * 2 + c, ((y + dy) % 4 * 4 + (x + dx) % 4) * 2 + c))
    return lax.ppermute(value, "chan", pairs)


def swap(value):
    return lax.ppermute(value, "chan", [(i, i ^ 1) for i in range(32)])


def later(value, steps):
    return lax.ppermute(value, "seq", [(i, i + steps) for i in range(8 - steps)])


def kernel(body, outs, n_in, smem=0, scratch=(), flops=0, place=True, inputs=None):
    inner = pl.pallas_call(
        body,
        out_shape=jax.tree.map(lambda o: pltpu.VMEM(o.shape, o.dtype), outs) if place else outs,
        in_specs=[pl.BlockSpec(memory_space=pltpu.SMEM)] * smem + [pl.BlockSpec(memory_space=pltpu.VMEM)] * (n_in - smem),
        out_specs=jax.tree.map(lambda _: pl.BlockSpec(memory_space=pltpu.VMEM), outs),
        scratch_shapes=list(scratch),
        compiler_params=pltpu.CompilerParams(vmem_limit_bytes=16 * 1024 * 1024),
        cost_estimate=pl.CostEstimate(flops=flops, transcendentals=0, bytes_accessed=1 << 20),
    )

    def call(*args):
        spaces = inputs or (pltpu.VMEM,) * (n_in - smem)
        placed = [pltpu.with_memory_space_constraint(a, m) if m else a for a, m in zip(args[smem:], spaces)]
        return inner(*args[:smem], *placed)

    return call


def shape(dims, kind=F32):
    return jax.ShapeDtypeStruct(dims, kind)


def dot(a, b, precision=None):
    return jnp.dot(a, b, preferred_element_type=F32, precision=precision)


def eye(n):
    return lax.broadcasted_iota(jnp.int32, (n, n), 0) == lax.broadcasted_iota(jnp.int32, (n, n), 1)


def stand(row):
    return jnp.sum(jnp.where(eye(N), jnp.broadcast_to(row, (N, N)), 0.0), axis=1, keepdims=True)


def lay(column):
    return jnp.sum(jnp.where(eye(N), jnp.broadcast_to(column, (N, N)), 0.0), axis=0, keepdims=True)


def as_rows(column):
    return jnp.concatenate([lay(column[i * N : (i + 1) * N]) for i in range(4)], axis=0)


def as_column(rows):
    return jnp.concatenate([stand(rows[i : i + 1]) for i in range(4)], axis=0)


def half(index):
    return pl.ds(pl.multiple_of(index * HALF, HALF), HALF)


BLOCK = 2 * HALF + 3 * N


def block_body(pos, tokens, away, state_w, gain, out):
    c, ci = pos[2], pos[3]
    out[half(c)] = tokens[half(c)]
    out[half(1 - c)] = away[half(c)]
    scaled = (state_w[...].astype(F32) * stand(gain[pl.ds(ci, 1)])).astype(BF16)
    for b in range(3):
        out[2 * HALF + b * N : 2 * HALF + (b + 1) * N] = scaled[:, b * N : (b + 1) * N]


def scale_body(gate, inner, gain, out):
    def step(i, _):
        rows = pl.ds(pl.multiple_of(i * N, N), N)
        column = stand(gain[pl.ds(i, 1)])
        out[rows, :CH] = (gate[rows].astype(F32) * column).astype(BF16)
        out[rows, CH:] = (inner[rows].astype(F32) * column).astype(BF16)
        return 0

    lax.fori_loop(0, 2 * 16, step, 0, unroll=4)


def mark_body(ref, out):
    out[...] = ref[:16]


def mark(piece):
    return kernel(mark_body, shape((16, N), BF16), 1)(piece)


def blocks_of(refs):
    found = []
    for ref in refs:
        found += [ref] if len(ref.shape) == 2 else [ref.at[0], ref.at[1]]
    return found


def pick_body(count):
    def body(*refs):
        for i, ref in enumerate(blocks_of(refs[:count])):
            refs[-1][i] = ref[2 * HALF :]

    return body


def pick(*pieces, marks=()):
    blocks = sum(1 if p.ndim == 2 else 2 for p in pieces)
    out = shape((blocks, 3 * N, N), BF16)
    return kernel(pick_body(len(pieces)), out, len(pieces) + len(marks))(*pieces, *marks)


def owner(pos, s, t):
    first = pos[2] == 0
    dy = jnp.where(first, s, t)
    dx = jnp.where(first, t, s)
    return ((pos[0] - dy) & 3) * 4 + ((pos[1] - dx) & 3)


STEP = 256


def add_slots(pos, slots, keep, got, acc, squares, fresh):
    def rows_of(r, _):
        rows = pl.ds(pl.multiple_of(r * STEP, STEP), STEP)
        low = pl.ds(pl.multiple_of(r * STEP, STEP), STEP)
        high = pl.ds(pl.multiple_of(HALF + r * STEP, STEP), STEP)
        square = None if fresh else squares[rows]
        for n, (s, blocks) in enumerate(slots):
            parts = []
            for ref in blocks:
                parts += [ref[low], ref[high]]
            for v in parts:
                v = v.astype(F32)
                square = v * v if square is None else square + v * v
            lhs = jnp.concatenate(parts, axis=1)
            ids = [pl.ds(pl.multiple_of(owner(pos, s, t) * 2 * N, 2 * N), 2 * N) for t in range(4)]
            for w, ref in enumerate((keep, got)):
                for b in range(2):
                    cols = slice(w * 2 * CH + b * CH, w * 2 * CH + (b + 1) * CH)
                    rhs = jnp.concatenate([ref[i, b * CH : (b + 1) * CH] for i in ids], axis=0)
                    part = dot(lhs, rhs)
                    if fresh and n == 0:
                        acc[rows, cols] = part
                    else:
                        acc[rows, cols] += part
        squares[rows] = square
        return 0

    lax.fori_loop(0, HALF // STEP, rows_of, 0)


def most_body(pos, *refs):
    blocks, (keep, got, acc, squares) = blocks_of(refs[:-4]), refs[-4:]
    slots = ((0, blocks[:4]), (1, blocks[4:8]), (3, blocks[8:]))
    add_slots(pos, slots, keep, got, acc, squares, True)


def most(pos, *parts):
    outs = (shape((HALF, 4 * CH)), shape((HALF, N)))
    return kernel(most_body, outs, len(parts) + 1, 1, (), 2 * HALF * 3072 * 1024)(pos, *parts)


def rest_body(pos, c0, c1, keep, got, acc, squares, own, send, scale):
    blocks = blocks_of((c0, c1))

    def rows_of(r, _):
        rows = pl.ds(pl.multiple_of(r * STEP, STEP), STEP)
        high = pl.ds(pl.multiple_of(HALF + r * STEP, STEP), STEP)
        square = squares[rows]
        parts = []
        for ref in blocks:
            parts += [ref[rows], ref[high]]
        for v in parts:
            v = v.astype(F32)
            square = square + v * v
        inverse = lax.rsqrt(jnp.sum(square, axis=1, keepdims=True) / D + EPS)
        scale[rows] = jnp.broadcast_to(inverse, (STEP, N))
        lhs = jnp.concatenate(parts, axis=1)
        ids = [pl.ds(pl.multiple_of(owner(pos, 2, t) * 2 * N, 2 * N), 2 * N) for t in range(4)]
        for w, (ref, out) in enumerate(((keep, own), (got, send))):
            for b in range(2):
                cols = slice(b * CH, (b + 1) * CH)
                rhs = jnp.concatenate([ref[i, cols] for i in ids], axis=0)
                part = acc[rows, w * 2 * CH + b * CH : w * 2 * CH + (b + 1) * CH] + dot(lhs, rhs)
                out[rows, cols] = (part * inverse).astype(BF16)
        return 0

    lax.fori_loop(0, HALF // STEP, rows_of, 0)


def rest(pos, *parts):
    outs = (shape((HALF, 2 * CH), BF16), shape((HALF, 2 * CH), BF16), shape((HALF, N)))
    return kernel(rest_body, outs, 7, 1, (), 2 * HALF * 1024 * 1024)(pos, *parts)


ORDER = (0, 1, 3, 2)


def state_sum(pos, blocks, most_own, most_got, last_own, last_got, slots, finish):
    c = pos[2]

    def rows_of(r, _):
        mine = pl.ds(pl.multiple_of(c * HALF + r * STEP, STEP), STEP)
        other = pl.ds(pl.multiple_of((1 - c) * HALF + r * STEP, STEP), STEP)
        lhs, w = [], [[], [], []]
        for g, k in slots:
            i = 4 * g + k
            lhs += [blocks[i][mine], blocks[i][other]]
            j = 4 * ORDER.index(k) + ORDER[g]
            for b in range(3):
                cut = slice(b * N, (b + 1) * N)
                w[b].append(most_own[i, cut] if i < 12 else last_own[i - 12, cut])
                w[b].append(most_got[j, cut] if j < 12 else last_got[j - 12, cut])
        lhs = jnp.concatenate(lhs, axis=1)
        w = [jnp.concatenate(v, axis=0) for v in w]
        finish(r, dot(lhs, jnp.concatenate(w[:2], axis=1)), dot(lhs, w[2]))
        return 0

    lax.fori_loop(0, HALF // STEP, rows_of, 0)


EARLY = [(g, k) for g in range(3) for k in (0, 1, 3)]
LATE = [(g, 2) for g in range(3)] + [(3, k) for k in range(4)]


def state_most_body(pos, *refs):
    blocks, (most_own, most_got, out) = blocks_of(refs[:-3]), refs[-3:]

    def finish(r, left, right):
        rows = pl.ds(pl.multiple_of(r * STEP, STEP), STEP)
        out[rows, : 2 * N] = left
        out[rows, 2 * N :] = right

    state_sum(pos, blocks, most_own, most_got, None, None, EARLY, finish)


def state_most(pos, *parts):
    call = kernel(state_most_body, shape((HALF, 3 * N)), len(parts) + 1, 1, (), 2 * HALF * 2304 * 384)
    return call(pos, *parts)


def state_body(pos, a23, p23, m2, c0, c1, most_own, most_got, last_own, last_got, acc, scale, out):
    ci = pos[3]

    def finish(r, left, right):
        rows = pl.ds(pl.multiple_of(r * STEP, STEP), STEP)
        inverse = scale[rows]
        out[rows, :N] = (acc[rows, :N] + left[:, :N]) * inverse
        out[rows, N : 2 * N] = (acc[rows, N : 2 * N] + left[:, N:]) * inverse
        rates = (acc[rows, 2 * N :] + right) * inverse
        lane = lax.broadcasted_iota(jnp.int32, (STEP, N), 1)
        own_rate = pltpu.roll(rates, (N - ci * HEADS) & (N - 1), 1)
        away_rate = pltpu.roll(rates, (N + HEADS - (ci ^ 1) * HEADS) & (N - 1), 1)
        out[rows, 2 * N :] = jnp.where(lane < HEADS, own_rate, away_rate)

    late = [None] * 12 + blocks_of((c0, c1))
    late[2], late[6], late[10] = a23.at[0], p23.at[0], m2
    state_sum(pos, late, most_own, most_got, last_own, last_got, LATE, finish)


def state_rest(pos, *parts):
    return kernel(state_body, shape((HALF, 3 * N)), 12, 1, (), 2 * HALF * 1792 * 384)(pos, *parts)


def silu(v):
    return v / (1.0 + jnp.exp(-v))


def widen(columns, rows):
    return jnp.concatenate(
        [jnp.broadcast_to(columns[:, h : h + 1], (rows, P_SIZE)) for h in range(HEADS)], axis=1
    )


def scan_body(
    pos, rim, own_gi, got_gi, own_st, got_st, conv_inner, conv_state, small,
    values, in_map, out_map, within, until, step, entering, packet,
    pad_i, pad_s, rate, carry, passed,
):
    c = pos[2]
    pad_i[:8] = rim[:, :CH]
    pad_s[:8] = rim[:, CH:]
    for which, gi, st in ((c, own_gi, own_st), (1 - c, got_gi, got_st)):
        rows = pl.ds(pl.multiple_of(8 + which * HALF, 8), HALF)
        pad_i[rows] = gi[:, CH:].astype(F32)
        pad_s[rows] = st[:, : 2 * N]
        tail = st[:, 2 * N :]
        rate[half(which)] = tail if st is own_st else pltpu.roll(tail, N - HEADS, 1)
    lane = lax.broadcasted_iota(jnp.int32, (Q, N), 1)
    lower = (
        lax.broadcasted_iota(jnp.int32, (Q, Q), 0) >= lax.broadcasted_iota(jnp.int32, (Q, Q), 1)
    ).astype(F32)
    carry[...] = jnp.zeros((N, CH), F32)
    passed[...] = jnp.zeros((8, N), F32)

    def chunk(i, _):
        rows = pl.ds(pl.multiple_of(i * Q, Q), Q)
        window = pl.ds(pl.multiple_of(i * Q, Q), Q + 8)
        wi, ws = pad_i[window], pad_s[window]
        vi = jnp.zeros((Q, CH), F32)
        vs = jnp.zeros((Q, CH), F32)
        for k in range(K):
            vi = vi + conv_inner[k : k + 1] * wi[5 + k : 5 + k + Q]
            vs = vs + conv_state[k : k + 1] * ws[5 + k : 5 + k + Q]
        vi = silu(vi)
        vs = silu(vs)
        values[rows] = vi
        b = vs[:, :N].astype(BF16)
        in_map[rows] = b
        out_map[rows] = vs[:, N:].astype(BF16)
        v = rate[rows] + small[0:1]
        soft = jnp.maximum(v, 0.0) + jnp.log1p(jnp.exp(-jnp.abs(v)))
        steps = jnp.where(lane < HEADS, soft, 0.0)
        step[rows] = steps
        w = dot(lower, steps * small[1:2], HIGH)
        within[rows] = w
        before = passed[:1]
        until[rows] = w + before
        last = w[Q - 1 : Q]
        scaled = (vi * widen(jnp.exp(last - w) * steps, Q)).astype(BF16)
        block = lax.dot_general(b, scaled, (((0,), (0,)), ((), ())), preferred_element_type=F32)
        old = carry[...]
        entering[i] = old.astype(BF16)
        carry[...] = widen(jnp.exp(last), 1) * old + block
        passed[:1] = before + last
        return 0

    lax.fori_loop(0, CHUNKS, chunk, 0)
    total = widen(passed[:1], 1)
    high = total.astype(BF16)
    low = (total - high.astype(F32)).astype(BF16)
    packet[:N] = carry[...].astype(BF16)
    packet[N:] = jnp.concatenate([high, low, jnp.zeros((14, CH), BF16)], axis=0)


def scan(pos, *parts):
    outs = (
        shape((ROWS, CH)),
        shape((ROWS, N), BF16),
        shape((ROWS, N), BF16),
        shape((ROWS, N)),
        shape((ROWS, N)),
        shape((ROWS, N)),
        shape((CHUNKS, N, CH), BF16),
        shape((N + 16, CH), BF16),
    )
    scratch = (
        pltpu.VMEM((ROWS + 8, CH), F32),
        pltpu.VMEM((ROWS + 8, CH), F32),
        pltpu.VMEM((ROWS, N), F32),
        pltpu.VMEM((N, CH), F32),
        pltpu.VMEM((8, N), F32),
    )
    return kernel(scan_body, outs, 9, 1, scratch)(pos, *parts)


def inside_body(h):
    def body(pos, own_gi, got_gi, values, in_map, out_map, within, step, entering, small, result, opened):
        own_half = pos[2] == h
        skip = widen(small[2:3], 1)
        lower = lax.broadcasted_iota(jnp.int32, (Q, Q), 0) >= lax.broadcasted_iota(jnp.int32, (Q, Q), 1)

        def chunk(i, _):
            here = pl.ds(pl.multiple_of(i * Q, Q), Q)
            rows = pl.ds(pl.multiple_of(h * HALF + i * Q, Q), Q)
            gate = jnp.where(own_half, own_gi[here, :CH].astype(F32), got_gi[here, :CH].astype(F32))
            opened[here] = silu(gate)
            b, out, w, vi = in_map[rows], out_map[rows], within[rows], values[rows]
            scores = lax.dot_general(out, b, (((1,), (1,)), ((), ())), preferred_element_type=F32)
            flat = w.T
            stepped = (vi * widen(step[rows], Q)).astype(BF16)
            parts = []
            for k in range(HEADS):
                gap = w[:, k : k + 1] - flat[k : k + 1]
                mixing = (scores * jnp.exp(jnp.where(lower, gap, -jnp.inf))).astype(BF16)
                parts.append(dot(mixing, stepped[:, k * P_SIZE : (k + 1) * P_SIZE]))
            local = jnp.concatenate(parts, axis=1)
            local = local + dot(out, entering[2 * h + i]) * widen(jnp.exp(w), Q)
            result[here] = local + skip * vi
            return 0

        lax.fori_loop(0, 2, chunk, 0)

    return body


def inside(h, pos, *parts):
    outs = (shape((HALF, CH)), shape((HALF, CH)))
    return kernel(inside_body(h), outs, 10, 1)(pos, *parts)


def edge_body(pos, own_gi, got_gi, own_st, got_st, out):
    second = pos[2] == 1
    last = slice(HALF - 16, HALF)
    inner = jnp.where(second, own_gi[last, CH:].astype(F32), got_gi[last, CH:].astype(F32))
    out[:, :CH] = inner[8:]
    out[:, CH:] = jnp.where(second, own_st[HALF - 8 :, : 2 * N], got_st[HALF - 8 :, : 2 * N])


def split(energy):
    high = energy.astype(BF16)
    return high, (energy - high.astype(F32)).astype(BF16)


def gated_body(pos, p1, p2, p3, p4, p5, p6, p7, r0, o0, r1, o1, out_map, until, gate_gain, own, send, energy):
    c = pos[2]
    zero = c == 0
    carried = jnp.zeros((N, CH), F32)
    log = jnp.zeros((1, CH), F32)
    for p in (p1, p2, p3, p4, p5, p6, p7):
        carried = carried + jnp.exp(log) * p[:N].astype(F32)
        tail = p[N:].astype(F32)
        log = log + (tail[0:1] + tail[1:2])
    carried = carried.astype(BF16)
    for which, to in ((1 - c, send), (c, own)):
        rows = half(which)
        lower = zero if to is own else jnp.logical_not(zero)
        out = jnp.where(lower, r0[...], r1[...]) + dot(out_map[rows], carried) * widen(jnp.exp(until[rows]), HALF)
        out = out * jnp.where(lower, o0[...], o1[...])
        to[:HALF] = (out * gate_gain[...]).astype(BF16)
        e = as_rows(jnp.sum(out * out, axis=1, keepdims=True))
        if to is own:
            energy[...] = jnp.concatenate([e, jnp.zeros((4, N), F32)], axis=0)
        else:
            e = jnp.concatenate(split(e), axis=1)
            to[HALF:] = jnp.concatenate([e, jnp.zeros((12, CH), BF16)], axis=0)


def gated(pos, *parts):
    outs = (shape((HALF, CH), BF16), shape((HALF + 16, CH), BF16), shape((8, N)))
    return kernel(gated_body, outs, 15, 1)(pos, *parts)


TALL = 2 * HALF + 16


def energy_rows(energy):
    return jnp.concatenate([*split(energy), jnp.zeros((8, N), BF16)], axis=0)


def stack_body(own, got, out):
    out[:CH] = own[...]
    out[CH:] = got[...]


def pair_energy(got, energy):
    tail = got[HALF:].astype(F32)
    return energy[:4] + (tail[:4, :N] + tail[:4, N:])


def product(pos, own, got, weights, s, t):
    first = pos[2] == 0
    dy = jnp.where(first, t, s)
    dx = jnp.where(first, s, t)
    chip = ((pos[0] + dy) & 3) * 4 + ((pos[1] + dx) & 3)
    cols = pl.ds(pl.multiple_of(chip * 2 * N, 2 * N), 2 * N)
    return dot(jnp.concatenate([own[...], got[:HALF]], axis=1), weights[:, cols])


def spread_body(specs, adds):
    def body(pos, own, got, energy, weights, *refs):
        extra, outs = refs[:adds], refs[adds:]
        for n, (s, pair) in enumerate(specs):
            tail = pair_energy(got, energy)
            if adds:
                rows = extra[n][0, 2 * HALF :].astype(F32)
                tail = tail + (rows[:4] + rows[4:8])
            tail = energy_rows(tail)
            for k, t in enumerate(pair):
                part = product(pos, own, got, weights, s, t)
                for side in range(2):
                    rows = slice(side * HALF, (side + 1) * HALF)
                    value = part[:, side * N : (side + 1) * N]
                    if adds:
                        value = value + extra[n][k, rows].astype(F32)
                    outs[n][k, rows] = value.astype(BF16)
                outs[n][k, 2 * HALF :] = tail

    return body


def spread(pos, specs, parts, extra=()):
    outs = tuple(shape((2, TALL, N), BF16) for _ in specs)
    count = len(extra)
    flops = 2 * HALF * 512 * 512 * len(specs)
    return kernel(spread_body(specs, count), outs, 5 + count, 1, (), flops)(pos, *parts, *extra)


def keep_body(pos, own, got, energy, weights, out, tail):
    for t in range(4):
        part = product(pos, own, got, weights, 0, t)
        out[t, :HALF] = part[:, :N]
        out[t, HALF:] = part[:, N:]
    tail[...] = jnp.concatenate([pair_energy(got, energy), jnp.zeros((4, N), F32)], axis=0)


def half_sum_body(own, tail, u_plus, d_minus, d_plus, u_minus, q0, q1, q2, q3):
    for t, q in enumerate((q0, q1, q2, q3)):
        x, y = ((u_plus, d_minus), (d_plus, u_minus))[t // 2]
        k = t % 2
        value = own[t] + x[k, : 2 * HALF].astype(F32) + y[k, : 2 * HALF].astype(F32)
        q[: 2 * HALF] = value.astype(q.dtype)
        e = x[k, 2 * HALF :].astype(F32) + y[k, 2 * HALF :].astype(F32)
        e = tail[:4] + (e[:4] + e[4:8])
        if q.dtype == BF16:
            q[2 * HALF :] = energy_rows(e)
        else:
            q[2 * HALF :] = jnp.concatenate([e, jnp.zeros((12, N), F32)], axis=0)


def half_sum(*parts):
    outs = (shape((TALL, N)),) + (shape((TALL, N), BF16),) * 3
    return kernel(half_sum_body, outs, 6)(*parts)


def total_body(pos, v0, v1, v2, v3, own, send):
    c = pos[2]
    e = v0[2 * HALF :] + v1[2 * HALF :].astype(F32) + v2[2 * HALF :].astype(F32) + v3[2 * HALF :].astype(F32)
    scale = lax.rsqrt(as_column(e[:4] + e[4:8]) / DI + EPS)
    for which, to in ((1 - c, send), (c, own)):
        rows = half(which)
        to[...] = (v0[rows] + v1[rows].astype(F32) + v2[rows].astype(F32) + v3[rows].astype(F32)) * scale


def total(pos, *parts):
    return kernel(total_body, (shape((HALF, N)), shape((HALF, N))), 5, 1)(pos, *parts)


def finish_body(pos, tokens, own, got, out):
    c = pos[2]
    for which, part in ((c, own), (1 - c, got)):
        rows = half(which)
        out[rows] = (tokens[rows].astype(F32) + part[...]).astype(BF16)


def finish(pos, *parts):
    return kernel(finish_body, shape((ROWS, N), BF16), 4, 1, place=False)(pos, *parts)


def local(
    tokens,
    norm_gain,
    gate_proj,
    inner_proj,
    state_proj,
    conv_inner,
    conv_state,
    log_rate,
    rate_bias,
    skip_gain,
    gate_gain,
    out_proj,
):
    ci = lax.axis_index("chan")
    core = ci & 1
    pos = jnp.stack([ci >> 3, (ci >> 1) & 3, core, ci]).astype(jnp.int32)
    gain = norm_gain.reshape(32, N)

    small = jnp.pad(jnp.stack([rate_bias, -jnp.exp(log_rate), skip_gain]), ((0, 5), (0, N - HEADS)))

    away_tokens = swap(tokens)
    spaces = (None, None, pltpu.HBM, pltpu.HBM)
    block = kernel(block_body, shape((BLOCK, N), BF16), 5, 1, inputs=spaces)(pos, tokens, away_tokens, state_proj, gain)

    n1, n3 = plane_move(block, 1, 0), plane_move(block, -1, 0)
    p0, m0 = plane_move(block, 1, 1), plane_move(block, -1, 1)
    p1, m3 = plane_move(n1, 1, 1), plane_move(n3, -1, 1)
    low = plane_move(n1[: BLOCK // 2], 1, 0)
    high = plane_move(n3[BLOCK // 2 :], -1, 0)
    m1 = plane_move(n1, -1, 1)
    n2 = jnp.concatenate([low, high], axis=0)
    a23 = jnp.stack([n2, n3])
    p23, m2 = plane_move(a23, 1, 1), plane_move(n2, -1, 1)
    c0 = plane_move(jnp.stack([p0, p1]), 1, 1)
    c1 = plane_move(jnp.stack([m2, m3]), -1, 1)
    mark1 = mark(p1)
    mark2 = mark(m2)
    early = (block, n1, a23, p0, p1, p23, m0, m1, m2, m3)

    keep = kernel(scale_body, shape((D, 2 * CH), BF16), 3)(gate_proj, inner_proj, gain)
    got = swap(keep)
    got_w = swap(out_proj)

    most_own = pick(*early, marks=(mark1, mark2))
    most_got = swap(most_own)
    acc, squares = most(pos, *early, keep, got)
    acc_st = state_most(pos, *early, most_own, most_got)
    w_all = kernel(stack_body, shape((2 * CH, D), BF16), 2)(out_proj, got_w)
    last_own = pick(c0, c1)
    last_got = swap(last_own)
    own_gi, send_gi, scale = rest(pos, c0, c1, keep, got, acc, squares)
    got_gi = swap(send_gi)
    own_st = state_rest(pos, a23, p23, m2, c0, c1, most_own, most_got, last_own, last_got, acc_st, scale)
    got_st = swap(own_st)

    edge = kernel(edge_body, shape((8, 2 * CH)), 5, 1)(pos, own_gi, got_gi, own_st, got_st)
    rim = later(edge, 1)

    values, in_map, out_map, within, until, step, entering, packet = scan(
        pos, rim, own_gi, got_gi, own_st, got_st, conv_inner, conv_state, small
    )
    packets = {s: later(packet, s) for s in (3, 7, 2, 6, 1, 5)}
    packets[4] = later(packets[3], 1)
    packets = [packets[s] for s in range(1, 8)]
    insides = (own_gi, got_gi, values, in_map, out_map, within, step, entering, small)
    first = inside(0, pos, *insides)
    second = inside(1, pos, *insides)
    own_g, send_g, energy = gated(pos, *packets, *first, *second, out_map, until, gate_gain[None])

    got_g = swap(send_g)
    parts = (own_g, got_g, energy, w_all)
    far_low, far_high = spread(pos, ((2, (0, 1)), (2, (2, 3))), parts)
    t_plus, t_minus = plane_move(far_low, 1, 0), plane_move(far_high, -1, 0)
    near_plus, near_minus = spread(pos, ((1, (2, 3)), (3, (0, 1))), parts)
    d_plus, d_minus = plane_move(near_plus, 1, 0), plane_move(near_minus, -1, 0)
    keep_outs = (shape((4, 2 * HALF, N)), shape((8, N)))
    kept, tail = kernel(keep_body, keep_outs, 5, 1, (), 2 * HALF * 512 * 1024)(pos, *parts)
    (on_plus,) = spread(pos, ((1, (0, 1)),), parts, (t_plus,))
    u_plus = plane_move(on_plus, 1, 0)
    (on_minus,) = spread(pos, ((3, (2, 3)),), parts, (t_minus,))
    u_minus = plane_move(on_minus, -1, 0)
    q = half_sum(kept, tail, u_plus, d_minus, d_plus, u_minus)
    last = [q[0]] + [plane_move(q[t], t, 1) for t in (1, 2, 3)]
    own, send = total(pos, *last)
    return finish(pos, tokens, own, swap(send))


def solution(mesh):
    return jax.shard_map(
        local,
        mesh=mesh,
        in_specs=(
            P("seq", "chan"),
            P(),
            P(None, "chan"),
            P(None, "chan"),
            P("chan", None),
            P(None, "chan"),
            P(),
            P("chan"),
            P("chan"),
            P("chan"),
            P("chan"),
            P("chan", None),
        ),
        out_specs=P("seq", "chan"),
        check_vma=False,
    )
```

```python
import jax
import jax.numpy as jnp
from jax import lax
from jax.experimental import pallas as pl
from jax.experimental.pallas import tpu as pltpu
from jax.sharding import PartitionSpec as P


D = 4096
DI = 8192
N = 128
P_SIZE = 64
K = 4
Q = 256
ROWS = 1024
HALF = 512
CHUNKS = 4
HEADS = 4
CH = 256
EPS = 1e-05
F32 = jnp.float32
BF16 = jnp.bfloat16


def plane_move(value, steps, phase):
    pairs = []
    for y in range(4):
        for x in range(4):
            for c in range(2):
                dy, dx = (0, steps) if c == phase else (steps, 0)
                pairs.append(((y * 4 + x) * 2 + c, ((y + dy) % 4 * 4 + (x + dx) % 4) * 2 + c))
    return lax.ppermute(value, "chan", pairs)


def swap(value):
    return lax.ppermute(value, "chan", [(i, i ^ 1) for i in range(32)])


def later(value, steps):
    return lax.ppermute(value, "seq", [(i, i + steps) for i in range(8 - steps)])


def kernel(body, outs, n_in, smem=0, scratch=(), flops=0, place=True, inputs=None, last=pltpu.VMEM):
    inner = pl.pallas_call(
        body,
        out_shape=jax.tree.map(lambda o: pltpu.VMEM(o.shape, o.dtype), outs) if place else outs,
        in_specs=[pl.BlockSpec(memory_space=pltpu.SMEM)] * smem + [pl.BlockSpec(memory_space=pltpu.VMEM)] * (n_in - smem - 1)
        + [pl.BlockSpec(memory_space=last)],
        out_specs=jax.tree.map(lambda _: pl.BlockSpec(memory_space=pltpu.VMEM), outs),
        scratch_shapes=list(scratch),
        compiler_params=pltpu.CompilerParams(vmem_limit_bytes=16 * 1024 * 1024),
        cost_estimate=pl.CostEstimate(flops=flops, transcendentals=0, bytes_accessed=1 << 20),
    )

    def call(*args):
        spaces = inputs or (pltpu.VMEM,) * (n_in - smem)
        placed = [pltpu.with_memory_space_constraint(a, m) if m else a for a, m in zip(args[smem:], spaces)]
        return inner(*args[:smem], *placed)

    return call


def shape(dims, kind=F32):
    return jax.ShapeDtypeStruct(dims, kind)


def dot(a, b, precision=None):
    return jnp.dot(a, b, preferred_element_type=F32, precision=precision)


def eye(n):
    return lax.broadcasted_iota(jnp.int32, (n, n), 0) == lax.broadcasted_iota(jnp.int32, (n, n), 1)


def stand(row):
    return jnp.sum(jnp.where(eye(N), jnp.broadcast_to(row, (N, N)), 0.0), axis=1, keepdims=True)


def lay(column):
    return jnp.sum(jnp.where(eye(N), jnp.broadcast_to(column, (N, N)), 0.0), axis=0, keepdims=True)


def as_rows(column):
    return jnp.concatenate([lay(column[i * N : (i + 1) * N]) for i in range(4)], axis=0)


def as_column(rows):
    return jnp.concatenate([stand(rows[i : i + 1]) for i in range(4)], axis=0)


def half(index):
    return pl.ds(pl.multiple_of(index * HALF, HALF), HALF)


BLOCK = 2 * HALF + 3 * N


def block_body(pos, away, state_w, gain, tokens, out, sem):
    c, ci = pos[2], pos[3]
    copy = pltpu.make_async_copy(tokens.at[half(c)], out.at[half(c)], sem)
    copy.start()
    out[half(1 - c)] = away[half(c)]
    scaled = (state_w[...].astype(F32) * stand(gain[pl.ds(ci, 1)])).astype(BF16)
    for b in range(3):
        out[2 * HALF + b * N : 2 * HALF + (b + 1) * N] = scaled[:, b * N : (b + 1) * N]
    copy.wait()


def scale_body(gate, inner, gain, out):
    def step(i, _):
        rows = pl.ds(pl.multiple_of(i * N, N), N)
        column = stand(gain[pl.ds(i, 1)])
        out[rows, :CH] = (gate[rows].astype(F32) * column).astype(BF16)
        out[rows, CH:] = (inner[rows].astype(F32) * column).astype(BF16)
        return 0

    lax.fori_loop(0, 2 * 16, step, 0, unroll=4)


def mark_body(ref, out):
    out[...] = ref[:16]


def mark(piece):
    return kernel(mark_body, shape((16, N), BF16), 1)(piece)


def blocks_of(refs):
    found = []
    for ref in refs:
        found += [ref] if len(ref.shape) == 2 else [ref.at[0], ref.at[1]]
    return found


def pick_body(count):
    def body(*refs):
        for i, ref in enumerate(blocks_of(refs[:count])):
            refs[-1][i] = ref[2 * HALF :]

    return body


def pick(*pieces, marks=()):
    blocks = sum(1 if p.ndim == 2 else 2 for p in pieces)
    out = shape((blocks, 3 * N, N), BF16)
    return kernel(pick_body(len(pieces)), out, len(pieces) + len(marks))(*pieces, *marks)


def owner(pos, s, t):
    first = pos[2] == 0
    dy = jnp.where(first, s, t)
    dx = jnp.where(first, t, s)
    return ((pos[0] - dy) & 3) * 4 + ((pos[1] - dx) & 3)


STEP = 256


def add_slots(pos, slots, keep, got, acc, squares, fresh):
    def rows_of(r, _):
        rows = pl.ds(pl.multiple_of(r * STEP, STEP), STEP)
        low = pl.ds(pl.multiple_of(r * STEP, STEP), STEP)
        high = pl.ds(pl.multiple_of(HALF + r * STEP, STEP), STEP)
        square = None if fresh else squares[rows]
        for n, (s, blocks) in enumerate(slots):
            parts = []
            for ref in blocks:
                parts += [ref[low], ref[high]]
            for v in parts:
                v = v.astype(F32)
                square = v * v if square is None else square + v * v
            lhs = jnp.concatenate(parts, axis=1)
            ids = [pl.ds(pl.multiple_of(owner(pos, s, t) * 2 * N, 2 * N), 2 * N) for t in range(4)]
            for w, ref in enumerate((keep, got)):
                for b in range(2):
                    cols = slice(w * 2 * CH + b * CH, w * 2 * CH + (b + 1) * CH)
                    rhs = jnp.concatenate([ref[i, b * CH : (b + 1) * CH] for i in ids], axis=0)
                    part = dot(lhs, rhs)
                    if fresh and n == 0:
                        acc[rows, cols] = part
                    else:
                        acc[rows, cols] += part
        squares[rows] = square
        return 0

    lax.fori_loop(0, HALF // STEP, rows_of, 0)


def most_body(pos, *refs):
    blocks, (keep, got, acc, squares) = blocks_of(refs[:-4]), refs[-4:]
    slots = ((0, blocks[:4]), (1, blocks[4:8]), (3, blocks[8:]))
    add_slots(pos, slots, keep, got, acc, squares, True)


def most(pos, *parts):
    outs = (shape((HALF, 4 * CH)), shape((HALF, N)))
    return kernel(most_body, outs, len(parts) + 1, 1, (), 2 * HALF * 3072 * 1024)(pos, *parts)


def rest_body(pos, c0, c1, keep, got, acc, squares, own, send, scale):
    blocks = blocks_of((c0, c1))

    def rows_of(r, _):
        rows = pl.ds(pl.multiple_of(r * STEP, STEP), STEP)
        high = pl.ds(pl.multiple_of(HALF + r * STEP, STEP), STEP)
        square = squares[rows]
        parts = []
        for ref in blocks:
            parts += [ref[rows], ref[high]]
        for v in parts:
            v = v.astype(F32)
            square = square + v * v
        inverse = lax.rsqrt(jnp.sum(square, axis=1, keepdims=True) / D + EPS)
        scale[rows] = jnp.broadcast_to(inverse, (STEP, N))
        lhs = jnp.concatenate(parts, axis=1)
        ids = [pl.ds(pl.multiple_of(owner(pos, 2, t) * 2 * N, 2 * N), 2 * N) for t in range(4)]
        for w, (ref, out) in enumerate(((keep, own), (got, send))):
            for b in range(2):
                cols = slice(b * CH, (b + 1) * CH)
                rhs = jnp.concatenate([ref[i, cols] for i in ids], axis=0)
                part = acc[rows, w * 2 * CH + b * CH : w * 2 * CH + (b + 1) * CH] + dot(lhs, rhs)
                out[rows, cols] = (part * inverse).astype(BF16)
        return 0

    lax.fori_loop(0, HALF // STEP, rows_of, 0)


def rest(pos, *parts):
    outs = (shape((HALF, 2 * CH), BF16), shape((HALF, 2 * CH), BF16), shape((HALF, N)))
    return kernel(rest_body, outs, 7, 1, (), 2 * HALF * 1024 * 1024)(pos, *parts)


ORDER = (0, 1, 3, 2)


def state_sum(pos, blocks, most_own, most_got, last_own, last_got, slots, finish):
    c = pos[2]

    def rows_of(r, _):
        mine = pl.ds(pl.multiple_of(c * HALF + r * STEP, STEP), STEP)
        other = pl.ds(pl.multiple_of((1 - c) * HALF + r * STEP, STEP), STEP)
        lhs, w = [], [[], [], []]
        for g, k in slots:
            i = 4 * g + k
            lhs += [blocks[i][mine], blocks[i][other]]
            j = 4 * ORDER.index(k) + ORDER[g]
            for b in range(3):
                cut = slice(b * N, (b + 1) * N)
                w[b].append(most_own[i, cut] if i < 12 else last_own[i - 12, cut])
                w[b].append(most_got[j, cut] if j < 12 else last_got[j - 12, cut])
        lhs = jnp.concatenate(lhs, axis=1)
        w = [jnp.concatenate(v, axis=0) for v in w]
        finish(r, dot(lhs, jnp.concatenate(w[:2], axis=1)), dot(lhs, w[2]))
        return 0

    lax.fori_loop(0, HALF // STEP, rows_of, 0)


EARLY = [(g, k) for g in range(3) for k in (0, 1, 3)]
LATE = [(g, 2) for g in range(3)] + [(3, k) for k in range(4)]


def state_most_body(pos, *refs):
    blocks, (most_own, most_got, out) = blocks_of(refs[:-3]), refs[-3:]

    def finish(r, left, right):
        rows = pl.ds(pl.multiple_of(r * STEP, STEP), STEP)
        out[rows, : 2 * N] = left
        out[rows, 2 * N :] = right

    state_sum(pos, blocks, most_own, most_got, None, None, EARLY, finish)


def state_most(pos, *parts):
    call = kernel(state_most_body, shape((HALF, 3 * N)), len(parts) + 1, 1, (), 2 * HALF * 2304 * 384)
    return call(pos, *parts)


def state_body(pos, a23, p23, m2, c0, c1, most_own, most_got, last_own, last_got, acc, scale, out, send):
    ci = pos[3]

    def finish(r, left, right):
        rows = pl.ds(pl.multiple_of(r * STEP, STEP), STEP)
        inverse = scale[rows]
        out[rows, :N] = (acc[rows, :N] + left[:, :N]) * inverse
        out[rows, N : 2 * N] = (acc[rows, N : 2 * N] + left[:, N:]) * inverse
        rates = (acc[rows, 2 * N :] + right) * inverse
        lane = lax.broadcasted_iota(jnp.int32, (STEP, N), 1)
        out[rows, 2 * N :] = pltpu.roll(rates, (N - ci * HEADS) & (N - 1), 1)
        send[rows, : 2 * N] = out[rows, : 2 * N].astype(BF16)
        left = pltpu.roll(rates, (N - (ci ^ 1) * HEADS) & (N - 1), 1)
        packed = jnp.zeros((STEP, N), F32)
        for k in range(3):
            piece = left.astype(BF16).astype(F32)
            left = left - piece
            packed = jnp.where(lane // HEADS == k, pltpu.roll(piece, k * HEADS, 1), packed)
        send[rows, 2 * N :] = packed.astype(BF16)

    late = [None] * 12 + blocks_of((c0, c1))
    late[2], late[6], late[10] = a23.at[0], p23.at[0], m2
    state_sum(pos, late, most_own, most_got, last_own, last_got, LATE, finish)


def state_rest(pos, *parts):
    outs = (shape((HALF, 3 * N)), shape((HALF, 3 * N), BF16))
    return kernel(state_body, outs, 12, 1, (), 2 * HALF * 1792 * 384)(pos, *parts)


def silu(v):
    h = 0.5 * v
    return h + h * jnp.tanh(h)


def widen(columns, rows):
    return jnp.concatenate(
        [jnp.broadcast_to(columns[:, h : h + 1], (rows, P_SIZE)) for h in range(HEADS)], axis=1
    )


def convolve(window, taps):
    total = jnp.zeros((Q, CH), F32)
    for k in range(K):
        total = total + taps[k : k + 1] * window[5 + k : 5 + k + Q]
    return silu(total)


def fresh_state(values, b, w, step):
    scaled = (values * widen(jnp.exp(w[Q - 1 : Q] - w) * step, Q)).astype(BF16)
    return lax.dot_general(b, scaled, (((0,), (0,)), ((), ())), preferred_element_type=F32)


def rows_body(
    pos, own_gi, got_gi, own_st, got_st, conv_inner, conv_state, small,
    values, in_map, out_map, within, until, step, fresh, head_i, head_s, pad_i, pad_s, rate, passed,
):
    c = pos[2]
    for which, gi, st in ((c, own_gi, own_st), (1 - c, got_gi, got_st)):
        rows = pl.ds(pl.multiple_of(8 + which * HALF, 8), HALF)
        pad_i[rows] = gi[:, CH:].astype(F32)
        pad_s[rows] = st[:, : 2 * N].astype(F32)
        tail = st[:, 2 * N :].astype(F32)
        if st is got_st:
            tail = tail + (pltpu.roll(tail, N - HEADS, 1) + pltpu.roll(tail, N - 2 * HEADS, 1))
        rate[half(which)] = tail
    lane = lax.broadcasted_iota(jnp.int32, (Q, N), 1)
    lower = (
        lax.broadcasted_iota(jnp.int32, (Q, Q), 0) >= lax.broadcasted_iota(jnp.int32, (Q, Q), 1)
    ).astype(BF16)
    passed[...] = jnp.zeros((8, N), F32)

    def rates(i, _):
        rows = pl.ds(pl.multiple_of(i * Q, Q), Q)
        v = rate[rows] + small[0:1]
        soft = jnp.maximum(v, 0.0) + jnp.log1p(jnp.exp(-jnp.abs(v)))
        steps = jnp.where(lane < HEADS, soft, 0.0)
        step[rows] = steps
        left = steps * small[1:2]
        w = jnp.zeros((Q, N), F32)
        for _ in range(3):
            piece = left.astype(BF16)
            left = left - piece.astype(F32)
            w = w + dot(lower, piece)
        within[rows] = w
        before = passed[:1]
        until[rows] = w + before
        passed[:1] = before + w[Q - 1 : Q]
        return 0

    lax.fori_loop(0, CHUNKS, rates, 0)

    def chunk(i, _):
        rows = pl.ds(pl.multiple_of(i * Q, Q), Q)
        window = pl.ds(pl.multiple_of(i * Q, Q), Q + 8)
        vi = convolve(pad_i[window], conv_inner)
        vs = convolve(pad_s[window], conv_state)
        b = vs[:, :N].astype(BF16)
        values[rows] = vi
        in_map[rows] = b
        out_map[rows] = vs[:, N:].astype(BF16)
        fresh[i] = fresh_state(vi, b, within[rows], step[rows])
        return 0

    lax.fori_loop(1, CHUNKS, chunk, 0)
    head_i[...] = pad_i[8 : 8 + Q]
    head_s[...] = pad_s[8 : 8 + Q]


def rows_of_all(pos, *parts):
    outs = (
        shape((ROWS, CH)),
        shape((ROWS, N), BF16),
        shape((ROWS, N), BF16),
        shape((ROWS, N)),
        shape((ROWS, N)),
        shape((ROWS, N)),
        shape((CHUNKS, N, CH)),
        shape((Q, CH)),
        shape((Q, CH)),
    )
    scratch = (
        pltpu.VMEM((ROWS + 8, CH), F32),
        pltpu.VMEM((ROWS + 8, CH), F32),
        pltpu.VMEM((ROWS, N), F32),
        pltpu.VMEM((8, N), F32),
    )
    return kernel(rows_body, outs, 8, 1, scratch)(pos, *parts)


def scan_body(
    rim, within, until, step, fresh, head_i, head_s, conv_inner, conv_state,
    new_values, new_in, new_out, entering, packet,
):
    vi = convolve(jnp.concatenate([rim[:, :CH], head_i[...]], axis=0), conv_inner)
    vs = convolve(jnp.concatenate([rim[:, CH:], head_s[...]], axis=0), conv_state)
    b = vs[:, :N].astype(BF16)
    new_values[...] = vi
    new_in[...] = b
    new_out[...] = vs[:, N:].astype(BF16)
    carry = fresh_state(vi, b, within[:Q], step[:Q])
    entering[0] = jnp.zeros((N, CH), BF16)
    for i in range(1, CHUNKS):
        entering[i] = carry.astype(BF16)
        end = (i + 1) * Q
        carry = widen(jnp.exp(within[end - 1 : end]), 1) * carry + fresh[i]
    total = widen(until[ROWS - 1 : ROWS], 1)
    high = total.astype(BF16)
    low = (total - high.astype(F32)).astype(BF16)
    packet[:N] = carry.astype(BF16)
    packet[N:] = jnp.concatenate([high, low, jnp.zeros((14, CH), BF16)], axis=0)


def scan(*parts):
    outs = (
        shape((Q, CH)),
        shape((Q, N), BF16),
        shape((Q, N), BF16),
        shape((CHUNKS, N, CH), BF16),
        shape((N + 16, CH), BF16),
    )
    return kernel(scan_body, outs, 9)(*parts)


def inside_body(
    pos, own_gi, got_gi, values, in_map, out_map, within, step, new_values, new_in, new_out, entering, small,
    result, opened, out_all, gate,
):
    c = pos[2]
    skip = widen(small[2:3], 1)
    gate[half(c)] = own_gi[:, :CH]
    gate[half(1 - c)] = got_gi[:, :CH]
    lower = lax.broadcasted_iota(jnp.int32, (Q, Q), 0) >= lax.broadcasted_iota(jnp.int32, (Q, Q), 1)

    def chunk(i, _):
        rows = pl.ds(pl.multiple_of(i * Q, Q), Q)
        opened[rows] = silu(gate[rows].astype(F32))
        head = i == 0
        vi = jnp.where(head, new_values[...], values[rows])
        b = jnp.where(head, new_in[...].astype(F32), in_map[rows].astype(F32)).astype(BF16)
        out = jnp.where(head, new_out[...].astype(F32), out_map[rows].astype(F32)).astype(BF16)
        out_all[rows] = out
        w = within[rows]
        scores = lax.dot_general(out, b, (((1,), (1,)), ((), ())), preferred_element_type=F32)
        flat = w.T
        stepped = (vi * widen(step[rows], Q)).astype(BF16)
        parts = []
        for h in range(HEADS):
            gap = w[:, h : h + 1] - flat[h : h + 1]
            mixing = (scores * jnp.exp(jnp.where(lower, gap, -jnp.inf))).astype(BF16)
            parts.append(dot(mixing, stepped[:, h * P_SIZE : (h + 1) * P_SIZE]))
        local = jnp.concatenate(parts, axis=1)
        local = local + dot(out, entering[i]) * widen(jnp.exp(w), Q)
        result[rows] = local + skip * vi
        return 0

    lax.fori_loop(0, CHUNKS, chunk, 0)


def inside(pos, *parts):
    outs = (shape((ROWS, CH)), shape((ROWS, CH)), shape((ROWS, N), BF16))
    return kernel(inside_body, outs, 13, 1, (pltpu.VMEM((ROWS, CH), BF16),))(pos, *parts)


def edge_body(pos, own_gi, got_gi, own_st, got_st, out):
    second = pos[2] == 1
    last = slice(HALF - 16, HALF)
    inner = jnp.where(second, own_gi[last, CH:].astype(F32), got_gi[last, CH:].astype(F32))
    out[:, :CH] = inner[8:]
    state = jnp.where(second, own_st[last, : 2 * N], got_st[last, : 2 * N].astype(F32))
    out[:, CH:] = state[8:]


def split(energy):
    high = energy.astype(BF16)
    return high, (energy - high.astype(F32)).astype(BF16)


def gated_body(pos, p1, p2, p3, p4, p5, p6, p7, local, opened, out_map, until, gate_gain, own, send, energy):
    c = pos[2]
    carried = jnp.zeros((N, CH), F32)
    log = jnp.zeros((1, CH), F32)
    for p in (p1, p2, p3, p4, p5, p6, p7):
        carried = carried + jnp.exp(log) * p[:N].astype(F32)
        tail = p[N:].astype(F32)
        log = log + (tail[0:1] + tail[1:2])
    carried = carried.astype(BF16)
    for which, to in ((1 - c, send), (c, own)):
        rows = half(which)
        out = local[rows] + dot(out_map[rows], carried) * widen(jnp.exp(until[rows]), HALF)
        out = out * opened[rows]
        to[:HALF] = (out * gate_gain[...]).astype(BF16)
        e = as_rows(jnp.sum(out * out, axis=1, keepdims=True))
        if to is own:
            energy[...] = jnp.concatenate([e, jnp.zeros((4, N), F32)], axis=0)
        else:
            e = jnp.concatenate(split(e), axis=1)
            to[HALF:] = jnp.concatenate([e, jnp.zeros((12, CH), BF16)], axis=0)


def gated(pos, *parts):
    outs = (shape((HALF, CH), BF16), shape((HALF + 16, CH), BF16), shape((8, N)))
    return kernel(gated_body, outs, 13, 1)(pos, *parts)


TALL = 2 * HALF + 16


def energy_rows(energy):
    return jnp.concatenate([*split(energy), jnp.zeros((8, N), BF16)], axis=0)


def stack_body(own, got, out):
    out[:CH] = own[...]
    out[CH:] = got[...]


def pair_energy(got, energy):
    tail = got[HALF:].astype(F32)
    return energy[:4] + (tail[:4, :N] + tail[:4, N:])


def product(pos, own, got, weights, s, t):
    first = pos[2] == 0
    dy = jnp.where(first, t, s)
    dx = jnp.where(first, s, t)
    chip = ((pos[0] + dy) & 3) * 4 + ((pos[1] + dx) & 3)
    cols = pl.ds(pl.multiple_of(chip * 2 * N, 2 * N), 2 * N)
    return dot(jnp.concatenate([own[...], got[:HALF]], axis=1), weights[:, cols])


def spread_body(specs, adds):
    def body(pos, own, got, energy, weights, *refs):
        extra, outs = refs[:adds], refs[adds:]
        for n, (s, pair) in enumerate(specs):
            tail = pair_energy(got, energy)
            if adds:
                rows = extra[n][0, 2 * HALF :].astype(F32)
                tail = tail + (rows[:4] + rows[4:8])
            tail = energy_rows(tail)
            for k, t in enumerate(pair):
                part = product(pos, own, got, weights, s, t)
                for side in range(2):
                    rows = slice(side * HALF, (side + 1) * HALF)
                    value = part[:, side * N : (side + 1) * N]
                    if adds:
                        value = value + extra[n][k, rows].astype(F32)
                    outs[n][k, rows] = value.astype(BF16)
                outs[n][k, 2 * HALF :] = tail

    return body


def spread(pos, specs, parts, extra=()):
    outs = tuple(shape((2, TALL, N), BF16) for _ in specs)
    count = len(extra)
    flops = 2 * HALF * 512 * 512 * len(specs)
    return kernel(spread_body(specs, count), outs, 5 + count, 1, (), flops)(pos, *parts, *extra)


def keep_body(pos, own, got, energy, weights, out, tail):
    for t in range(4):
        part = product(pos, own, got, weights, 0, t)
        out[t, :HALF] = part[:, :N]
        out[t, HALF:] = part[:, N:]
    tail[...] = jnp.concatenate([pair_energy(got, energy), jnp.zeros((4, N), F32)], axis=0)


def half_sum_body(own, tail, u_plus, d_minus, d_plus, u_minus, q0, q1, q2, q3):
    for t, q in enumerate((q0, q1, q2, q3)):
        x, y = ((u_plus, d_minus), (d_plus, u_minus))[t // 2]
        k = t % 2
        value = own[t] + x[k, : 2 * HALF].astype(F32) + y[k, : 2 * HALF].astype(F32)
        q[: 2 * HALF] = value.astype(q.dtype)
        e = x[k, 2 * HALF :].astype(F32) + y[k, 2 * HALF :].astype(F32)
        e = tail[:4] + (e[:4] + e[4:8])
        if q.dtype == BF16:
            q[2 * HALF :] = energy_rows(e)
        else:
            q[2 * HALF :] = jnp.concatenate([e, jnp.zeros((12, N), F32)], axis=0)


def half_sum(*parts):
    outs = (shape((TALL, N)),) + (shape((TALL, N), BF16),) * 3
    return kernel(half_sum_body, outs, 6)(*parts)


def total_body(pos, v0, v1, v2, v3, own, send):
    c = pos[2]
    e = v0[2 * HALF :] + v1[2 * HALF :].astype(F32) + v2[2 * HALF :].astype(F32) + v3[2 * HALF :].astype(F32)
    scale = lax.rsqrt(as_column(e[:4] + e[4:8]) / DI + EPS)
    for which, to in ((1 - c, send), (c, own)):
        rows = half(which)
        to[...] = (v0[rows] + v1[rows].astype(F32) + v2[rows].astype(F32) + v3[rows].astype(F32)) * scale


def total(pos, *parts):
    return kernel(total_body, (shape((HALF, N)), shape((HALF, N))), 5, 1)(pos, *parts)


def finish_body(pos, tokens, own, got, out):
    c = pos[2]
    for which, part in ((c, own), (1 - c, got)):
        rows = half(which)
        out[rows] = (tokens[rows].astype(F32) + part[...]).astype(BF16)


def finish(pos, *parts):
    return kernel(finish_body, shape((ROWS, N), BF16), 4, 1, place=False)(pos, *parts)


def local(
    tokens,
    norm_gain,
    gate_proj,
    inner_proj,
    state_proj,
    conv_inner,
    conv_state,
    log_rate,
    rate_bias,
    skip_gain,
    gate_gain,
    out_proj,
):
    ci = lax.axis_index("chan")
    core = ci & 1
    pos = jnp.stack([ci >> 3, (ci >> 1) & 3, core, ci]).astype(jnp.int32)
    gain = norm_gain.reshape(32, N)

    small = jnp.pad(jnp.stack([rate_bias, -jnp.exp(log_rate), skip_gain]), ((0, 5), (0, N - HEADS)))

    away_tokens = swap(tokens)
    spaces = (None, pltpu.HBM, pltpu.HBM, pltpu.HBM)
    sem = (pltpu.SemaphoreType.DMA,)
    block = kernel(block_body, shape((BLOCK, N), BF16), 5, 1, sem, inputs=spaces, last=pl.ANY)(
        pos, away_tokens, state_proj, gain, tokens
    )

    n1, n3 = plane_move(block, 1, 0), plane_move(block, -1, 0)
    p0, m0 = plane_move(block, 1, 1), plane_move(block, -1, 1)
    p1, m3 = plane_move(n1, 1, 1), plane_move(n3, -1, 1)
    low = plane_move(n1[: BLOCK // 2], 1, 0)
    high = plane_move(n3[BLOCK // 2 :], -1, 0)
    m1 = plane_move(n1, -1, 1)
    n2 = jnp.concatenate([low, high], axis=0)
    a23 = jnp.stack([n2, n3])
    p23, m2 = plane_move(a23, 1, 1), plane_move(n2, -1, 1)
    c0 = plane_move(jnp.stack([p0, p1]), 1, 1)
    c1 = plane_move(jnp.stack([m2, m3]), -1, 1)
    mark1 = mark(p1)
    mark2 = mark(m2)
    early = (block, n1, a23, p0, p1, p23, m0, m1, m2, m3)

    keep = kernel(scale_body, shape((D, 2 * CH), BF16), 3)(gate_proj, inner_proj, gain)
    got = swap(keep)
    got_w = swap(out_proj)

    most_own = pick(*early, marks=(mark1, mark2))
    most_got = swap(most_own)
    acc, squares = most(pos, *early, keep, got)
    acc_st = state_most(pos, *early, most_own, most_got)
    w_all = kernel(stack_body, shape((2 * CH, D), BF16), 2)(out_proj, got_w)
    last_own = pick(c0, c1)
    last_got = swap(last_own)
    own_gi, send_gi, scale = rest(pos, c0, c1, keep, got, acc, squares)
    got_gi = swap(send_gi)
    own_st, send_st = state_rest(pos, a23, p23, m2, c0, c1, most_own, most_got, last_own, last_got, acc_st, scale)
    got_st = swap(send_st)

    edge = kernel(edge_body, shape((8, 2 * CH)), 5, 1)(pos, own_gi, got_gi, own_st, got_st)
    rim = later(edge, 1)

    values, in_map, out_map, within, until, step, *fresh = rows_of_all(
        pos, own_gi, got_gi, own_st, got_st, conv_inner, conv_state, small
    )
    *new, entering, packet = scan(
        rim, within, until, step, *fresh, conv_inner, conv_state
    )
    packets = {s: later(packet, s) for s in (3, 7, 2, 6, 1, 5)}
    packets[4] = later(packets[3], 1)
    packets = [packets[s] for s in range(1, 8)]
    result, opened, out_all = inside(pos, own_gi, got_gi, values, in_map, out_map, within, step, *new, entering, small)
    own_g, send_g, energy = gated(pos, *packets, result, opened, out_all, until, gate_gain[None])

    got_g = swap(send_g)
    parts = (own_g, got_g, energy, w_all)
    far_low, far_high = spread(pos, ((2, (0, 1)), (2, (2, 3))), parts)
    t_plus, t_minus = plane_move(far_low, 1, 0), plane_move(far_high, -1, 0)
    near_plus, near_minus = spread(pos, ((1, (2, 3)), (3, (0, 1))), parts)
    d_plus, d_minus = plane_move(near_plus, 1, 0), plane_move(near_minus, -1, 0)
    keep_outs = (shape((4, 2 * HALF, N)), shape((8, N)))
    kept, tail = kernel(keep_body, keep_outs, 5, 1, (), 2 * HALF * 512 * 1024)(pos, *parts)
    (on_plus,) = spread(pos, ((1, (0, 1)),), parts, (t_plus,))
    u_plus = plane_move(on_plus, 1, 0)
    (on_minus,) = spread(pos, ((3, (2, 3)),), parts, (t_minus,))
    u_minus = plane_move(on_minus, -1, 0)
    q = half_sum(kept, tail, u_plus, d_minus, d_plus, u_minus)
    last = [q[0]] + [plane_move(q[t], t, 1) for t in (1, 2, 3)]
    own, send = total(pos, *last)
    return finish(pos, tokens, own, swap(send))


def solution(mesh):
    return jax.shard_map(
        local,
        mesh=mesh,
        in_specs=(
            P("seq", "chan"),
            P(),
            P(None, "chan"),
            P(None, "chan"),
            P("chan", None),
            P(None, "chan"),
            P(),
            P("chan"),
            P("chan"),
            P("chan"),
            P("chan"),
            P("chan", None),
        ),
        out_specs=P("seq", "chan"),
        check_vma=False,
    )
```

```python
import jax
import jax.numpy as jnp
from jax import lax
from jax.experimental import pallas as pl
from jax.experimental.pallas import tpu as pltpu
from jax.sharding import PartitionSpec as P


D = 4096
DI = 8192
N = 128
P_SIZE = 64
K = 4
Q = 256
ROWS = 1024
HALF = 512
CHUNKS = 4
HEADS = 4
CH = 256
EPS = 1e-05
F32 = jnp.float32
BF16 = jnp.bfloat16


def plane_move(value, steps, phase):
    pairs = []
    for y in range(4):
        for x in range(4):
            for c in range(2):
                dy, dx = (0, steps) if c == phase else (steps, 0)
                pairs.append(((y * 4 + x) * 2 + c, ((y + dy) % 4 * 4 + (x + dx) % 4) * 2 + c))
    return lax.ppermute(value, "chan", pairs)


def swap(value):
    return lax.ppermute(value, "chan", [(i, i ^ 1) for i in range(32)])


def later(value, steps):
    return lax.ppermute(value, "seq", [(i, i + steps) for i in range(8 - steps)])


def kernel(body, outs, n_in, smem=0, scratch=(), flops=0, place=True, inputs=None, last=pltpu.VMEM):
    inner = pl.pallas_call(
        body,
        out_shape=jax.tree.map(lambda o: pltpu.VMEM(o.shape, o.dtype), outs) if place else outs,
        in_specs=[pl.BlockSpec(memory_space=pltpu.SMEM)] * smem + [pl.BlockSpec(memory_space=pltpu.VMEM)] * (n_in - smem - 1)
        + [pl.BlockSpec(memory_space=last)],
        out_specs=jax.tree.map(lambda _: pl.BlockSpec(memory_space=pltpu.VMEM), outs),
        scratch_shapes=list(scratch),
        compiler_params=pltpu.CompilerParams(vmem_limit_bytes=16 * 1024 * 1024),
        cost_estimate=pl.CostEstimate(flops=flops, transcendentals=0, bytes_accessed=1 << 20),
    )

    def call(*args):
        spaces = inputs or (pltpu.VMEM,) * (n_in - smem)
        placed = [pltpu.with_memory_space_constraint(a, m) if m else a for a, m in zip(args[smem:], spaces)]
        return inner(*args[:smem], *placed)

    return call


def shape(dims, kind=F32):
    return jax.ShapeDtypeStruct(dims, kind)


def dot(a, b, precision=None):
    return jnp.dot(a, b, preferred_element_type=F32, precision=precision)


def eye(n):
    return lax.broadcasted_iota(jnp.int32, (n, n), 0) == lax.broadcasted_iota(jnp.int32, (n, n), 1)


def stand(row):
    return jnp.sum(jnp.where(eye(N), jnp.broadcast_to(row, (N, N)), 0.0), axis=1, keepdims=True)


def lay(column):
    return jnp.sum(jnp.where(eye(N), jnp.broadcast_to(column, (N, N)), 0.0), axis=0, keepdims=True)


def as_rows(column):
    return jnp.concatenate([lay(column[i * N : (i + 1) * N]) for i in range(4)], axis=0)


def as_column(rows):
    return jnp.concatenate([stand(rows[i : i + 1]) for i in range(4)], axis=0)


def half(index):
    return pl.ds(pl.multiple_of(index * HALF, HALF), HALF)


BLOCK = 2 * HALF + 3 * N


def own_body(pos, state_w, gain, tokens, out, sem):
    c, ci = pos[2], pos[3]
    copy = pltpu.make_async_copy(tokens.at[half(c)], out.at[:HALF], sem)
    copy.start()
    scaled = (state_w[...].astype(F32) * stand(gain[pl.ds(ci, 1)])).astype(BF16)
    for b in range(3):
        out[HALF + b * N : HALF + (b + 1) * N] = scaled[:, b * N : (b + 1) * N]
    copy.wait()


def block_body(pos, own, away, out):
    c = pos[2]
    out[half(c)] = own[:HALF]
    out[half(1 - c)] = away[half(c)]
    out[2 * HALF :] = own[HALF:]


def scale_body(gate, inner, gain, out):
    def step(i, _):
        rows = pl.ds(pl.multiple_of(i * N, N), N)
        column = stand(gain[pl.ds(i, 1)])
        out[rows, :CH] = (gate[rows].astype(F32) * column).astype(BF16)
        out[rows, CH:] = (inner[rows].astype(F32) * column).astype(BF16)
        return 0

    lax.fori_loop(0, 2 * 16, step, 0, unroll=4)


def mark_body(ref, out):
    out[...] = ref[:16]


def mark(piece):
    return kernel(mark_body, shape((16, N), BF16), 1)(piece)


def blocks_of(refs):
    found = []
    for ref in refs:
        found += [ref] if len(ref.shape) == 2 else [ref.at[0], ref.at[1]]
    return found


def pick_body(count):
    def body(*refs):
        for i, ref in enumerate(blocks_of(refs[:count])):
            refs[-1][i] = ref[2 * HALF :]

    return body


def pick(*pieces, marks=()):
    blocks = sum(1 if p.ndim == 2 else 2 for p in pieces)
    out = shape((blocks, 3 * N, N), BF16)
    return kernel(pick_body(len(pieces)), out, len(pieces) + len(marks))(*pieces, *marks)


def owner(pos, s, t):
    first = pos[2] == 0
    dy = jnp.where(first, s, t)
    dx = jnp.where(first, t, s)
    return ((pos[0] - dy) & 3) * 4 + ((pos[1] - dx) & 3)


STEP = 256


def add_slots(pos, slots, keep, got, acc, squares, fresh):
    def rows_of(r, _):
        rows = pl.ds(pl.multiple_of(r * STEP, STEP), STEP)
        low = pl.ds(pl.multiple_of(r * STEP, STEP), STEP)
        high = pl.ds(pl.multiple_of(HALF + r * STEP, STEP), STEP)
        square = None if fresh else squares[rows]
        for n, (s, blocks) in enumerate(slots):
            parts = []
            for ref in blocks:
                parts += [ref[low], ref[high]]
            for v in parts:
                v = v.astype(F32)
                square = v * v if square is None else square + v * v
            lhs = jnp.concatenate(parts, axis=1)
            ids = [pl.ds(pl.multiple_of(owner(pos, s, t) * 2 * N, 2 * N), 2 * N) for t in range(4)]
            for w, ref in enumerate((keep, got)):
                for b in range(2):
                    cols = slice(w * 2 * CH + b * CH, w * 2 * CH + (b + 1) * CH)
                    rhs = jnp.concatenate([ref[i, b * CH : (b + 1) * CH] for i in ids], axis=0)
                    part = dot(lhs, rhs)
                    if fresh and n == 0:
                        acc[rows, cols] = part
                    else:
                        acc[rows, cols] += part
        squares[rows] = square
        return 0

    lax.fori_loop(0, HALF // STEP, rows_of, 0)


def most_body(pos, *refs):
    blocks, (keep, got, acc, squares) = blocks_of(refs[:-4]), refs[-4:]
    slots = ((0, blocks[:4]), (1, blocks[4:8]), (3, blocks[8:]))
    add_slots(pos, slots, keep, got, acc, squares, True)


def most(pos, *parts):
    outs = (shape((HALF, 4 * CH)), shape((HALF, N)))
    return kernel(most_body, outs, len(parts) + 1, 1, (), 2 * HALF * 3072 * 1024)(pos, *parts)


def rest_body(pos, c0, c1, keep, got, acc, squares, own, send, scale):
    blocks = blocks_of((c0, c1))

    def rows_of(r, _):
        rows = pl.ds(pl.multiple_of(r * STEP, STEP), STEP)
        high = pl.ds(pl.multiple_of(HALF + r * STEP, STEP), STEP)
        square = squares[rows]
        parts = []
        for ref in blocks:
            parts += [ref[rows], ref[high]]
        for v in parts:
            v = v.astype(F32)
            square = square + v * v
        inverse = lax.rsqrt(jnp.sum(square, axis=1, keepdims=True) / D + EPS)
        scale[rows] = jnp.broadcast_to(inverse, (STEP, N))
        lhs = jnp.concatenate(parts, axis=1)
        ids = [pl.ds(pl.multiple_of(owner(pos, 2, t) * 2 * N, 2 * N), 2 * N) for t in range(4)]
        for w, (ref, out) in enumerate(((keep, own), (got, send))):
            for b in range(2):
                cols = slice(b * CH, (b + 1) * CH)
                rhs = jnp.concatenate([ref[i, cols] for i in ids], axis=0)
                part = acc[rows, w * 2 * CH + b * CH : w * 2 * CH + (b + 1) * CH] + dot(lhs, rhs)
                out[rows, cols] = (part * inverse).astype(BF16)
        return 0

    lax.fori_loop(0, HALF // STEP, rows_of, 0)


def rest(pos, *parts):
    outs = (shape((HALF, 2 * CH), BF16), shape((HALF, 2 * CH), BF16), shape((HALF, N)))
    return kernel(rest_body, outs, 7, 1, (), 2 * HALF * 1024 * 1024)(pos, *parts)


ORDER = (0, 1, 3, 2)


def state_sum(pos, blocks, most_own, most_got, last_own, last_got, slots, finish):
    c = pos[2]

    def rows_of(r, _):
        mine = pl.ds(pl.multiple_of(c * HALF + r * STEP, STEP), STEP)
        other = pl.ds(pl.multiple_of((1 - c) * HALF + r * STEP, STEP), STEP)
        lhs, w = [], [[], [], []]
        for g, k in slots:
            i = 4 * g + k
            lhs += [blocks[i][mine], blocks[i][other]]
            j = 4 * ORDER.index(k) + ORDER[g]
            for b in range(3):
                cut = slice(b * N, (b + 1) * N)
                w[b].append(most_own[i, cut] if i < 12 else last_own[i - 12, cut])
                w[b].append(most_got[j, cut] if j < 12 else last_got[j - 12, cut])
        lhs = jnp.concatenate(lhs, axis=1)
        w = [jnp.concatenate(v, axis=0) for v in w]
        finish(r, dot(lhs, jnp.concatenate(w[:2], axis=1)), dot(lhs, w[2]))
        return 0

    lax.fori_loop(0, HALF // STEP, rows_of, 0)


EARLY = [(g, k) for g in range(3) for k in (0, 1, 3)]
LATE = [(g, 2) for g in range(3)] + [(3, k) for k in range(4)]


def state_most_body(pos, *refs):
    blocks, (most_own, most_got, out) = blocks_of(refs[:-3]), refs[-3:]

    def finish(r, left, right):
        rows = pl.ds(pl.multiple_of(r * STEP, STEP), STEP)
        out[rows, : 2 * N] = left
        out[rows, 2 * N :] = right

    state_sum(pos, blocks, most_own, most_got, None, None, EARLY, finish)


def state_most(pos, *parts):
    call = kernel(state_most_body, shape((HALF, 3 * N)), len(parts) + 1, 1, (), 2 * HALF * 2304 * 384)
    return call(pos, *parts)


def state_body(pos, a23, p23, m2, c0, c1, most_own, most_got, last_own, last_got, acc, scale, out, send):
    ci = pos[3]

    def finish(r, left, right):
        rows = pl.ds(pl.multiple_of(r * STEP, STEP), STEP)
        inverse = scale[rows]
        out[rows, :N] = (acc[rows, :N] + left[:, :N]) * inverse
        out[rows, N : 2 * N] = (acc[rows, N : 2 * N] + left[:, N:]) * inverse
        rates = (acc[rows, 2 * N :] + right) * inverse
        lane = lax.broadcasted_iota(jnp.int32, (STEP, N), 1)
        out[rows, 2 * N :] = pltpu.roll(rates, (N - ci * HEADS) & (N - 1), 1)
        send[rows, : 2 * N] = out[rows, : 2 * N].astype(BF16)
        left = pltpu.roll(rates, (N - (ci ^ 1) * HEADS) & (N - 1), 1)
        packed = jnp.zeros((STEP, N), F32)
        for k in range(3):
            piece = left.astype(BF16).astype(F32)
            left = left - piece
            packed = jnp.where(lane // HEADS == k, pltpu.roll(piece, k * HEADS, 1), packed)
        send[rows, 2 * N :] = packed.astype(BF16)

    late = [None] * 12 + blocks_of((c0, c1))
    late[2], late[6], late[10] = a23.at[0], p23.at[0], m2
    state_sum(pos, late, most_own, most_got, last_own, last_got, LATE, finish)


def state_rest(pos, *parts):
    outs = (shape((HALF, 3 * N)), shape((HALF, 3 * N), BF16))
    return kernel(state_body, outs, 12, 1, (), 2 * HALF * 1792 * 384)(pos, *parts)


def silu(v):
    h = 0.5 * v
    return h + h * jnp.tanh(h)


def widen(columns, rows):
    return jnp.concatenate(
        [jnp.broadcast_to(columns[:, h : h + 1], (rows, P_SIZE)) for h in range(HEADS)], axis=1
    )


def convolve(window, taps):
    total = jnp.zeros((Q, CH), F32)
    for k in range(K):
        total = total + taps[k : k + 1] * window[5 + k : 5 + k + Q]
    return silu(total)


def fresh_state(values, b, w, step):
    scaled = (values * widen(jnp.exp(w[Q - 1 : Q] - w) * step, Q)).astype(BF16)
    return lax.dot_general(b, scaled, (((0,), (0,)), ((), ())), preferred_element_type=F32)


def values_body(pos, own_gi, got_gi, taps, values, head, pad):
    c = pos[2]
    for which, gi in ((c, own_gi), (1 - c, got_gi)):
        pad[pl.ds(pl.multiple_of(8 + which * HALF, 8), HALF)] = gi[:, CH:].astype(F32)

    def chunk(i, _):
        rows = pl.ds(pl.multiple_of(i * Q, Q), Q)
        values[rows] = convolve(pad[pl.ds(pl.multiple_of(i * Q, Q), Q + 8)], taps)
        return 0

    lax.fori_loop(1, CHUNKS, chunk, 0)
    head[...] = pad[8 : 8 + Q]


def values_of(pos, *parts):
    scratch = (pltpu.VMEM((ROWS + 8, CH), F32),)
    return kernel(values_body, (shape((ROWS, CH)), shape((Q, CH))), 4, 1, scratch)(pos, *parts)


def rows_body(
    pos, own_st, got_st, values, conv_state, small,
    in_map, out_map, within, until, step, fresh, head, pad, rate, passed,
):
    c = pos[2]
    for which, st in ((c, own_st), (1 - c, got_st)):
        pad[pl.ds(pl.multiple_of(8 + which * HALF, 8), HALF)] = st[:, : 2 * N].astype(F32)
        tail = st[:, 2 * N :].astype(F32)
        if st is got_st:
            tail = tail + (pltpu.roll(tail, N - HEADS, 1) + pltpu.roll(tail, N - 2 * HEADS, 1))
        rate[half(which)] = tail
    lane = lax.broadcasted_iota(jnp.int32, (Q, N), 1)
    lower = (
        lax.broadcasted_iota(jnp.int32, (Q, Q), 0) >= lax.broadcasted_iota(jnp.int32, (Q, Q), 1)
    ).astype(BF16)
    passed[...] = jnp.zeros((8, N), F32)

    def rates(i, _):
        rows = pl.ds(pl.multiple_of(i * Q, Q), Q)
        v = rate[rows] + small[0:1]
        soft = jnp.maximum(v, 0.0) + jnp.log1p(jnp.exp(-jnp.abs(v)))
        steps = jnp.where(lane < HEADS, soft, 0.0)
        step[rows] = steps
        left = steps * small[1:2]
        w = jnp.zeros((Q, N), F32)
        for _ in range(3):
            piece = left.astype(BF16)
            left = left - piece.astype(F32)
            w = w + dot(lower, piece)
        within[rows] = w
        before = passed[:1]
        until[rows] = w + before
        passed[:1] = before + w[Q - 1 : Q]
        return 0

    lax.fori_loop(0, CHUNKS, rates, 0)

    def chunk(i, _):
        rows = pl.ds(pl.multiple_of(i * Q, Q), Q)
        vs = convolve(pad[pl.ds(pl.multiple_of(i * Q, Q), Q + 8)], conv_state)
        b = vs[:, :N].astype(BF16)
        in_map[rows] = b
        out_map[rows] = vs[:, N:].astype(BF16)
        fresh[i] = fresh_state(values[rows], b, within[rows], step[rows])
        return 0

    lax.fori_loop(1, CHUNKS, chunk, 0)
    head[...] = pad[8 : 8 + Q]


def rows_of_all(pos, *parts):
    outs = (
        shape((ROWS, N), BF16),
        shape((ROWS, N), BF16),
        shape((ROWS, N)),
        shape((ROWS, N)),
        shape((ROWS, N)),
        shape((CHUNKS, N, CH)),
        shape((Q, CH)),
    )
    scratch = (pltpu.VMEM((ROWS + 8, CH), F32), pltpu.VMEM((ROWS, N), F32), pltpu.VMEM((8, N), F32))
    return kernel(rows_body, outs, 6, 1, scratch)(pos, *parts)


def scan_body(
    rim, within, until, step, fresh, head_s, head_i, conv_inner, conv_state,
    new_values, new_in, new_out, entering, packet,
):
    vi = convolve(jnp.concatenate([rim[:, :CH], head_i[...]], axis=0), conv_inner)
    vs = convolve(jnp.concatenate([rim[:, CH:], head_s[...]], axis=0), conv_state)
    b = vs[:, :N].astype(BF16)
    new_values[...] = vi
    new_in[...] = b
    new_out[...] = vs[:, N:].astype(BF16)
    carry = fresh_state(vi, b, within[:Q], step[:Q])
    entering[0] = jnp.zeros((N, CH), BF16)
    for i in range(1, CHUNKS):
        entering[i] = carry.astype(BF16)
        end = (i + 1) * Q
        carry = widen(jnp.exp(within[end - 1 : end]), 1) * carry + fresh[i]
    total = widen(until[ROWS - 1 : ROWS], 1)
    high = total.astype(BF16)
    low = (total - high.astype(F32)).astype(BF16)
    packet[:N] = carry.astype(BF16)
    packet[N:] = jnp.concatenate([high, low, jnp.zeros((14, CH), BF16)], axis=0)


def scan(*parts):
    outs = (
        shape((Q, CH)),
        shape((Q, N), BF16),
        shape((Q, N), BF16),
        shape((CHUNKS, N, CH), BF16),
        shape((N + 16, CH), BF16),
    )
    return kernel(scan_body, outs, 9)(*parts)


def inside_body(
    pos, own_gi, got_gi, values, in_map, out_map, within, step, new_values, new_in, new_out, entering, small,
    result, opened, out_all, gate,
):
    c = pos[2]
    skip = widen(small[2:3], 1)
    gate[half(c)] = own_gi[:, :CH]
    gate[half(1 - c)] = got_gi[:, :CH]
    lower = lax.broadcasted_iota(jnp.int32, (Q, Q), 0) >= lax.broadcasted_iota(jnp.int32, (Q, Q), 1)

    def chunk(i, _):
        rows = pl.ds(pl.multiple_of(i * Q, Q), Q)
        opened[rows] = silu(gate[rows].astype(F32))
        head = i == 0
        vi = jnp.where(head, new_values[...], values[rows])
        b = jnp.where(head, new_in[...].astype(F32), in_map[rows].astype(F32)).astype(BF16)
        out = jnp.where(head, new_out[...].astype(F32), out_map[rows].astype(F32)).astype(BF16)
        out_all[rows] = out
        w = within[rows]
        scores = lax.dot_general(out, b, (((1,), (1,)), ((), ())), preferred_element_type=F32)
        flat = w.T
        stepped = (vi * widen(step[rows], Q)).astype(BF16)
        parts = []
        for h in range(HEADS):
            gap = w[:, h : h + 1] - flat[h : h + 1]
            mixing = (scores * jnp.exp(jnp.where(lower, gap, -jnp.inf))).astype(BF16)
            parts.append(dot(mixing, stepped[:, h * P_SIZE : (h + 1) * P_SIZE]))
        local = jnp.concatenate(parts, axis=1)
        local = local + dot(out, entering[i]) * widen(jnp.exp(w), Q)
        result[rows] = local + skip * vi
        return 0

    lax.fori_loop(0, CHUNKS, chunk, 0)


def inside(pos, *parts):
    outs = (shape((ROWS, CH)), shape((ROWS, CH)), shape((ROWS, N), BF16))
    return kernel(inside_body, outs, 13, 1, (pltpu.VMEM((ROWS, CH), BF16),))(pos, *parts)


def edge_body(pos, own_gi, got_gi, own_st, got_st, out):
    second = pos[2] == 1
    last = slice(HALF - 16, HALF)
    inner = jnp.where(second, own_gi[last, CH:].astype(F32), got_gi[last, CH:].astype(F32))
    out[:, :CH] = inner[8:]
    state = jnp.where(second, own_st[last, : 2 * N], got_st[last, : 2 * N].astype(F32))
    out[:, CH:] = state[8:]


def split(energy):
    high = energy.astype(BF16)
    return high, (energy - high.astype(F32)).astype(BF16)


def gated_body(pos, p1, p2, p3, p4, p5, p6, p7, local, opened, out_map, until, gate_gain, own, send, energy):
    c = pos[2]
    carried = jnp.zeros((N, CH), F32)
    log = jnp.zeros((1, CH), F32)
    for p in (p1, p2, p3, p4, p5, p6, p7):
        carried = carried + jnp.exp(log) * p[:N].astype(F32)
        tail = p[N:].astype(F32)
        log = log + (tail[0:1] + tail[1:2])
    carried = carried.astype(BF16)
    for which, to in ((1 - c, send), (c, own)):
        rows = half(which)
        out = local[rows] + dot(out_map[rows], carried) * widen(jnp.exp(until[rows]), HALF)
        out = out * opened[rows]
        to[:HALF] = (out * gate_gain[...]).astype(BF16)
        e = as_rows(jnp.sum(out * out, axis=1, keepdims=True))
        if to is own:
            energy[...] = jnp.concatenate([e, jnp.zeros((4, N), F32)], axis=0)
        else:
            e = jnp.concatenate(split(e), axis=1)
            to[HALF:] = jnp.concatenate([e, jnp.zeros((12, CH), BF16)], axis=0)


def gated(pos, *parts):
    outs = (shape((HALF, CH), BF16), shape((HALF + 16, CH), BF16), shape((8, N)))
    return kernel(gated_body, outs, 13, 1)(pos, *parts)


TALL = 2 * HALF + 16


def energy_rows(energy):
    return jnp.concatenate([*split(energy), jnp.zeros((8, N), BF16)], axis=0)


def stack_body(own, got, out):
    out[:CH] = own[...]
    out[CH:] = got[...]


def pair_energy(got, energy):
    tail = got[HALF:].astype(F32)
    return energy[:4] + (tail[:4, :N] + tail[:4, N:])


def product(pos, own, got, weights, s, t):
    first = pos[2] == 0
    dy = jnp.where(first, t, s)
    dx = jnp.where(first, s, t)
    chip = ((pos[0] + dy) & 3) * 4 + ((pos[1] + dx) & 3)
    cols = pl.ds(pl.multiple_of(chip * 2 * N, 2 * N), 2 * N)
    return dot(jnp.concatenate([own[...], got[:HALF]], axis=1), weights[:, cols])


def spread_body(specs, adds):
    def body(pos, own, got, energy, weights, *refs):
        extra, outs = refs[:adds], refs[adds:]
        for n, (s, pair) in enumerate(specs):
            tail = pair_energy(got, energy)
            if adds:
                rows = extra[n][0, 2 * HALF :].astype(F32)
                tail = tail + (rows[:4] + rows[4:8])
            tail = energy_rows(tail)
            for k, t in enumerate(pair):
                part = product(pos, own, got, weights, s, t)
                for side in range(2):
                    rows = slice(side * HALF, (side + 1) * HALF)
                    value = part[:, side * N : (side + 1) * N]
                    if adds:
                        value = value + extra[n][k, rows].astype(F32)
                    outs[n][k, rows] = value.astype(BF16)
                outs[n][k, 2 * HALF :] = tail

    return body


def spread(pos, specs, parts, extra=()):
    outs = tuple(shape((2, TALL, N), BF16) for _ in specs)
    count = len(extra)
    flops = 2 * HALF * 512 * 512 * len(specs)
    return kernel(spread_body(specs, count), outs, 5 + count, 1, (), flops)(pos, *parts, *extra)


def keep_body(pos, own, got, energy, weights, out, tail):
    for t in range(4):
        part = product(pos, own, got, weights, 0, t)
        out[t, :HALF] = part[:, :N]
        out[t, HALF:] = part[:, N:]
    tail[...] = jnp.concatenate([pair_energy(got, energy), jnp.zeros((4, N), F32)], axis=0)


def half_sum_body(own, tail, u_plus, d_minus, d_plus, u_minus, q0, q1, q2, q3):
    for t, q in enumerate((q0, q1, q2, q3)):
        x, y = ((u_plus, d_minus), (d_plus, u_minus))[t // 2]
        k = t % 2
        value = own[t] + x[k, : 2 * HALF].astype(F32) + y[k, : 2 * HALF].astype(F32)
        q[: 2 * HALF] = value.astype(q.dtype)
        e = x[k, 2 * HALF :].astype(F32) + y[k, 2 * HALF :].astype(F32)
        e = tail[:4] + (e[:4] + e[4:8])
        if q.dtype == BF16:
            q[2 * HALF :] = energy_rows(e)
        else:
            q[2 * HALF :] = jnp.concatenate([e, jnp.zeros((12, N), F32)], axis=0)


def half_sum(*parts):
    outs = (shape((TALL, N)),) + (shape((TALL, N), BF16),) * 3
    return kernel(half_sum_body, outs, 6)(*parts)


def total_body(pos, v0, v1, v2, v3, own, send):
    c = pos[2]
    e = v0[2 * HALF :] + v1[2 * HALF :].astype(F32) + v2[2 * HALF :].astype(F32) + v3[2 * HALF :].astype(F32)
    scale = lax.rsqrt(as_column(e[:4] + e[4:8]) / DI + EPS)
    for which, to in ((1 - c, send), (c, own)):
        rows = half(which)
        to[...] = (v0[rows] + v1[rows].astype(F32) + v2[rows].astype(F32) + v3[rows].astype(F32)) * scale


def total(pos, *parts):
    return kernel(total_body, (shape((HALF, N)), shape((HALF, N))), 5, 1)(pos, *parts)


def finish_body(pos, tokens, own, got, out):
    c = pos[2]
    for which, part in ((c, own), (1 - c, got)):
        rows = half(which)
        out[rows] = (tokens[rows].astype(F32) + part[...]).astype(BF16)


def finish(pos, *parts):
    return kernel(finish_body, shape((ROWS, N), BF16), 4, 1, place=False)(pos, *parts)


def local(
    tokens,
    norm_gain,
    gate_proj,
    inner_proj,
    state_proj,
    conv_inner,
    conv_state,
    log_rate,
    rate_bias,
    skip_gain,
    gate_gain,
    out_proj,
):
    ci = lax.axis_index("chan")
    core = ci & 1
    pos = jnp.stack([ci >> 3, (ci >> 1) & 3, core, ci]).astype(jnp.int32)
    gain = norm_gain.reshape(32, N)

    small = jnp.pad(jnp.stack([rate_bias, -jnp.exp(log_rate), skip_gain]), ((0, 5), (0, N - HEADS)))

    away_tokens = swap(tokens)
    sem = (pltpu.SemaphoreType.DMA,)
    own_block = kernel(
        own_body, shape((HALF + 3 * N, N), BF16), 4, 1, sem, inputs=(pltpu.HBM,) * 3, last=pl.ANY
    )(pos, state_proj, gain, tokens)
    block = kernel(block_body, shape((BLOCK, N), BF16), 3, 1)(pos, own_block, away_tokens)

    n1, n3 = plane_move(block, 1, 0), plane_move(block, -1, 0)
    p0, m0 = plane_move(block, 1, 1), plane_move(block, -1, 1)
    p1, m3 = plane_move(n1, 1, 1), plane_move(n3, -1, 1)
    low = plane_move(n1[: BLOCK // 2], 1, 0)
    high = plane_move(n3[BLOCK // 2 :], -1, 0)
    m1 = plane_move(n1, -1, 1)
    n2 = jnp.concatenate([low, high], axis=0)
    a23 = jnp.stack([n2, n3])
    p23, m2 = plane_move(a23, 1, 1), plane_move(n2, -1, 1)
    c0 = plane_move(jnp.stack([p0, p1]), 1, 1)
    c1 = plane_move(jnp.stack([m2, m3]), -1, 1)
    mark1 = mark(p1)
    mark2 = mark(m2)
    early = (block, n1, a23, p0, p1, p23, m0, m1, m2, m3)

    keep = kernel(scale_body, shape((D, 2 * CH), BF16), 3)(gate_proj, inner_proj, gain)
    got = swap(keep)
    got_w = swap(out_proj)

    most_own = pick(*early, marks=(mark1, mark2))
    most_got = swap(most_own)
    acc, squares = most(pos, *early, keep, got)
    acc_st = state_most(pos, *early, most_own, most_got)
    w_all = kernel(stack_body, shape((2 * CH, D), BF16), 2)(out_proj, got_w)
    last_own = pick(c0, c1)
    last_got = swap(last_own)
    own_gi, send_gi, scale = rest(pos, c0, c1, keep, got, acc, squares)
    got_gi = swap(send_gi)
    own_st, send_st = state_rest(pos, a23, p23, m2, c0, c1, most_own, most_got, last_own, last_got, acc_st, scale)
    got_st = swap(send_st)

    edge = kernel(edge_body, shape((8, 2 * CH)), 5, 1)(pos, own_gi, got_gi, own_st, got_st)
    rim = later(edge, 1)

    values, head = values_of(pos, own_gi, got_gi, conv_inner)
    in_map, out_map, within, until, step, *fresh = rows_of_all(pos, own_st, got_st, values, conv_state, small)
    *new, entering, packet = scan(
        rim, within, until, step, *fresh, head, conv_inner, conv_state
    )
    packets = {s: later(packet, s) for s in (3, 7, 2, 6, 1, 5)}
    packets[4] = later(packets[3], 1)
    packets = [packets[s] for s in range(1, 8)]
    result, opened, out_all = inside(pos, own_gi, got_gi, values, in_map, out_map, within, step, *new, entering, small)
    own_g, send_g, energy = gated(pos, *packets, result, opened, out_all, until, gate_gain[None])

    got_g = swap(send_g)
    parts = (own_g, got_g, energy, w_all)
    far_low, far_high = spread(pos, ((2, (0, 1)), (2, (2, 3))), parts)
    t_plus, t_minus = plane_move(far_low, 1, 0), plane_move(far_high, -1, 0)
    near_plus, near_minus = spread(pos, ((1, (2, 3)), (3, (0, 1))), parts)
    d_plus, d_minus = plane_move(near_plus, 1, 0), plane_move(near_minus, -1, 0)
    keep_outs = (shape((4, 2 * HALF, N)), shape((8, N)))
    kept, tail = kernel(keep_body, keep_outs, 5, 1, (), 2 * HALF * 512 * 1024)(pos, *parts)
    (on_plus,) = spread(pos, ((1, (0, 1)),), parts, (t_plus,))
    u_plus = plane_move(on_plus, 1, 0)
    (on_minus,) = spread(pos, ((3, (2, 3)),), parts, (t_minus,))
    u_minus = plane_move(on_minus, -1, 0)
    q = half_sum(kept, tail, u_plus, d_minus, d_plus, u_minus)
    last = [q[0]] + [plane_move(q[t], t, 1) for t in (1, 2, 3)]
    own, send = total(pos, *last)
    return finish(pos, tokens, own, swap(send))


def solution(mesh):
    return jax.shard_map(
        local,
        mesh=mesh,
        in_specs=(
            P("seq", "chan"),
            P(),
            P(None, "chan"),
            P(None, "chan"),
            P("chan", None),
            P(None, "chan"),
            P(),
            P("chan"),
            P("chan"),
            P("chan"),
            P("chan"),
            P("chan", None),
        ),
        out_specs=P("seq", "chan"),
        check_vma=False,
    )
```

```python
import jax
import jax.numpy as jnp
from jax import lax
from jax.experimental import pallas as pl
from jax.experimental.pallas import tpu as pltpu
from jax.sharding import PartitionSpec as P


D = 4096
DI = 8192
N = 128
P_SIZE = 64
K = 4
Q = 256
ROWS = 1024
HALF = 512
CHUNKS = 4
HEADS = 4
CH = 256
EPS = 1e-05
F32 = jnp.float32
BF16 = jnp.bfloat16


def plane_move(value, steps, phase):
    pairs = []
    for y in range(4):
        for x in range(4):
            for c in range(2):
                dy, dx = (0, steps) if c == phase else (steps, 0)
                pairs.append(((y * 4 + x) * 2 + c, ((y + dy) % 4 * 4 + (x + dx) % 4) * 2 + c))
    return lax.ppermute(value, "chan", pairs)


def swap(value):
    return lax.ppermute(value, "chan", [(i, i ^ 1) for i in range(32)])


def later(value, steps):
    return lax.ppermute(value, "seq", [(i, i + steps) for i in range(8 - steps)])


def kernel(body, outs, n_in, smem=0, scratch=(), flops=0, place=True, inputs=None, last=pltpu.VMEM):
    inner = pl.pallas_call(
        body,
        out_shape=jax.tree.map(lambda o: pltpu.VMEM(o.shape, o.dtype), outs) if place else outs,
        in_specs=[pl.BlockSpec(memory_space=pltpu.SMEM)] * smem + [pl.BlockSpec(memory_space=pltpu.VMEM)] * (n_in - smem - 1)
        + [pl.BlockSpec(memory_space=last)],
        out_specs=jax.tree.map(lambda _: pl.BlockSpec(memory_space=pltpu.VMEM), outs),
        scratch_shapes=list(scratch),
        compiler_params=pltpu.CompilerParams(vmem_limit_bytes=16 * 1024 * 1024),
        cost_estimate=pl.CostEstimate(flops=flops, transcendentals=0, bytes_accessed=1 << 20),
    )

    def call(*args):
        spaces = inputs or (pltpu.VMEM,) * (n_in - smem)
        placed = [pltpu.with_memory_space_constraint(a, m) if m else a for a, m in zip(args[smem:], spaces)]
        return inner(*args[:smem], *placed)

    return call


def shape(dims, kind=F32):
    return jax.ShapeDtypeStruct(dims, kind)


def dot(a, b, precision=None):
    return jnp.dot(a, b, preferred_element_type=F32, precision=precision)


def eye(n):
    return lax.broadcasted_iota(jnp.int32, (n, n), 0) == lax.broadcasted_iota(jnp.int32, (n, n), 1)


def stand(row):
    return jnp.sum(jnp.where(eye(N), jnp.broadcast_to(row, (N, N)), 0.0), axis=1, keepdims=True)


def lay(column):
    return jnp.sum(jnp.where(eye(N), jnp.broadcast_to(column, (N, N)), 0.0), axis=0, keepdims=True)


def as_rows(column):
    return jnp.concatenate([lay(column[i * N : (i + 1) * N]) for i in range(4)], axis=0)


def as_column(rows):
    return jnp.concatenate([stand(rows[i : i + 1]) for i in range(4)], axis=0)


def half(index):
    return pl.ds(pl.multiple_of(index * HALF, HALF), HALF)


BLOCK = 2 * HALF + 3 * N


def own_body(pos, state_w, gain, tokens, out, sem):
    c, ci = pos[2], pos[3]
    copy = pltpu.make_async_copy(tokens.at[half(c)], out.at[:HALF], sem)
    copy.start()
    scaled = (state_w[...].astype(F32) * stand(gain[pl.ds(ci, 1)])).astype(BF16)
    for b in range(3):
        out[HALF + b * N : HALF + (b + 1) * N] = scaled[:, b * N : (b + 1) * N]
    copy.wait()


def block_body(pos, own, away, out):
    c = pos[2]
    out[half(c)] = own[:HALF]
    out[half(1 - c)] = away[half(c)]
    out[2 * HALF :] = own[HALF:]


def scale_body(gate, inner, gain, out):
    def step(i, _):
        rows = pl.ds(pl.multiple_of(i * N, N), N)
        column = stand(gain[pl.ds(i, 1)])
        out[rows, :CH] = (gate[rows].astype(F32) * column).astype(BF16)
        out[rows, CH:] = (inner[rows].astype(F32) * column).astype(BF16)
        return 0

    lax.fori_loop(0, 2 * 16, step, 0, unroll=4)


def mark_body(ref, out):
    out[...] = ref[:16]


def mark(piece):
    return kernel(mark_body, shape((16, N), BF16), 1)(piece)


def blocks_of(refs):
    found = []
    for ref in refs:
        found += [ref] if len(ref.shape) == 2 else [ref.at[0], ref.at[1]]
    return found


def pick_body(count):
    def body(*refs):
        for i, ref in enumerate(blocks_of(refs[:count])):
            refs[-1][i] = ref[2 * HALF :]

    return body


def pick(*pieces, marks=()):
    blocks = sum(1 if p.ndim == 2 else 2 for p in pieces)
    out = shape((blocks, 3 * N, N), BF16)
    return kernel(pick_body(len(pieces)), out, len(pieces) + len(marks))(*pieces, *marks)


def owner(pos, s, t):
    first = pos[2] == 0
    dy = jnp.where(first, s, t)
    dx = jnp.where(first, t, s)
    return ((pos[0] - dy) & 3) * 4 + ((pos[1] - dx) & 3)


STEP = 256


def add_slots(pos, slots, keep, got, acc, squares, fresh):
    def rows_of(r, _):
        rows = pl.ds(pl.multiple_of(r * STEP, STEP), STEP)
        low = pl.ds(pl.multiple_of(r * STEP, STEP), STEP)
        high = pl.ds(pl.multiple_of(HALF + r * STEP, STEP), STEP)
        square = None if fresh else squares[rows]
        for n, (s, blocks) in enumerate(slots):
            parts = []
            for ref in blocks:
                parts += [ref[low], ref[high]]
            for v in parts:
                v = v.astype(F32)
                square = v * v if square is None else square + v * v
            lhs = jnp.concatenate(parts, axis=1)
            ids = [pl.ds(pl.multiple_of(owner(pos, s, t) * 2 * N, 2 * N), 2 * N) for t in range(4)]
            for w, ref in enumerate((keep, got)):
                for b in range(2):
                    cols = slice(w * 2 * CH + b * CH, w * 2 * CH + (b + 1) * CH)
                    rhs = jnp.concatenate([ref[i, b * CH : (b + 1) * CH] for i in ids], axis=0)
                    part = dot(lhs, rhs)
                    if fresh and n == 0:
                        acc[rows, cols] = part
                    else:
                        acc[rows, cols] += part
        squares[rows] = square
        return 0

    lax.fori_loop(0, HALF // STEP, rows_of, 0)


def most_body(pos, *refs):
    blocks, (keep, got, acc, squares) = blocks_of(refs[:-4]), refs[-4:]
    slots = ((0, blocks[:4]), (1, blocks[4:8]), (3, blocks[8:]))
    add_slots(pos, slots, keep, got, acc, squares, True)


def most(pos, *parts):
    outs = (shape((HALF, 4 * CH)), shape((HALF, N)))
    return kernel(most_body, outs, len(parts) + 1, 1, (), 2 * HALF * 3072 * 1024)(pos, *parts)


def rest_body(pos, c0, c1, keep, got, acc, squares, own, send, scale):
    blocks = blocks_of((c0, c1))

    def rows_of(r, _):
        rows = pl.ds(pl.multiple_of(r * STEP, STEP), STEP)
        high = pl.ds(pl.multiple_of(HALF + r * STEP, STEP), STEP)
        square = squares[rows]
        parts = []
        for ref in blocks:
            parts += [ref[rows], ref[high]]
        for v in parts:
            v = v.astype(F32)
            square = square + v * v
        inverse = lax.rsqrt(jnp.sum(square, axis=1, keepdims=True) / D + EPS)
        scale[rows] = jnp.broadcast_to(inverse, (STEP, N))
        lhs = jnp.concatenate(parts, axis=1)
        ids = [pl.ds(pl.multiple_of(owner(pos, 2, t) * 2 * N, 2 * N), 2 * N) for t in range(4)]
        for w, (ref, out) in enumerate(((keep, own), (got, send))):
            for b in range(2):
                cols = slice(b * CH, (b + 1) * CH)
                rhs = jnp.concatenate([ref[i, cols] for i in ids], axis=0)
                part = acc[rows, w * 2 * CH + b * CH : w * 2 * CH + (b + 1) * CH] + dot(lhs, rhs)
                out[rows, cols] = (part * inverse).astype(BF16)
        return 0

    lax.fori_loop(0, HALF // STEP, rows_of, 0)


def rest(pos, *parts):
    outs = (shape((HALF, 2 * CH), BF16), shape((HALF, 2 * CH), BF16), shape((HALF, N)))
    return kernel(rest_body, outs, 7, 1, (), 2 * HALF * 1024 * 1024)(pos, *parts)


ORDER = (0, 1, 3, 2)


def state_sum(pos, blocks, most_own, most_got, last_own, last_got, slots, finish):
    c = pos[2]

    def rows_of(r, _):
        mine = pl.ds(pl.multiple_of(c * HALF + r * STEP, STEP), STEP)
        other = pl.ds(pl.multiple_of((1 - c) * HALF + r * STEP, STEP), STEP)
        lhs, w = [], [[], [], []]
        for g, k in slots:
            i = 4 * g + k
            lhs += [blocks[i][mine], blocks[i][other]]
            j = 4 * ORDER.index(k) + ORDER[g]
            for b in range(3):
                cut = slice(b * N, (b + 1) * N)
                w[b].append(most_own[i, cut] if i < 12 else last_own[i - 12, cut])
                w[b].append(most_got[j, cut] if j < 12 else last_got[j - 12, cut])
        lhs = jnp.concatenate(lhs, axis=1)
        w = [jnp.concatenate(v, axis=0) for v in w]
        finish(r, dot(lhs, jnp.concatenate(w[:2], axis=1)), dot(lhs, w[2]))
        return 0

    lax.fori_loop(0, HALF // STEP, rows_of, 0)


EARLY = [(g, k) for g in range(3) for k in (0, 1, 3)]
LATE = [(g, 2) for g in range(3)] + [(3, k) for k in range(4)]


def state_most_body(pos, *refs):
    blocks, (most_own, most_got, out) = blocks_of(refs[:-3]), refs[-3:]

    def finish(r, left, right):
        rows = pl.ds(pl.multiple_of(r * STEP, STEP), STEP)
        out[rows, : 2 * N] = left
        out[rows, 2 * N :] = right

    state_sum(pos, blocks, most_own, most_got, None, None, EARLY, finish)


def state_most(pos, *parts):
    call = kernel(state_most_body, shape((HALF, 3 * N)), len(parts) + 1, 1, (), 2 * HALF * 2304 * 384)
    return call(pos, *parts)


def state_body(pos, a23, p23, m2, c0, c1, most_own, most_got, last_own, last_got, acc, scale, out, send):
    ci = pos[3]

    def finish(r, left, right):
        rows = pl.ds(pl.multiple_of(r * STEP, STEP), STEP)
        inverse = scale[rows]
        out[rows, :N] = (acc[rows, :N] + left[:, :N]) * inverse
        out[rows, N : 2 * N] = (acc[rows, N : 2 * N] + left[:, N:]) * inverse
        rates = (acc[rows, 2 * N :] + right) * inverse
        lane = lax.broadcasted_iota(jnp.int32, (STEP, N), 1)
        out[rows, 2 * N :] = pltpu.roll(rates, (N - ci * HEADS) & (N - 1), 1)
        send[rows, : 2 * N] = out[rows, : 2 * N].astype(BF16)
        left = pltpu.roll(rates, (N - (ci ^ 1) * HEADS) & (N - 1), 1)
        packed = jnp.zeros((STEP, N), F32)
        for k in range(3):
            piece = left.astype(BF16).astype(F32)
            left = left - piece
            packed = jnp.where(lane // HEADS == k, pltpu.roll(piece, k * HEADS, 1), packed)
        send[rows, 2 * N :] = packed.astype(BF16)

    late = [None] * 12 + blocks_of((c0, c1))
    late[2], late[6], late[10] = a23.at[0], p23.at[0], m2
    state_sum(pos, late, most_own, most_got, last_own, last_got, LATE, finish)


def state_rest(pos, *parts):
    outs = (shape((HALF, 3 * N)), shape((HALF, 3 * N), BF16))
    return kernel(state_body, outs, 12, 1, (), 2 * HALF * 1792 * 384)(pos, *parts)


def silu(v):
    h = 0.5 * v
    return h + h * jnp.tanh(h)


def widen(columns, rows):
    return jnp.concatenate(
        [jnp.broadcast_to(columns[:, h : h + 1], (rows, P_SIZE)) for h in range(HEADS)], axis=1
    )


def convolve(window, taps):
    total = jnp.zeros((Q, CH), F32)
    for k in range(K):
        total = total + taps[k : k + 1] * window[5 + k : 5 + k + Q]
    return silu(total)


def fresh_state(values, b, w, step):
    scaled = (values * widen(jnp.exp(w[Q - 1 : Q] - w) * step, Q)).astype(BF16)
    return lax.dot_general(b, scaled, (((0,), (0,)), ((), ())), preferred_element_type=F32)


def values_body(pos, own_gi, got_gi, taps, values, head, pad):
    c = pos[2]
    for which, gi in ((c, own_gi), (1 - c, got_gi)):
        pad[pl.ds(pl.multiple_of(8 + which * HALF, 8), HALF)] = gi[:, CH:].astype(F32)

    def chunk(i, _):
        rows = pl.ds(pl.multiple_of(i * Q, Q), Q)
        values[rows] = convolve(pad[pl.ds(pl.multiple_of(i * Q, Q), Q + 8)], taps)
        return 0

    lax.fori_loop(1, CHUNKS, chunk, 0)
    head[...] = pad[8 : 8 + Q]


def values_of(pos, *parts):
    scratch = (pltpu.VMEM((ROWS + 8, CH), F32),)
    return kernel(values_body, (shape((ROWS, CH)), shape((Q, CH))), 4, 1, scratch)(pos, *parts)


def rows_body(
    pos, own_st, got_st, values, conv_state, small,
    in_map, out_map, within, until, step, fresh, head, pad, rate, passed,
):
    c = pos[2]
    for which, st in ((c, own_st), (1 - c, got_st)):
        pad[pl.ds(pl.multiple_of(8 + which * HALF, 8), HALF)] = st[:, : 2 * N].astype(F32)
        tail = st[:, 2 * N :].astype(F32)
        if st is got_st:
            tail = tail + (pltpu.roll(tail, N - HEADS, 1) + pltpu.roll(tail, N - 2 * HEADS, 1))
        rate[half(which)] = tail
    lane = lax.broadcasted_iota(jnp.int32, (Q, N), 1)
    lower = (
        lax.broadcasted_iota(jnp.int32, (Q, Q), 0) >= lax.broadcasted_iota(jnp.int32, (Q, Q), 1)
    ).astype(BF16)
    passed[...] = jnp.zeros((8, N), F32)

    def rates(i, _):
        rows = pl.ds(pl.multiple_of(i * Q, Q), Q)
        v = rate[rows] + small[0:1]
        soft = jnp.maximum(v, 0.0) + jnp.log1p(jnp.exp(-jnp.abs(v)))
        steps = jnp.where(lane < HEADS, soft, 0.0)
        step[rows] = steps
        left = steps * small[1:2]
        w = jnp.zeros((Q, N), F32)
        for _ in range(3):
            piece = left.astype(BF16)
            left = left - piece.astype(F32)
            w = w + dot(lower, piece)
        within[rows] = w
        before = passed[:1]
        until[rows] = w + before
        passed[:1] = before + w[Q - 1 : Q]
        return 0

    lax.fori_loop(0, CHUNKS, rates, 0)

    def chunk(i, _):
        rows = pl.ds(pl.multiple_of(i * Q, Q), Q)
        vs = convolve(pad[pl.ds(pl.multiple_of(i * Q, Q), Q + 8)], conv_state)
        b = vs[:, :N].astype(BF16)
        in_map[rows] = b
        out_map[rows] = vs[:, N:].astype(BF16)
        fresh[i] = fresh_state(values[rows], b, within[rows], step[rows])
        return 0

    lax.fori_loop(1, CHUNKS, chunk, 0)
    head[...] = pad[8 : 8 + Q]


def rows_of_all(pos, *parts):
    outs = (
        shape((ROWS, N), BF16),
        shape((ROWS, N), BF16),
        shape((ROWS, N)),
        shape((ROWS, N)),
        shape((ROWS, N)),
        shape((CHUNKS, N, CH)),
        shape((Q, CH)),
    )
    scratch = (pltpu.VMEM((ROWS + 8, CH), F32), pltpu.VMEM((ROWS, N), F32), pltpu.VMEM((8, N), F32))
    return kernel(rows_body, outs, 6, 1, scratch)(pos, *parts)


def write_packet(packet, state, log):
    high = log.astype(BF16)
    low = (log - high.astype(F32)).astype(BF16)
    packet[:N] = state.astype(BF16)
    packet[N:] = jnp.concatenate([high, low, jnp.zeros((14, CH), BF16)], axis=0)


def read_packets(packets):
    state = jnp.zeros((N, CH), F32)
    log = jnp.zeros((1, CH), F32)
    for p in packets:
        state = state + jnp.exp(log) * p[:N].astype(F32)
        tail = p[N:].astype(F32)
        log = log + (tail[0:1] + tail[1:2])
    return state, log


def three_body(own, p1, p2, out):
    write_packet(out, *read_packets((own, p1, p2)))


def three(*packets):
    return kernel(three_body, shape((N + 16, CH), BF16), 3)(*packets)


def scan_body(
    rim, within, until, step, fresh, head_s, head_i, conv_inner, conv_state,
    new_values, new_in, new_out, entering, packet,
):
    vi = convolve(jnp.concatenate([rim[:, :CH], head_i[...]], axis=0), conv_inner)
    vs = convolve(jnp.concatenate([rim[:, CH:], head_s[...]], axis=0), conv_state)
    b = vs[:, :N].astype(BF16)
    new_values[...] = vi
    new_in[...] = b
    new_out[...] = vs[:, N:].astype(BF16)
    carry = fresh_state(vi, b, within[:Q], step[:Q])
    entering[0] = jnp.zeros((N, CH), BF16)
    for i in range(1, CHUNKS):
        entering[i] = carry.astype(BF16)
        end = (i + 1) * Q
        carry = widen(jnp.exp(within[end - 1 : end]), 1) * carry + fresh[i]
    total = widen(until[ROWS - 1 : ROWS], 1)
    write_packet(packet, carry, total)


def scan(*parts):
    outs = (
        shape((Q, CH)),
        shape((Q, N), BF16),
        shape((Q, N), BF16),
        shape((CHUNKS, N, CH), BF16),
        shape((N + 16, CH), BF16),
    )
    return kernel(scan_body, outs, 9)(*parts)


def inside_body(
    pos, own_gi, got_gi, values, in_map, out_map, within, step, new_values, new_in, new_out, entering, small,
    result, opened, out_all, gate,
):
    c = pos[2]
    skip = widen(small[2:3], 1)
    gate[half(c)] = own_gi[:, :CH]
    gate[half(1 - c)] = got_gi[:, :CH]
    lower = lax.broadcasted_iota(jnp.int32, (Q, Q), 0) >= lax.broadcasted_iota(jnp.int32, (Q, Q), 1)

    def chunk(i, _):
        rows = pl.ds(pl.multiple_of(i * Q, Q), Q)
        opened[rows] = silu(gate[rows].astype(F32))
        head = i == 0
        vi = jnp.where(head, new_values[...], values[rows])
        b = jnp.where(head, new_in[...].astype(F32), in_map[rows].astype(F32)).astype(BF16)
        out = jnp.where(head, new_out[...].astype(F32), out_map[rows].astype(F32)).astype(BF16)
        out_all[rows] = out
        w = within[rows]
        scores = lax.dot_general(out, b, (((1,), (1,)), ((), ())), preferred_element_type=F32)
        flat = w.T
        stepped = (vi * widen(step[rows], Q)).astype(BF16)
        parts = []
        for h in range(HEADS):
            gap = w[:, h : h + 1] - flat[h : h + 1]
            mixing = (scores * jnp.exp(jnp.where(lower, gap, -jnp.inf))).astype(BF16)
            parts.append(dot(mixing, stepped[:, h * P_SIZE : (h + 1) * P_SIZE]))
        local = jnp.concatenate(parts, axis=1)
        local = local + dot(out, entering[i]) * widen(jnp.exp(w), Q)
        result[rows] = local + skip * vi
        return 0

    lax.fori_loop(0, CHUNKS, chunk, 0)


def inside(pos, *parts):
    outs = (shape((ROWS, CH)), shape((ROWS, CH)), shape((ROWS, N), BF16))
    return kernel(inside_body, outs, 13, 1, (pltpu.VMEM((ROWS, CH), BF16),))(pos, *parts)


def edge_body(pos, own_gi, got_gi, own_st, got_st, out):
    second = pos[2] == 1
    last = slice(HALF - 16, HALF)
    inner = jnp.where(second, own_gi[last, CH:].astype(F32), got_gi[last, CH:].astype(F32))
    out[:, :CH] = inner[8:]
    state = jnp.where(second, own_st[last, : 2 * N], got_st[last, : 2 * N].astype(F32))
    out[:, CH:] = state[8:]


def split(energy):
    high = energy.astype(BF16)
    return high, (energy - high.astype(F32)).astype(BF16)


def gated_body(pos, p1, p2, e3, e6, local, opened, out_map, until, gate_gain, own, send, energy):
    c = pos[2]
    carried = read_packets((p1, p2, e3, e6))[0].astype(BF16)
    for which, to in ((1 - c, send), (c, own)):
        rows = half(which)
        out = local[rows] + dot(out_map[rows], carried) * widen(jnp.exp(until[rows]), HALF)
        out = out * opened[rows]
        to[:HALF] = (out * gate_gain[...]).astype(BF16)
        e = as_rows(jnp.sum(out * out, axis=1, keepdims=True))
        if to is own:
            energy[...] = jnp.concatenate([e, jnp.zeros((4, N), F32)], axis=0)
        else:
            e = jnp.concatenate(split(e), axis=1)
            to[HALF:] = jnp.concatenate([e, jnp.zeros((12, CH), BF16)], axis=0)


def gated(pos, *parts):
    outs = (shape((HALF, CH), BF16), shape((HALF + 16, CH), BF16), shape((8, N)))
    return kernel(gated_body, outs, 10, 1)(pos, *parts)


TALL = 2 * HALF + 16


def energy_rows(energy):
    return jnp.concatenate([*split(energy), jnp.zeros((8, N), BF16)], axis=0)


def stack_body(own, got, out):
    out[:CH] = own[...]
    out[CH:] = got[...]


def pair_energy(got, energy):
    tail = got[HALF:].astype(F32)
    return energy[:4] + (tail[:4, :N] + tail[:4, N:])


def product(pos, own, got, weights, s, t):
    first = pos[2] == 0
    dy = jnp.where(first, t, s)
    dx = jnp.where(first, s, t)
    chip = ((pos[0] + dy) & 3) * 4 + ((pos[1] + dx) & 3)
    cols = pl.ds(pl.multiple_of(chip * 2 * N, 2 * N), 2 * N)
    return dot(jnp.concatenate([own[...], got[:HALF]], axis=1), weights[:, cols])


def spread_body(specs, adds):
    def body(pos, own, got, energy, weights, *refs):
        extra, outs = refs[:adds], refs[adds:]
        for n, (s, pair) in enumerate(specs):
            tail = pair_energy(got, energy)
            if adds:
                rows = extra[n][0, 2 * HALF :].astype(F32)
                tail = tail + (rows[:4] + rows[4:8])
            tail = energy_rows(tail)
            for k, t in enumerate(pair):
                part = product(pos, own, got, weights, s, t)
                for side in range(2):
                    rows = slice(side * HALF, (side + 1) * HALF)
                    value = part[:, side * N : (side + 1) * N]
                    if adds:
                        value = value + extra[n][k, rows].astype(F32)
                    outs[n][k, rows] = value.astype(BF16)
                outs[n][k, 2 * HALF :] = tail

    return body


def spread(pos, specs, parts, extra=()):
    outs = tuple(shape((2, TALL, N), BF16) for _ in specs)
    count = len(extra)
    flops = 2 * HALF * 512 * 512 * len(specs)
    return kernel(spread_body(specs, count), outs, 5 + count, 1, (), flops)(pos, *parts, *extra)


def keep_body(pos, own, got, energy, weights, out, tail):
    for t in range(4):
        part = product(pos, own, got, weights, 0, t)
        out[t, :HALF] = part[:, :N]
        out[t, HALF:] = part[:, N:]
    tail[...] = jnp.concatenate([pair_energy(got, energy), jnp.zeros((4, N), F32)], axis=0)


def half_sum_body(own, tail, u_plus, d_minus, d_plus, u_minus, q0, q1, q2, q3):
    for t, q in enumerate((q0, q1, q2, q3)):
        x, y = ((u_plus, d_minus), (d_plus, u_minus))[t // 2]
        k = t % 2
        value = own[t] + x[k, : 2 * HALF].astype(F32) + y[k, : 2 * HALF].astype(F32)
        q[: 2 * HALF] = value.astype(q.dtype)
        e = x[k, 2 * HALF :].astype(F32) + y[k, 2 * HALF :].astype(F32)
        e = tail[:4] + (e[:4] + e[4:8])
        if q.dtype == BF16:
            q[2 * HALF :] = energy_rows(e)
        else:
            q[2 * HALF :] = jnp.concatenate([e, jnp.zeros((12, N), F32)], axis=0)


def half_sum(*parts):
    outs = (shape((TALL, N)),) + (shape((TALL, N), BF16),) * 3
    return kernel(half_sum_body, outs, 6)(*parts)


def total_body(pos, v0, v1, v2, v3, own, send):
    c = pos[2]
    e = v0[2 * HALF :] + v1[2 * HALF :].astype(F32) + v2[2 * HALF :].astype(F32) + v3[2 * HALF :].astype(F32)
    scale = lax.rsqrt(as_column(e[:4] + e[4:8]) / DI + EPS)
    for which, to in ((1 - c, send), (c, own)):
        rows = half(which)
        to[...] = (v0[rows] + v1[rows].astype(F32) + v2[rows].astype(F32) + v3[rows].astype(F32)) * scale


def total(pos, *parts):
    return kernel(total_body, (shape((HALF, N)), shape((HALF, N))), 5, 1)(pos, *parts)


def finish_body(pos, tokens, own, got, out):
    c = pos[2]
    for which, part in ((c, own), (1 - c, got)):
        rows = half(which)
        out[rows] = (tokens[rows].astype(F32) + part[...]).astype(BF16)


def finish(pos, *parts):
    return kernel(finish_body, shape((ROWS, N), BF16), 4, 1, place=False)(pos, *parts)


def local(
    tokens,
    norm_gain,
    gate_proj,
    inner_proj,
    state_proj,
    conv_inner,
    conv_state,
    log_rate,
    rate_bias,
    skip_gain,
    gate_gain,
    out_proj,
):
    ci = lax.axis_index("chan")
    core = ci & 1
    pos = jnp.stack([ci >> 3, (ci >> 1) & 3, core, ci]).astype(jnp.int32)
    gain = norm_gain.reshape(32, N)

    small = jnp.pad(jnp.stack([rate_bias, -jnp.exp(log_rate), skip_gain]), ((0, 5), (0, N - HEADS)))

    away_tokens = swap(tokens)
    sem = (pltpu.SemaphoreType.DMA,)
    own_block = kernel(
        own_body, shape((HALF + 3 * N, N), BF16), 4, 1, sem, inputs=(pltpu.HBM,) * 3, last=pl.ANY
    )(pos, state_proj, gain, tokens)
    block = kernel(block_body, shape((BLOCK, N), BF16), 3, 1)(pos, own_block, away_tokens)

    n1, n3 = plane_move(block, 1, 0), plane_move(block, -1, 0)
    p0, m0 = plane_move(block, 1, 1), plane_move(block, -1, 1)
    p1, m3 = plane_move(n1, 1, 1), plane_move(n3, -1, 1)
    low = plane_move(n1[: BLOCK // 2], 1, 0)
    high = plane_move(n3[BLOCK // 2 :], -1, 0)
    m1 = plane_move(n1, -1, 1)
    n2 = jnp.concatenate([low, high], axis=0)
    a23 = jnp.stack([n2, n3])
    p23, m2 = plane_move(a23, 1, 1), plane_move(n2, -1, 1)
    c0 = plane_move(jnp.stack([p0, p1]), 1, 1)
    c1 = plane_move(jnp.stack([m2, m3]), -1, 1)
    mark1 = mark(p1)
    mark2 = mark(m2)
    early = (block, n1, a23, p0, p1, p23, m0, m1, m2, m3)

    keep = kernel(scale_body, shape((D, 2 * CH), BF16), 3)(gate_proj, inner_proj, gain)
    got = swap(keep)
    got_w = swap(out_proj)

    most_own = pick(*early, marks=(mark1, mark2))
    most_got = swap(most_own)
    acc, squares = most(pos, *early, keep, got)
    acc_st = state_most(pos, *early, most_own, most_got)
    w_all = kernel(stack_body, shape((2 * CH, D), BF16), 2)(out_proj, got_w)
    last_own = pick(c0, c1)
    last_got = swap(last_own)
    own_gi, send_gi, scale = rest(pos, c0, c1, keep, got, acc, squares)
    got_gi = swap(send_gi)
    own_st, send_st = state_rest(pos, a23, p23, m2, c0, c1, most_own, most_got, last_own, last_got, acc_st, scale)
    got_st = swap(send_st)

    edge = kernel(edge_body, shape((8, 2 * CH)), 5, 1)(pos, own_gi, got_gi, own_st, got_st)
    rim = later(edge, 1)

    values, head = values_of(pos, own_gi, got_gi, conv_inner)
    in_map, out_map, within, until, step, *fresh = rows_of_all(pos, own_st, got_st, values, conv_state, small)
    *new, entering, packet = scan(
        rim, within, until, step, *fresh, head, conv_inner, conv_state
    )
    p2, p1 = later(packet, 2), later(packet, 1)
    window = three(packet, p1, p2)
    e6, e3 = later(window, 6), later(window, 3)
    result, opened, out_all = inside(pos, own_gi, got_gi, values, in_map, out_map, within, step, *new, entering, small)
    own_g, send_g, energy = gated(pos, p1, p2, e3, e6, result, opened, out_all, until, gate_gain[None])

    got_g = swap(send_g)
    parts = (own_g, got_g, energy, w_all)
    far_low, far_high = spread(pos, ((2, (0, 1)), (2, (2, 3))), parts)
    t_plus, t_minus = plane_move(far_low, 1, 0), plane_move(far_high, -1, 0)
    near_plus, near_minus = spread(pos, ((1, (2, 3)), (3, (0, 1))), parts)
    d_plus, d_minus = plane_move(near_plus, 1, 0), plane_move(near_minus, -1, 0)
    keep_outs = (shape((4, 2 * HALF, N)), shape((8, N)))
    kept, tail = kernel(keep_body, keep_outs, 5, 1, (), 2 * HALF * 512 * 1024)(pos, *parts)
    (on_plus,) = spread(pos, ((1, (0, 1)),), parts, (t_plus,))
    u_plus = plane_move(on_plus, 1, 0)
    (on_minus,) = spread(pos, ((3, (2, 3)),), parts, (t_minus,))
    u_minus = plane_move(on_minus, -1, 0)
    q = half_sum(kept, tail, u_plus, d_minus, d_plus, u_minus)
    last = [q[0]] + [plane_move(q[t], t, 1) for t in (1, 2, 3)]
    own, send = total(pos, *last)
    return finish(pos, tokens, own, swap(send))


def solution(mesh):
    return jax.shard_map(
        local,
        mesh=mesh,
        in_specs=(
            P("seq", "chan"),
            P(),
            P(None, "chan"),
            P(None, "chan"),
            P("chan", None),
            P(None, "chan"),
            P(),
            P("chan"),
            P("chan"),
            P("chan"),
            P("chan"),
            P("chan", None),
        ),
        out_specs=P("seq", "chan"),
        check_vma=False,
    )
```

```python
import jax
import jax.numpy as jnp
from jax import lax
from jax.experimental import pallas as pl
from jax.experimental.pallas import tpu as pltpu
from jax.sharding import PartitionSpec as P


D = 4096
DI = 8192
N = 128
P_SIZE = 64
K = 4
Q = 256
ROWS = 1024
HALF = 512
CHUNKS = 4
HEADS = 4
CH = 256
EPS = 1e-05
F32 = jnp.float32
BF16 = jnp.bfloat16


def plane_move(value, steps, phase):
    pairs = []
    for y in range(4):
        for x in range(4):
            for c in range(2):
                dy, dx = (0, steps) if c == phase else (steps, 0)
                pairs.append(((y * 4 + x) * 2 + c, ((y + dy) % 4 * 4 + (x + dx) % 4) * 2 + c))
    return lax.ppermute(value, "chan", pairs)


def swap(value):
    return lax.ppermute(value, "chan", [(i, i ^ 1) for i in range(32)])


def later(value, steps):
    return lax.ppermute(value, "seq", [(i, i + steps) for i in range(8 - steps)])


def kernel(body, outs, n_in, smem=0, scratch=(), flops=0, place=True, inputs=None, last=pltpu.VMEM):
    inner = pl.pallas_call(
        body,
        out_shape=jax.tree.map(lambda o: pltpu.VMEM(o.shape, o.dtype), outs) if place else outs,
        in_specs=[pl.BlockSpec(memory_space=pltpu.SMEM)] * smem + [pl.BlockSpec(memory_space=pltpu.VMEM)] * (n_in - smem - 1)
        + [pl.BlockSpec(memory_space=last)],
        out_specs=jax.tree.map(lambda _: pl.BlockSpec(memory_space=pltpu.VMEM), outs),
        scratch_shapes=list(scratch),
        compiler_params=pltpu.CompilerParams(vmem_limit_bytes=16 * 1024 * 1024),
        cost_estimate=pl.CostEstimate(flops=flops, transcendentals=0, bytes_accessed=1 << 20),
    )

    def call(*args):
        spaces = inputs or (pltpu.VMEM,) * (n_in - smem)
        placed = [pltpu.with_memory_space_constraint(a, m) if m else a for a, m in zip(args[smem:], spaces)]
        return inner(*args[:smem], *placed)

    return call


def shape(dims, kind=F32):
    return jax.ShapeDtypeStruct(dims, kind)


def dot(a, b, precision=None):
    return jnp.dot(a, b, preferred_element_type=F32, precision=precision)


def eye(n):
    return lax.broadcasted_iota(jnp.int32, (n, n), 0) == lax.broadcasted_iota(jnp.int32, (n, n), 1)


def stand(row):
    return jnp.sum(jnp.where(eye(N), jnp.broadcast_to(row, (N, N)), 0.0), axis=1, keepdims=True)


def lay(column):
    return jnp.sum(jnp.where(eye(N), jnp.broadcast_to(column, (N, N)), 0.0), axis=0, keepdims=True)


def as_rows(column):
    return jnp.concatenate([lay(column[i * N : (i + 1) * N]) for i in range(4)], axis=0)


def as_column(rows):
    return jnp.concatenate([stand(rows[i : i + 1]) for i in range(4)], axis=0)


def half(index):
    return pl.ds(pl.multiple_of(index * HALF, HALF), HALF)


BLOCK = 2 * HALF + 3 * N


def own_body(pos, state_w, gain, tokens, out, sem):
    c, ci = pos[2], pos[3]
    copy = pltpu.make_async_copy(tokens.at[half(c)], out.at[:HALF], sem)
    copy.start()
    scaled = (state_w[...].astype(F32) * stand(gain[pl.ds(ci, 1)])).astype(BF16)
    for b in range(3):
        out[HALF + b * N : HALF + (b + 1) * N] = scaled[:, b * N : (b + 1) * N]
    copy.wait()


def block_body(pos, own, away, out):
    c = pos[2]
    out[half(c)] = own[:HALF]
    out[half(1 - c)] = away[half(c)]
    out[2 * HALF :] = own[HALF:]


def scale_body(weight, gain, out):
    def step(i, _):
        rows = pl.ds(pl.multiple_of(i * N, N), N)
        out[rows] = (weight[rows].astype(F32) * stand(gain[pl.ds(i, 1)])).astype(BF16)
        return 0

    lax.fori_loop(0, 2 * 16, step, 0, unroll=4)


def mark_body(ref, out):
    out[...] = ref[:16]


def mark(piece):
    return kernel(mark_body, shape((16, N), BF16), 1)(piece)


def blocks_of(refs):
    found = []
    for ref in refs:
        found += [ref] if len(ref.shape) == 2 else [ref.at[0], ref.at[1]]
    return found


def pick_body(count):
    def body(*refs):
        for i, ref in enumerate(blocks_of(refs[:count])):
            refs[-1][i] = ref[2 * HALF :]

    return body


def pick(*pieces, marks=()):
    blocks = sum(1 if p.ndim == 2 else 2 for p in pieces)
    out = shape((blocks, 3 * N, N), BF16)
    return kernel(pick_body(len(pieces)), out, len(pieces) + len(marks))(*pieces, *marks)


def owner(pos, s, t):
    first = pos[2] == 0
    dy = jnp.where(first, s, t)
    dx = jnp.where(first, t, s)
    return ((pos[0] - dy) & 3) * 4 + ((pos[1] - dx) & 3)


STEP = 256


def add_slots(pos, slots, weights, acc, squares, fresh):
    def rows_of(r, _):
        rows = pl.ds(pl.multiple_of(r * STEP, STEP), STEP)
        low = pl.ds(pl.multiple_of(r * STEP, STEP), STEP)
        high = pl.ds(pl.multiple_of(HALF + r * STEP, STEP), STEP)
        square = None if fresh else squares[rows]
        for n, (s, blocks) in enumerate(slots):
            parts = []
            for ref in blocks:
                parts += [ref[low], ref[high]]
            for v in parts:
                v = v.astype(F32)
                square = v * v if square is None else square + v * v
            lhs = jnp.concatenate(parts, axis=1)
            ids = [pl.ds(pl.multiple_of(owner(pos, s, t) * 2 * N, 2 * N), 2 * N) for t in range(4)]
            for w, ref in enumerate(weights):
                cols = slice(w * CH, (w + 1) * CH)
                part = dot(lhs, jnp.concatenate([ref[i] for i in ids], axis=0))
                if fresh and n == 0:
                    acc[rows, cols] = part
                else:
                    acc[rows, cols] += part
        squares[rows] = square
        return 0

    lax.fori_loop(0, HALF // STEP, rows_of, 0)


def most_body(pos, *refs):
    blocks, weights, (acc, squares) = blocks_of(refs[:-6]), refs[-6:-2], refs[-2:]
    slots = ((0, blocks[:4]), (1, blocks[4:8]), (3, blocks[8:]))
    add_slots(pos, slots, weights, acc, squares, True)


def most(pos, *parts):
    outs = (shape((HALF, 4 * CH)), shape((HALF, N)))
    return kernel(most_body, outs, len(parts) + 1, 1, (), 2 * HALF * 3072 * 1024)(pos, *parts)


def rest_body(pos, c0, c1, w0, w1, w2, w3, acc, squares, own, send, scale):
    blocks = blocks_of((c0, c1))

    def rows_of(r, _):
        rows = pl.ds(pl.multiple_of(r * STEP, STEP), STEP)
        high = pl.ds(pl.multiple_of(HALF + r * STEP, STEP), STEP)
        square = squares[rows]
        parts = []
        for ref in blocks:
            parts += [ref[rows], ref[high]]
        for v in parts:
            v = v.astype(F32)
            square = square + v * v
        inverse = lax.rsqrt(jnp.sum(square, axis=1, keepdims=True) / D + EPS)
        scale[rows] = jnp.broadcast_to(inverse, (STEP, N))
        lhs = jnp.concatenate(parts, axis=1)
        ids = [pl.ds(pl.multiple_of(owner(pos, 2, t) * 2 * N, 2 * N), 2 * N) for t in range(4)]
        for w, ref in enumerate((w0, w1, w2, w3)):
            out = (own, send)[w // 2]
            cols = slice(w % 2 * CH, (w % 2 + 1) * CH)
            rhs = jnp.concatenate([ref[i] for i in ids], axis=0)
            part = acc[rows, w * CH : (w + 1) * CH] + dot(lhs, rhs)
            out[rows, cols] = (part * inverse).astype(BF16)
        return 0

    lax.fori_loop(0, HALF // STEP, rows_of, 0)


def rest(pos, *parts):
    outs = (shape((HALF, 2 * CH), BF16), shape((HALF, 2 * CH), BF16), shape((HALF, N)))
    return kernel(rest_body, outs, 9, 1, (), 2 * HALF * 1024 * 1024)(pos, *parts)


ORDER = (0, 1, 3, 2)


def state_sum(pos, blocks, most_own, most_got, last_own, last_got, slots, finish):
    c = pos[2]

    def rows_of(r, _):
        mine = pl.ds(pl.multiple_of(c * HALF + r * STEP, STEP), STEP)
        other = pl.ds(pl.multiple_of((1 - c) * HALF + r * STEP, STEP), STEP)
        lhs, w = [], [[], [], []]
        for g, k in slots:
            i = 4 * g + k
            lhs += [blocks[i][mine], blocks[i][other]]
            j = 4 * ORDER.index(k) + ORDER[g]
            for b in range(3):
                cut = slice(b * N, (b + 1) * N)
                w[b].append(most_own[i, cut] if i < 12 else last_own[i - 12, cut])
                w[b].append(most_got[j, cut] if j < 12 else last_got[j - 12, cut])
        lhs = jnp.concatenate(lhs, axis=1)
        w = [jnp.concatenate(v, axis=0) for v in w]
        finish(r, dot(lhs, jnp.concatenate(w[:2], axis=1)), dot(lhs, w[2]))
        return 0

    lax.fori_loop(0, HALF // STEP, rows_of, 0)


EARLY = [(g, k) for g in range(3) for k in (0, 1, 3)]
LATE = [(g, 2) for g in range(3)] + [(3, k) for k in range(4)]


def state_most_body(pos, *refs):
    blocks, (most_own, most_got, out) = blocks_of(refs[:-3]), refs[-3:]

    def finish(r, left, right):
        rows = pl.ds(pl.multiple_of(r * STEP, STEP), STEP)
        out[rows, : 2 * N] = left
        out[rows, 2 * N :] = right

    state_sum(pos, blocks, most_own, most_got, None, None, EARLY, finish)


def state_most(pos, *parts):
    call = kernel(state_most_body, shape((HALF, 3 * N)), len(parts) + 1, 1, (), 2 * HALF * 2304 * 384)
    return call(pos, *parts)


def state_body(pos, a23, p23, m2, c0, c1, most_own, most_got, last_own, last_got, acc, scale, out, send):
    ci = pos[3]

    def finish(r, left, right):
        rows = pl.ds(pl.multiple_of(r * STEP, STEP), STEP)
        inverse = scale[rows]
        out[rows, :N] = (acc[rows, :N] + left[:, :N]) * inverse
        out[rows, N : 2 * N] = (acc[rows, N : 2 * N] + left[:, N:]) * inverse
        rates = (acc[rows, 2 * N :] + right) * inverse
        lane = lax.broadcasted_iota(jnp.int32, (STEP, N), 1)
        out[rows, 2 * N :] = pltpu.roll(rates, (N - ci * HEADS) & (N - 1), 1)
        send[rows, : 2 * N] = out[rows, : 2 * N].astype(BF16)
        left = pltpu.roll(rates, (N - (ci ^ 1) * HEADS) & (N - 1), 1)
        packed = jnp.zeros((STEP, N), F32)
        for k in range(3):
            piece = left.astype(BF16).astype(F32)
            left = left - piece
            packed = jnp.where(lane // HEADS == k, pltpu.roll(piece, k * HEADS, 1), packed)
        send[rows, 2 * N :] = packed.astype(BF16)

    late = [None] * 12 + blocks_of((c0, c1))
    late[2], late[6], late[10] = a23.at[0], p23.at[0], m2
    state_sum(pos, late, most_own, most_got, last_own, last_got, LATE, finish)


def state_rest(pos, *parts):
    outs = (shape((HALF, 3 * N)), shape((HALF, 3 * N), BF16))
    return kernel(state_body, outs, 12, 1, (), 2 * HALF * 1792 * 384)(pos, *parts)


def silu(v):
    h = 0.5 * v
    return h + h * jnp.tanh(h)


def widen(columns, rows):
    return jnp.concatenate(
        [jnp.broadcast_to(columns[:, h : h + 1], (rows, P_SIZE)) for h in range(HEADS)], axis=1
    )


def convolve(window, taps):
    total = jnp.zeros((Q, CH), F32)
    for k in range(K):
        total = total + taps[k : k + 1] * window[5 + k : 5 + k + Q]
    return silu(total)


def fresh_state(values, b, w, step):
    scaled = (values * widen(jnp.exp(w[Q - 1 : Q] - w) * step, Q)).astype(BF16)
    return lax.dot_general(b, scaled, (((0,), (0,)), ((), ())), preferred_element_type=F32)


def values_body(pos, own_gi, got_gi, taps, values, head, pad):
    c = pos[2]
    for which, gi in ((c, own_gi), (1 - c, got_gi)):
        pad[pl.ds(pl.multiple_of(8 + which * HALF, 8), HALF)] = gi[:, CH:].astype(F32)

    def chunk(i, _):
        rows = pl.ds(pl.multiple_of(i * Q, Q), Q)
        values[rows] = convolve(pad[pl.ds(pl.multiple_of(i * Q, Q), Q + 8)], taps)
        return 0

    lax.fori_loop(1, CHUNKS, chunk, 0)
    head[...] = pad[8 : 8 + Q]


def values_of(pos, *parts):
    scratch = (pltpu.VMEM((ROWS + 8, CH), F32),)
    return kernel(values_body, (shape((ROWS, CH)), shape((Q, CH))), 4, 1, scratch)(pos, *parts)


def rows_body(
    pos, own_st, got_st, values, conv_state, small,
    in_map, out_map, within, until, step, fresh, head, pad, rate, passed,
):
    c = pos[2]
    for which, st in ((c, own_st), (1 - c, got_st)):
        pad[pl.ds(pl.multiple_of(8 + which * HALF, 8), HALF)] = st[:, : 2 * N].astype(F32)
        tail = st[:, 2 * N :].astype(F32)
        if st is got_st:
            tail = tail + (pltpu.roll(tail, N - HEADS, 1) + pltpu.roll(tail, N - 2 * HEADS, 1))
        rate[half(which)] = tail
    lane = lax.broadcasted_iota(jnp.int32, (Q, N), 1)
    lower = (
        lax.broadcasted_iota(jnp.int32, (Q, Q), 0) >= lax.broadcasted_iota(jnp.int32, (Q, Q), 1)
    ).astype(BF16)
    passed[...] = jnp.zeros((8, N), F32)

    def rates(i, _):
        rows = pl.ds(pl.multiple_of(i * Q, Q), Q)
        v = rate[rows] + small[0:1]
        soft = jnp.maximum(v, 0.0) + jnp.log1p(jnp.exp(-jnp.abs(v)))
        steps = jnp.where(lane < HEADS, soft, 0.0)
        step[rows] = steps
        left = steps * small[1:2]
        w = jnp.zeros((Q, N), F32)
        for _ in range(3):
            piece = left.astype(BF16)
            left = left - piece.astype(F32)
            w = w + dot(lower, piece)
        within[rows] = w
        before = passed[:1]
        until[rows] = w + before
        passed[:1] = before + w[Q - 1 : Q]
        return 0

    lax.fori_loop(0, CHUNKS, rates, 0)

    def chunk(i, _):
        rows = pl.ds(pl.multiple_of(i * Q, Q), Q)
        vs = convolve(pad[pl.ds(pl.multiple_of(i * Q, Q), Q + 8)], conv_state)
        b = vs[:, :N].astype(BF16)
        in_map[rows] = b
        out_map[rows] = vs[:, N:].astype(BF16)
        fresh[i] = fresh_state(values[rows], b, within[rows], step[rows])
        return 0

    lax.fori_loop(1, CHUNKS, chunk, 0)
    head[...] = pad[8 : 8 + Q]


def rows_of_all(pos, *parts):
    outs = (
        shape((ROWS, N), BF16),
        shape((ROWS, N), BF16),
        shape((ROWS, N)),
        shape((ROWS, N)),
        shape((ROWS, N)),
        shape((CHUNKS, N, CH)),
        shape((Q, CH)),
    )
    scratch = (pltpu.VMEM((ROWS + 8, CH), F32), pltpu.VMEM((ROWS, N), F32), pltpu.VMEM((8, N), F32))
    return kernel(rows_body, outs, 6, 1, scratch)(pos, *parts)


def write_packet(packet, state, log):
    high = log.astype(BF16)
    low = (log - high.astype(F32)).astype(BF16)
    packet[:N] = state.astype(BF16)
    packet[N:] = jnp.concatenate([high, low, jnp.zeros((14, CH), BF16)], axis=0)


def read_packets(packets):
    state = jnp.zeros((N, CH), F32)
    log = jnp.zeros((1, CH), F32)
    for p in packets:
        state = state + jnp.exp(log) * p[:N].astype(F32)
        tail = p[N:].astype(F32)
        log = log + (tail[0:1] + tail[1:2])
    return state, log


def three_body(own, p1, p2, out):
    write_packet(out, *read_packets((own, p1, p2)))


def three(*packets):
    return kernel(three_body, shape((N + 16, CH), BF16), 3)(*packets)


def scan_body(
    rim, within, until, step, fresh, head_s, head_i, conv_inner, conv_state,
    new_values, new_in, new_out, entering, packet,
):
    vi = convolve(jnp.concatenate([rim[:, :CH], head_i[...]], axis=0), conv_inner)
    vs = convolve(jnp.concatenate([rim[:, CH:], head_s[...]], axis=0), conv_state)
    b = vs[:, :N].astype(BF16)
    new_values[...] = vi
    new_in[...] = b
    new_out[...] = vs[:, N:].astype(BF16)
    carry = fresh_state(vi, b, within[:Q], step[:Q])
    entering[0] = jnp.zeros((N, CH), BF16)
    for i in range(1, CHUNKS):
        entering[i] = carry.astype(BF16)
        end = (i + 1) * Q
        carry = widen(jnp.exp(within[end - 1 : end]), 1) * carry + fresh[i]
    total = widen(until[ROWS - 1 : ROWS], 1)
    write_packet(packet, carry, total)


def scan(*parts):
    outs = (
        shape((Q, CH)),
        shape((Q, N), BF16),
        shape((Q, N), BF16),
        shape((CHUNKS, N, CH), BF16),
        shape((N + 16, CH), BF16),
    )
    return kernel(scan_body, outs, 9)(*parts)


def inside_body(
    pos, own_gi, got_gi, values, in_map, out_map, within, step, new_values, new_in, new_out, entering, small,
    result, opened, out_all, gate,
):
    c = pos[2]
    skip = widen(small[2:3], 1)
    gate[half(c)] = own_gi[:, :CH]
    gate[half(1 - c)] = got_gi[:, :CH]
    lower = lax.broadcasted_iota(jnp.int32, (Q, Q), 0) >= lax.broadcasted_iota(jnp.int32, (Q, Q), 1)

    def chunk(i, _):
        rows = pl.ds(pl.multiple_of(i * Q, Q), Q)
        opened[rows] = silu(gate[rows].astype(F32))
        head = i == 0
        vi = jnp.where(head, new_values[...], values[rows])
        b = jnp.where(head, new_in[...].astype(F32), in_map[rows].astype(F32)).astype(BF16)
        out = jnp.where(head, new_out[...].astype(F32), out_map[rows].astype(F32)).astype(BF16)
        out_all[rows] = out
        w = within[rows]
        scores = lax.dot_general(out, b, (((1,), (1,)), ((), ())), preferred_element_type=F32)
        flat = w.T
        stepped = (vi * widen(step[rows], Q)).astype(BF16)
        parts = []
        for h in range(HEADS):
            gap = w[:, h : h + 1] - flat[h : h + 1]
            mixing = (scores * jnp.exp(jnp.where(lower, gap, -jnp.inf))).astype(BF16)
            parts.append(dot(mixing, stepped[:, h * P_SIZE : (h + 1) * P_SIZE]))
        local = jnp.concatenate(parts, axis=1)
        local = local + dot(out, entering[i]) * widen(jnp.exp(w), Q)
        result[rows] = local + skip * vi
        return 0

    lax.fori_loop(0, CHUNKS, chunk, 0)


def inside(pos, *parts):
    outs = (shape((ROWS, CH)), shape((ROWS, CH)), shape((ROWS, N), BF16))
    return kernel(inside_body, outs, 13, 1, (pltpu.VMEM((ROWS, CH), BF16),))(pos, *parts)


def edge_body(pos, own_gi, got_gi, own_st, got_st, out):
    second = pos[2] == 1
    last = slice(HALF - 16, HALF)
    inner = jnp.where(second, own_gi[last, CH:].astype(F32), got_gi[last, CH:].astype(F32))
    out[:, :CH] = inner[8:]
    state = jnp.where(second, own_st[last, : 2 * N], got_st[last, : 2 * N].astype(F32))
    out[:, CH:] = state[8:]


def split(energy):
    high = energy.astype(BF16)
    return high, (energy - high.astype(F32)).astype(BF16)


def gated_body(pos, p1, p2, e3, e6, local, opened, out_map, until, gate_gain, own, send, energy):
    c = pos[2]
    carried = read_packets((p1, p2, e3, e6))[0].astype(BF16)
    for which, to in ((1 - c, send), (c, own)):
        rows = half(which)
        out = local[rows] + dot(out_map[rows], carried) * widen(jnp.exp(until[rows]), HALF)
        out = out * opened[rows]
        to[:HALF] = (out * gate_gain[...]).astype(BF16)
        e = as_rows(jnp.sum(out * out, axis=1, keepdims=True))
        if to is own:
            energy[...] = jnp.concatenate([e, jnp.zeros((4, N), F32)], axis=0)
        else:
            e = jnp.concatenate(split(e), axis=1)
            to[HALF:] = jnp.concatenate([e, jnp.zeros((12, CH), BF16)], axis=0)


def gated(pos, *parts):
    outs = (shape((HALF, CH), BF16), shape((HALF + 16, CH), BF16), shape((8, N)))
    return kernel(gated_body, outs, 10, 1)(pos, *parts)


TALL = 2 * HALF + 16


def energy_rows(energy):
    return jnp.concatenate([*split(energy), jnp.zeros((8, N), BF16)], axis=0)


def stack_body(own, got, out):
    out[:CH] = own[...]
    out[CH:] = got[...]


def pair_energy(got, energy):
    tail = got[HALF:].astype(F32)
    return energy[:4] + (tail[:4, :N] + tail[:4, N:])


def product(pos, own, got, weights, s, t):
    first = pos[2] == 0
    dy = jnp.where(first, t, s)
    dx = jnp.where(first, s, t)
    chip = ((pos[0] + dy) & 3) * 4 + ((pos[1] + dx) & 3)
    cols = pl.ds(pl.multiple_of(chip * 2 * N, 2 * N), 2 * N)
    return dot(jnp.concatenate([own[...], got[:HALF]], axis=1), weights[:, cols])


def spread_body(specs, adds):
    def body(pos, own, got, energy, weights, *refs):
        extra, outs = refs[:adds], refs[adds:]
        for n, (s, pair) in enumerate(specs):
            tail = pair_energy(got, energy)
            if adds:
                rows = extra[n][0, 2 * HALF :].astype(F32)
                tail = tail + (rows[:4] + rows[4:8])
            tail = energy_rows(tail)
            for k, t in enumerate(pair):
                part = product(pos, own, got, weights, s, t)
                for side in range(2):
                    rows = slice(side * HALF, (side + 1) * HALF)
                    value = part[:, side * N : (side + 1) * N]
                    if adds:
                        value = value + extra[n][k, rows].astype(F32)
                    outs[n][k, rows] = value.astype(BF16)
                outs[n][k, 2 * HALF :] = tail

    return body


def spread(pos, specs, parts, extra=()):
    outs = tuple(shape((2, TALL, N), BF16) for _ in specs)
    count = len(extra)
    flops = 2 * HALF * 512 * 512 * len(specs)
    return kernel(spread_body(specs, count), outs, 5 + count, 1, (), flops)(pos, *parts, *extra)


def keep_body(pos, own, got, energy, weights, out, tail):
    for t in range(4):
        part = product(pos, own, got, weights, 0, t)
        out[t, :HALF] = part[:, :N]
        out[t, HALF:] = part[:, N:]
    tail[...] = jnp.concatenate([pair_energy(got, energy), jnp.zeros((4, N), F32)], axis=0)


def half_sum_body(own, tail, u_plus, d_minus, d_plus, u_minus, q0, q1, q2, q3):
    for t, q in enumerate((q0, q1, q2, q3)):
        x, y = ((u_plus, d_minus), (d_plus, u_minus))[t // 2]
        k = t % 2
        value = own[t] + x[k, : 2 * HALF].astype(F32) + y[k, : 2 * HALF].astype(F32)
        q[: 2 * HALF] = value.astype(q.dtype)
        e = x[k, 2 * HALF :].astype(F32) + y[k, 2 * HALF :].astype(F32)
        e = tail[:4] + (e[:4] + e[4:8])
        if q.dtype == BF16:
            q[2 * HALF :] = energy_rows(e)
        else:
            q[2 * HALF :] = jnp.concatenate([e, jnp.zeros((12, N), F32)], axis=0)


def half_sum(*parts):
    outs = (shape((TALL, N)),) + (shape((TALL, N), BF16),) * 3
    return kernel(half_sum_body, outs, 6)(*parts)


def total_body(pos, v0, v1, v2, v3, own, send):
    c = pos[2]
    e = v0[2 * HALF :] + v1[2 * HALF :].astype(F32) + v2[2 * HALF :].astype(F32) + v3[2 * HALF :].astype(F32)
    scale = lax.rsqrt(as_column(e[:4] + e[4:8]) / DI + EPS)
    for which, to in ((1 - c, send), (c, own)):
        rows = half(which)
        to[...] = (v0[rows] + v1[rows].astype(F32) + v2[rows].astype(F32) + v3[rows].astype(F32)) * scale


def total(pos, *parts):
    return kernel(total_body, (shape((HALF, N)), shape((HALF, N))), 5, 1)(pos, *parts)


def finish_body(pos, tokens, own, got, out):
    c = pos[2]
    for which, part in ((c, own), (1 - c, got)):
        rows = half(which)
        out[rows] = (tokens[rows].astype(F32) + part[...]).astype(BF16)


def finish(pos, *parts):
    return kernel(finish_body, shape((ROWS, N), BF16), 4, 1, place=False)(pos, *parts)


def local(
    tokens,
    norm_gain,
    gate_proj,
    inner_proj,
    state_proj,
    conv_inner,
    conv_state,
    log_rate,
    rate_bias,
    skip_gain,
    gate_gain,
    out_proj,
):
    ci = lax.axis_index("chan")
    core = ci & 1
    pos = jnp.stack([ci >> 3, (ci >> 1) & 3, core, ci]).astype(jnp.int32)
    gain = norm_gain.reshape(32, N)

    small = jnp.pad(jnp.stack([rate_bias, -jnp.exp(log_rate), skip_gain]), ((0, 5), (0, N - HEADS)))

    away_tokens = swap(tokens)
    sem = (pltpu.SemaphoreType.DMA,)
    own_block = kernel(
        own_body, shape((HALF + 3 * N, N), BF16), 4, 1, sem, inputs=(pltpu.HBM,) * 3, last=pl.ANY
    )(pos, state_proj, gain, tokens)
    block = kernel(block_body, shape((BLOCK, N), BF16), 3, 1)(pos, own_block, away_tokens)

    n1, n3 = plane_move(block, 1, 0), plane_move(block, -1, 0)
    p0, m0 = plane_move(block, 1, 1), plane_move(block, -1, 1)
    p1, m3 = plane_move(n1, 1, 1), plane_move(n3, -1, 1)
    low = plane_move(n1[: BLOCK // 2], 1, 0)
    high = plane_move(n3[BLOCK // 2 :], -1, 0)
    m1 = plane_move(n1, -1, 1)
    n2 = jnp.concatenate([low, high], axis=0)
    a23 = jnp.stack([n2, n3])
    p23, m2 = plane_move(a23, 1, 1), plane_move(n2, -1, 1)
    c0 = plane_move(jnp.stack([p0, p1]), 1, 1)
    c1 = plane_move(jnp.stack([m2, m3]), -1, 1)
    mark1 = mark(p1)
    mark2 = mark(m2)
    early = (block, n1, a23, p0, p1, p23, m0, m1, m2, m3)

    scale_weight = kernel(scale_body, shape((D, CH), BF16), 2)
    keep_g = scale_weight(gate_proj, gain)
    keep_i = scale_weight(inner_proj, gain)
    weights = (keep_g, keep_i, swap(keep_g), swap(keep_i))
    got_w = swap(out_proj)

    most_own = pick(*early, marks=(mark1, mark2))
    most_got = swap(most_own)
    acc, squares = most(pos, *early, *weights)
    acc_st = state_most(pos, *early, most_own, most_got)
    w_all = kernel(stack_body, shape((2 * CH, D), BF16), 2)(out_proj, got_w)
    last_own = pick(c0, c1)
    last_got = swap(last_own)
    own_gi, send_gi, scale = rest(pos, c0, c1, *weights, acc, squares)
    got_gi = swap(send_gi)
    own_st, send_st = state_rest(pos, a23, p23, m2, c0, c1, most_own, most_got, last_own, last_got, acc_st, scale)
    got_st = swap(send_st)

    edge = kernel(edge_body, shape((8, 2 * CH)), 5, 1)(pos, own_gi, got_gi, own_st, got_st)
    rim = later(edge, 1)

    values, head = values_of(pos, own_gi, got_gi, conv_inner)
    in_map, out_map, within, until, step, *fresh = rows_of_all(pos, own_st, got_st, values, conv_state, small)
    *new, entering, packet = scan(
        rim, within, until, step, *fresh, head, conv_inner, conv_state
    )
    p2, p1 = later(packet, 2), later(packet, 1)
    window = three(packet, p1, p2)
    e6, e3 = later(window, 6), later(window, 3)
    result, opened, out_all = inside(pos, own_gi, got_gi, values, in_map, out_map, within, step, *new, entering, small)
    own_g, send_g, energy = gated(pos, p1, p2, e3, e6, result, opened, out_all, until, gate_gain[None])

    got_g = swap(send_g)
    parts = (own_g, got_g, energy, w_all)
    far_low, far_high = spread(pos, ((2, (0, 1)), (2, (2, 3))), parts)
    t_plus, t_minus = plane_move(far_low, 1, 0), plane_move(far_high, -1, 0)
    near_plus, near_minus = spread(pos, ((1, (2, 3)), (3, (0, 1))), parts)
    d_plus, d_minus = plane_move(near_plus, 1, 0), plane_move(near_minus, -1, 0)
    keep_outs = (shape((4, 2 * HALF, N)), shape((8, N)))
    kept, tail = kernel(keep_body, keep_outs, 5, 1, (), 2 * HALF * 512 * 1024)(pos, *parts)
    (on_plus,) = spread(pos, ((1, (0, 1)),), parts, (t_plus,))
    u_plus = plane_move(on_plus, 1, 0)
    (on_minus,) = spread(pos, ((3, (2, 3)),), parts, (t_minus,))
    u_minus = plane_move(on_minus, -1, 0)
    q = half_sum(kept, tail, u_plus, d_minus, d_plus, u_minus)
    last = [q[0]] + [plane_move(q[t], t, 1) for t in (1, 2, 3)]
    own, send = total(pos, *last)
    return finish(pos, tokens, own, swap(send))


def solution(mesh):
    return jax.shard_map(
        local,
        mesh=mesh,
        in_specs=(
            P("seq", "chan"),
            P(),
            P(None, "chan"),
            P(None, "chan"),
            P("chan", None),
            P(None, "chan"),
            P(),
            P("chan"),
            P("chan"),
            P("chan"),
            P("chan"),
            P("chan", None),
        ),
        out_specs=P("seq", "chan"),
        check_vma=False,
    )
```

```python
import jax
import jax.numpy as jnp
from jax import lax
from jax.experimental import pallas as pl
from jax.experimental.pallas import tpu as pltpu
from jax.sharding import PartitionSpec as P


D = 4096
DI = 8192
N = 128
P_SIZE = 64
K = 4
Q = 256
ROWS = 1024
HALF = 512
CHUNKS = 4
HEADS = 4
CH = 256
EPS = 1e-05
F32 = jnp.float32
BF16 = jnp.bfloat16


def plane_move(value, steps, phase):
    pairs = []
    for y in range(4):
        for x in range(4):
            for c in range(2):
                dy, dx = (0, steps) if c == phase else (steps, 0)
                pairs.append(((y * 4 + x) * 2 + c, ((y + dy) % 4 * 4 + (x + dx) % 4) * 2 + c))
    return lax.ppermute(value, "chan", pairs)


def swap(value):
    return lax.ppermute(value, "chan", [(i, i ^ 1) for i in range(32)])


def later(value, steps):
    return lax.ppermute(value, "seq", [(i, i + steps) for i in range(8 - steps)])


def kernel(body, outs, n_in, smem=0, scratch=(), flops=0, place=True, inputs=None, last=pltpu.VMEM):
    inner = pl.pallas_call(
        body,
        out_shape=jax.tree.map(lambda o: pltpu.VMEM(o.shape, o.dtype), outs) if place else outs,
        in_specs=[pl.BlockSpec(memory_space=pltpu.SMEM)] * smem + [pl.BlockSpec(memory_space=pltpu.VMEM)] * (n_in - smem - 1)
        + [pl.BlockSpec(memory_space=last)],
        out_specs=jax.tree.map(lambda _: pl.BlockSpec(memory_space=pltpu.VMEM), outs),
        scratch_shapes=list(scratch),
        compiler_params=pltpu.CompilerParams(vmem_limit_bytes=16 * 1024 * 1024),
        cost_estimate=pl.CostEstimate(flops=flops, transcendentals=0, bytes_accessed=1 << 20),
    )

    def call(*args):
        spaces = inputs or (pltpu.VMEM,) * (n_in - smem)
        placed = [pltpu.with_memory_space_constraint(a, m) if m else a for a, m in zip(args[smem:], spaces)]
        return inner(*args[:smem], *placed)

    return call


def shape(dims, kind=F32):
    return jax.ShapeDtypeStruct(dims, kind)


def dot(a, b, precision=None):
    return jnp.dot(a, b, preferred_element_type=F32, precision=precision)


def eye(n):
    return lax.broadcasted_iota(jnp.int32, (n, n), 0) == lax.broadcasted_iota(jnp.int32, (n, n), 1)


def stand(row):
    return jnp.sum(jnp.where(eye(N), jnp.broadcast_to(row, (N, N)), 0.0), axis=1, keepdims=True)


def lay(column):
    return jnp.sum(jnp.where(eye(N), jnp.broadcast_to(column, (N, N)), 0.0), axis=0, keepdims=True)


def as_rows(column):
    return jnp.concatenate([lay(column[i * N : (i + 1) * N]) for i in range(4)], axis=0)


def as_column(rows):
    return jnp.concatenate([stand(rows[i : i + 1]) for i in range(4)], axis=0)


def half(index):
    return pl.ds(pl.multiple_of(index * HALF, HALF), HALF)


BLOCK = 2 * HALF + 3 * N


def own_body(pos, state_w, gain, tokens, out, sem):
    c, ci = pos[2], pos[3]
    copy = pltpu.make_async_copy(tokens.at[half(c)], out.at[:HALF], sem)
    copy.start()
    scaled = (state_w[...].astype(F32) * stand(gain[pl.ds(ci, 1)])).astype(BF16)
    for b in range(3):
        out[HALF + b * N : HALF + (b + 1) * N] = scaled[:, b * N : (b + 1) * N]
    copy.wait()


def block_body(pos, own, away, out):
    c = pos[2]
    out[half(c)] = own[:HALF]
    out[half(1 - c)] = away[half(c)]
    out[2 * HALF :] = own[HALF:]


def scale_body(gate, inner, gain, out):
    def step(i, _):
        rows = pl.ds(pl.multiple_of(i * N, N), N)
        column = stand(gain[pl.ds(i, 1)])
        out[rows, :CH] = (gate[rows].astype(F32) * column).astype(BF16)
        out[rows, CH:] = (inner[rows].astype(F32) * column).astype(BF16)
        return 0

    lax.fori_loop(0, 2 * 16, step, 0, unroll=4)


def mark_body(ref, out):
    out[...] = ref[:16]


def mark(piece):
    return kernel(mark_body, shape((16, N), BF16), 1)(piece)


def blocks_of(refs):
    found = []
    for ref in refs:
        found += [ref] if len(ref.shape) == 2 else [ref.at[0], ref.at[1]]
    return found


def pick_body(count):
    def body(*refs):
        for i, ref in enumerate(blocks_of(refs[:count])):
            refs[-1][i] = ref[2 * HALF :]

    return body


def pick(*pieces, marks=()):
    blocks = sum(1 if p.ndim == 2 else 2 for p in pieces)
    out = shape((blocks, 3 * N, N), BF16)
    return kernel(pick_body(len(pieces)), out, len(pieces) + len(marks))(*pieces, *marks)


def owner(pos, s, t):
    first = pos[2] == 0
    dy = jnp.where(first, s, t)
    dx = jnp.where(first, t, s)
    return ((pos[0] - dy) & 3) * 4 + ((pos[1] - dx) & 3)


STEP = 256


def add_slots(pos, slots, keep, got, acc, squares, fresh):
    def rows_of(r, _):
        rows = pl.ds(pl.multiple_of(r * STEP, STEP), STEP)
        low = pl.ds(pl.multiple_of(r * STEP, STEP), STEP)
        high = pl.ds(pl.multiple_of(HALF + r * STEP, STEP), STEP)
        square = None if fresh else squares[rows]
        for n, (s, blocks) in enumerate(slots):
            parts = []
            for ref in blocks:
                parts += [ref[low], ref[high]]
            for v in parts:
                v = v.astype(F32)
                square = v * v if square is None else square + v * v
            lhs = jnp.concatenate(parts, axis=1)
            ids = [pl.ds(pl.multiple_of(owner(pos, s, t) * 2 * N, 2 * N), 2 * N) for t in range(4)]
            for w, ref in enumerate((keep, got)):
                for b in range(2):
                    cols = slice(w * 2 * CH + b * CH, w * 2 * CH + (b + 1) * CH)
                    rhs = jnp.concatenate([ref[i, b * CH : (b + 1) * CH] for i in ids], axis=0)
                    part = dot(lhs, rhs)
                    if fresh and n == 0:
                        acc[rows, cols] = part
                    else:
                        acc[rows, cols] += part
        squares[rows] = square
        return 0

    lax.fori_loop(0, HALF // STEP, rows_of, 0)


def most_body(pos, *refs):
    blocks, (keep, got, acc, squares) = blocks_of(refs[:-4]), refs[-4:]
    slots = ((0, blocks[:4]), (1, blocks[4:8]), (3, blocks[8:]))
    add_slots(pos, slots, keep, got, acc, squares, True)


def most(pos, *parts):
    outs = (shape((HALF, 4 * CH)), shape((HALF, N)))
    return kernel(most_body, outs, len(parts) + 1, 1, (), 2 * HALF * 3072 * 1024)(pos, *parts)


def more_body(pos, c0, keep, got, acc_in, squares_in, acc, squares):
    blocks = blocks_of((c0,))

    def rows_of(r, _):
        rows = pl.ds(pl.multiple_of(r * STEP, STEP), STEP)
        high = pl.ds(pl.multiple_of(HALF + r * STEP, STEP), STEP)
        parts = []
        for ref in blocks:
            parts += [ref[rows], ref[high]]
        square = squares_in[rows]
        for v in parts:
            v = v.astype(F32)
            square = square + v * v
        squares[rows] = square
        lhs = jnp.concatenate(parts, axis=1)
        ids = [pl.ds(pl.multiple_of(owner(pos, 2, t) * 2 * N, 2 * N), 2 * N) for t in (0, 1)]
        for w, ref in enumerate((keep, got)):
            for b in range(2):
                cols = slice(w * 2 * CH + b * CH, w * 2 * CH + (b + 1) * CH)
                rhs = jnp.concatenate([ref[i, b * CH : (b + 1) * CH] for i in ids], axis=0)
                acc[rows, cols] = acc_in[rows, cols] + dot(lhs, rhs)
        return 0

    lax.fori_loop(0, HALF // STEP, rows_of, 0)


def more(pos, *parts):
    outs = (shape((HALF, 4 * CH)), shape((HALF, N)))
    return kernel(more_body, outs, 6, 1, (), 2 * HALF * 512 * 1024)(pos, *parts)


def rest_body(pos, c1, keep, got, acc, squares, own, send, scale):
    blocks = blocks_of((c1,))

    def rows_of(r, _):
        rows = pl.ds(pl.multiple_of(r * STEP, STEP), STEP)
        high = pl.ds(pl.multiple_of(HALF + r * STEP, STEP), STEP)
        square = squares[rows]
        parts = []
        for ref in blocks:
            parts += [ref[rows], ref[high]]
        for v in parts:
            v = v.astype(F32)
            square = square + v * v
        inverse = lax.rsqrt(jnp.sum(square, axis=1, keepdims=True) / D + EPS)
        scale[rows] = jnp.broadcast_to(inverse, (STEP, N))
        lhs = jnp.concatenate(parts, axis=1)
        ids = [pl.ds(pl.multiple_of(owner(pos, 2, t) * 2 * N, 2 * N), 2 * N) for t in (2, 3)]
        for w, (ref, out) in enumerate(((keep, own), (got, send))):
            for b in range(2):
                cols = slice(b * CH, (b + 1) * CH)
                rhs = jnp.concatenate([ref[i, cols] for i in ids], axis=0)
                part = acc[rows, w * 2 * CH + b * CH : w * 2 * CH + (b + 1) * CH] + dot(lhs, rhs)
                out[rows, cols] = (part * inverse).astype(BF16)
        return 0

    lax.fori_loop(0, HALF // STEP, rows_of, 0)


def rest(pos, *parts):
    outs = (shape((HALF, 2 * CH), BF16), shape((HALF, 2 * CH), BF16), shape((HALF, N)))
    return kernel(rest_body, outs, 6, 1, (), 2 * HALF * 512 * 1024)(pos, *parts)


ORDER = (0, 1, 3, 2)


def state_sum(pos, blocks, most_own, most_got, last_own, last_got, slots, finish):
    c = pos[2]

    def rows_of(r, _):
        mine = pl.ds(pl.multiple_of(c * HALF + r * STEP, STEP), STEP)
        other = pl.ds(pl.multiple_of((1 - c) * HALF + r * STEP, STEP), STEP)
        lhs, w = [], [[], [], []]
        for g, k in slots:
            i = 4 * g + k
            lhs += [blocks[i][mine], blocks[i][other]]
            j = 4 * ORDER.index(k) + ORDER[g]
            for b in range(3):
                cut = slice(b * N, (b + 1) * N)
                w[b].append(most_own[i, cut] if i < 12 else last_own[i - 12, cut])
                w[b].append(most_got[j, cut] if j < 12 else last_got[j - 12, cut])
        lhs = jnp.concatenate(lhs, axis=1)
        w = [jnp.concatenate(v, axis=0) for v in w]
        finish(r, dot(lhs, jnp.concatenate(w[:2], axis=1)), dot(lhs, w[2]))
        return 0

    lax.fori_loop(0, HALF // STEP, rows_of, 0)


EARLY = [(g, k) for g in range(3) for k in (0, 1, 3)]
LATE = [(g, 2) for g in range(3)] + [(3, k) for k in range(4)]


def state_most_body(pos, *refs):
    blocks, (most_own, most_got, out) = blocks_of(refs[:-3]), refs[-3:]

    def finish(r, left, right):
        rows = pl.ds(pl.multiple_of(r * STEP, STEP), STEP)
        out[rows, : 2 * N] = left
        out[rows, 2 * N :] = right

    state_sum(pos, blocks, most_own, most_got, None, None, EARLY, finish)


def state_most(pos, *parts):
    call = kernel(state_most_body, shape((HALF, 3 * N)), len(parts) + 1, 1, (), 2 * HALF * 2304 * 384)
    return call(pos, *parts)


def state_body(pos, a23, p23, m2, c0, c1, most_own, most_got, last_own, last_got, acc, scale, out, send):
    ci = pos[3]

    def finish(r, left, right):
        rows = pl.ds(pl.multiple_of(r * STEP, STEP), STEP)
        inverse = scale[rows]
        out[rows, :N] = (acc[rows, :N] + left[:, :N]) * inverse
        out[rows, N : 2 * N] = (acc[rows, N : 2 * N] + left[:, N:]) * inverse
        rates = (acc[rows, 2 * N :] + right) * inverse
        lane = lax.broadcasted_iota(jnp.int32, (STEP, N), 1)
        out[rows, 2 * N :] = pltpu.roll(rates, (N - ci * HEADS) & (N - 1), 1)
        send[rows, : 2 * N] = out[rows, : 2 * N].astype(BF16)
        left = pltpu.roll(rates, (N - (ci ^ 1) * HEADS) & (N - 1), 1)
        packed = jnp.zeros((STEP, N), F32)
        for k in range(3):
            piece = left.astype(BF16).astype(F32)
            left = left - piece
            packed = jnp.where(lane // HEADS == k, pltpu.roll(piece, k * HEADS, 1), packed)
        send[rows, 2 * N :] = packed.astype(BF16)

    late = [None] * 12 + blocks_of((c0, c1))
    late[2], late[6], late[10] = a23.at[0], p23.at[0], m2
    state_sum(pos, late, most_own, most_got, last_own, last_got, LATE, finish)


def state_rest(pos, *parts):
    outs = (shape((HALF, 3 * N)), shape((HALF, 3 * N), BF16))
    return kernel(state_body, outs, 12, 1, (), 2 * HALF * 1792 * 384)(pos, *parts)


def silu(v):
    h = 0.5 * v
    return h + h * jnp.tanh(h)


def widen(columns, rows):
    return jnp.concatenate(
        [jnp.broadcast_to(columns[:, h : h + 1], (rows, P_SIZE)) for h in range(HEADS)], axis=1
    )


def convolve(window, taps):
    total = jnp.zeros((Q, CH), F32)
    for k in range(K):
        total = total + taps[k : k + 1] * window[5 + k : 5 + k + Q]
    return silu(total)


def fresh_state(values, b, w, step):
    scaled = (values * widen(jnp.exp(w[Q - 1 : Q] - w) * step, Q)).astype(BF16)
    return lax.dot_general(b, scaled, (((0,), (0,)), ((), ())), preferred_element_type=F32)


def values_body(pos, own_gi, got_gi, taps, values, head, pad):
    c = pos[2]
    for which, gi in ((c, own_gi), (1 - c, got_gi)):
        pad[pl.ds(pl.multiple_of(8 + which * HALF, 8), HALF)] = gi[:, CH:].astype(F32)

    def chunk(i, _):
        rows = pl.ds(pl.multiple_of(i * Q, Q), Q)
        values[rows] = convolve(pad[pl.ds(pl.multiple_of(i * Q, Q), Q + 8)], taps)
        return 0

    lax.fori_loop(1, CHUNKS, chunk, 0)
    head[...] = pad[8 : 8 + Q]


def values_of(pos, *parts):
    scratch = (pltpu.VMEM((ROWS + 8, CH), F32),)
    return kernel(values_body, (shape((ROWS, CH)), shape((Q, CH))), 4, 1, scratch)(pos, *parts)


def rows_body(
    pos, own_st, got_st, values, conv_state, small,
    in_map, out_map, within, until, step, fresh, head, pad, rate, passed,
):
    c = pos[2]
    for which, st in ((c, own_st), (1 - c, got_st)):
        pad[pl.ds(pl.multiple_of(8 + which * HALF, 8), HALF)] = st[:, : 2 * N].astype(F32)
        tail = st[:, 2 * N :].astype(F32)
        if st is got_st:
            tail = tail + (pltpu.roll(tail, N - HEADS, 1) + pltpu.roll(tail, N - 2 * HEADS, 1))
        rate[half(which)] = tail
    lane = lax.broadcasted_iota(jnp.int32, (Q, N), 1)
    lower = (
        lax.broadcasted_iota(jnp.int32, (Q, Q), 0) >= lax.broadcasted_iota(jnp.int32, (Q, Q), 1)
    ).astype(BF16)
    passed[...] = jnp.zeros((8, N), F32)

    def rates(i, _):
        rows = pl.ds(pl.multiple_of(i * Q, Q), Q)
        v = rate[rows] + small[0:1]
        soft = jnp.maximum(v, 0.0) + jnp.log1p(jnp.exp(-jnp.abs(v)))
        steps = jnp.where(lane < HEADS, soft, 0.0)
        step[rows] = steps
        left = steps * small[1:2]
        w = jnp.zeros((Q, N), F32)
        for _ in range(3):
            piece = left.astype(BF16)
            left = left - piece.astype(F32)
            w = w + dot(lower, piece)
        within[rows] = w
        before = passed[:1]
        until[rows] = w + before
        passed[:1] = before + w[Q - 1 : Q]
        return 0

    lax.fori_loop(0, CHUNKS, rates, 0)

    def chunk(i, _):
        rows = pl.ds(pl.multiple_of(i * Q, Q), Q)
        vs = convolve(pad[pl.ds(pl.multiple_of(i * Q, Q), Q + 8)], conv_state)
        b = vs[:, :N].astype(BF16)
        in_map[rows] = b
        out_map[rows] = vs[:, N:].astype(BF16)
        fresh[i] = fresh_state(values[rows], b, within[rows], step[rows])
        return 0

    lax.fori_loop(1, CHUNKS, chunk, 0)
    head[...] = pad[8 : 8 + Q]


def rows_of_all(pos, *parts):
    outs = (
        shape((ROWS, N), BF16),
        shape((ROWS, N), BF16),
        shape((ROWS, N)),
        shape((ROWS, N)),
        shape((ROWS, N)),
        shape((CHUNKS, N, CH)),
        shape((Q, CH)),
    )
    scratch = (pltpu.VMEM((ROWS + 8, CH), F32), pltpu.VMEM((ROWS, N), F32), pltpu.VMEM((8, N), F32))
    return kernel(rows_body, outs, 6, 1, scratch)(pos, *parts)


def write_packet(packet, state, log):
    high = log.astype(BF16)
    low = (log - high.astype(F32)).astype(BF16)
    packet[:N] = state.astype(BF16)
    packet[N:] = jnp.concatenate([high, low, jnp.zeros((14, CH), BF16)], axis=0)


def read_packets(packets):
    state = jnp.zeros((N, CH), F32)
    log = jnp.zeros((1, CH), F32)
    for p in packets:
        state = state + jnp.exp(log) * p[:N].astype(F32)
        tail = p[N:].astype(F32)
        log = log + (tail[0:1] + tail[1:2])
    return state, log


def three_body(own, p1, p2, out):
    write_packet(out, *read_packets((own, p1, p2)))


def three(*packets):
    return kernel(three_body, shape((N + 16, CH), BF16), 3)(*packets)


def scan_body(
    rim, within, until, step, fresh, head_s, head_i, conv_inner, conv_state,
    new_values, new_in, new_out, entering, packet,
):
    vi = convolve(jnp.concatenate([rim[:, :CH], head_i[...]], axis=0), conv_inner)
    vs = convolve(jnp.concatenate([rim[:, CH:], head_s[...]], axis=0), conv_state)
    b = vs[:, :N].astype(BF16)
    new_values[...] = vi
    new_in[...] = b
    new_out[...] = vs[:, N:].astype(BF16)
    carry = fresh_state(vi, b, within[:Q], step[:Q])
    entering[0] = jnp.zeros((N, CH), BF16)
    for i in range(1, CHUNKS):
        entering[i] = carry.astype(BF16)
        end = (i + 1) * Q
        carry = widen(jnp.exp(within[end - 1 : end]), 1) * carry + fresh[i]
    total = widen(until[ROWS - 1 : ROWS], 1)
    write_packet(packet, carry, total)


def scan(*parts):
    outs = (
        shape((Q, CH)),
        shape((Q, N), BF16),
        shape((Q, N), BF16),
        shape((CHUNKS, N, CH), BF16),
        shape((N + 16, CH), BF16),
    )
    return kernel(scan_body, outs, 9)(*parts)


def inside_body(
    pos, own_gi, got_gi, values, in_map, out_map, within, step, new_values, new_in, new_out, entering, small,
    result, opened, out_all, gate,
):
    c = pos[2]
    skip = widen(small[2:3], 1)
    gate[half(c)] = own_gi[:, :CH]
    gate[half(1 - c)] = got_gi[:, :CH]
    lower = lax.broadcasted_iota(jnp.int32, (Q, Q), 0) >= lax.broadcasted_iota(jnp.int32, (Q, Q), 1)

    def chunk(i, _):
        rows = pl.ds(pl.multiple_of(i * Q, Q), Q)
        opened[rows] = silu(gate[rows].astype(F32))
        head = i == 0
        vi = jnp.where(head, new_values[...], values[rows])
        b = jnp.where(head, new_in[...].astype(F32), in_map[rows].astype(F32)).astype(BF16)
        out = jnp.where(head, new_out[...].astype(F32), out_map[rows].astype(F32)).astype(BF16)
        out_all[rows] = out
        w = within[rows]
        scores = lax.dot_general(out, b, (((1,), (1,)), ((), ())), preferred_element_type=F32)
        flat = w.T
        stepped = (vi * widen(step[rows], Q)).astype(BF16)
        parts = []
        for h in range(HEADS):
            gap = w[:, h : h + 1] - flat[h : h + 1]
            mixing = (scores * jnp.exp(jnp.where(lower, gap, -jnp.inf))).astype(BF16)
            parts.append(dot(mixing, stepped[:, h * P_SIZE : (h + 1) * P_SIZE]))
        local = jnp.concatenate(parts, axis=1)
        local = local + dot(out, entering[i]) * widen(jnp.exp(w), Q)
        result[rows] = local + skip * vi
        return 0

    lax.fori_loop(0, CHUNKS, chunk, 0)


def inside(pos, *parts):
    outs = (shape((ROWS, CH)), shape((ROWS, CH)), shape((ROWS, N), BF16))
    return kernel(inside_body, outs, 13, 1, (pltpu.VMEM((ROWS, CH), BF16),))(pos, *parts)


def edge_body(pos, own_gi, got_gi, own_st, got_st, out):
    second = pos[2] == 1
    last = slice(HALF - 16, HALF)
    inner = jnp.where(second, own_gi[last, CH:].astype(F32), got_gi[last, CH:].astype(F32))
    out[:, :CH] = inner[8:]
    state = jnp.where(second, own_st[last, : 2 * N], got_st[last, : 2 * N].astype(F32))
    out[:, CH:] = state[8:]


def split(energy):
    high = energy.astype(BF16)
    return high, (energy - high.astype(F32)).astype(BF16)


def gated_body(pos, p1, p2, e3, e6, local, opened, out_map, until, gate_gain, own, send, energy):
    c = pos[2]
    carried = read_packets((p1, p2, e3, e6))[0].astype(BF16)
    for which, to in ((1 - c, send), (c, own)):
        rows = half(which)
        out = local[rows] + dot(out_map[rows], carried) * widen(jnp.exp(until[rows]), HALF)
        out = out * opened[rows]
        to[:HALF] = (out * gate_gain[...]).astype(BF16)
        e = as_rows(jnp.sum(out * out, axis=1, keepdims=True))
        if to is own:
            energy[...] = jnp.concatenate([e, jnp.zeros((4, N), F32)], axis=0)
        else:
            e = jnp.concatenate(split(e), axis=1)
            to[HALF:] = jnp.concatenate([e, jnp.zeros((12, CH), BF16)], axis=0)


def gated(pos, *parts):
    outs = (shape((HALF, CH), BF16), shape((HALF + 16, CH), BF16), shape((8, N)))
    return kernel(gated_body, outs, 10, 1)(pos, *parts)


TALL = 2 * HALF + 16


def energy_rows(energy):
    return jnp.concatenate([*split(energy), jnp.zeros((8, N), BF16)], axis=0)


def stack_body(own, got, out):
    out[:CH] = own[...]
    out[CH:] = got[...]


def pair_energy(got, energy):
    tail = got[HALF:].astype(F32)
    return energy[:4] + (tail[:4, :N] + tail[:4, N:])


def product(pos, own, got, weights, s, t):
    first = pos[2] == 0
    dy = jnp.where(first, t, s)
    dx = jnp.where(first, s, t)
    chip = ((pos[0] + dy) & 3) * 4 + ((pos[1] + dx) & 3)
    cols = pl.ds(pl.multiple_of(chip * 2 * N, 2 * N), 2 * N)
    return dot(jnp.concatenate([own[...], got[:HALF]], axis=1), weights[:, cols])


def spread_body(specs, adds):
    def body(pos, own, got, energy, weights, *refs):
        extra, outs = refs[:adds], refs[adds:]
        for n, (s, pair) in enumerate(specs):
            tail = pair_energy(got, energy)
            if adds:
                rows = extra[n][0, 2 * HALF :].astype(F32)
                tail = tail + (rows[:4] + rows[4:8])
            tail = energy_rows(tail)
            for k, t in enumerate(pair):
                part = product(pos, own, got, weights, s, t)
                for side in range(2):
                    rows = slice(side * HALF, (side + 1) * HALF)
                    value = part[:, side * N : (side + 1) * N]
                    if adds:
                        value = value + extra[n][k, rows].astype(F32)
                    outs[n][k, rows] = value.astype(BF16)
                outs[n][k, 2 * HALF :] = tail

    return body


def spread(pos, specs, parts, extra=()):
    outs = tuple(shape((2, TALL, N), BF16) for _ in specs)
    count = len(extra)
    flops = 2 * HALF * 512 * 512 * len(specs)
    return kernel(spread_body(specs, count), outs, 5 + count, 1, (), flops)(pos, *parts, *extra)


def keep_body(pos, own, got, energy, weights, out, tail):
    for t in range(4):
        part = product(pos, own, got, weights, 0, t)
        out[t, :HALF] = part[:, :N]
        out[t, HALF:] = part[:, N:]
    tail[...] = jnp.concatenate([pair_energy(got, energy), jnp.zeros((4, N), F32)], axis=0)


def half_sum_body(own, tail, u_plus, d_minus, d_plus, u_minus, q0, q1, q2, q3):
    for t, q in enumerate((q0, q1, q2, q3)):
        x, y = ((u_plus, d_minus), (d_plus, u_minus))[t // 2]
        k = t % 2
        value = own[t] + x[k, : 2 * HALF].astype(F32) + y[k, : 2 * HALF].astype(F32)
        q[: 2 * HALF] = value.astype(q.dtype)
        e = x[k, 2 * HALF :].astype(F32) + y[k, 2 * HALF :].astype(F32)
        e = tail[:4] + (e[:4] + e[4:8])
        if q.dtype == BF16:
            q[2 * HALF :] = energy_rows(e)
        else:
            q[2 * HALF :] = jnp.concatenate([e, jnp.zeros((12, N), F32)], axis=0)


def half_sum(*parts):
    outs = (shape((TALL, N)),) + (shape((TALL, N), BF16),) * 3
    return kernel(half_sum_body, outs, 6)(*parts)


def total_body(mine):
    def body(pos, v0, v1, v2, v3, out):
        parts = (v0, v1, v2, v3)
        e = sum(v[2 * HALF :].astype(F32) for v in parts)
        scale = lax.rsqrt(as_column(e[:4] + e[4:8]) / DI + EPS)
        rows = half(pos[2] if mine else 1 - pos[2])
        out[...] = sum(v[rows].astype(F32) for v in parts) * scale

    return body


def total(mine, pos, *parts):
    return kernel(total_body(mine), shape((HALF, N)), 5, 1)(pos, *parts)


def finish_body(pos, tokens, own, got, out):
    c = pos[2]
    for which, part in ((c, own), (1 - c, got)):
        rows = half(which)
        out[rows] = (tokens[rows].astype(F32) + part[...]).astype(BF16)


def finish(pos, *parts):
    return kernel(finish_body, shape((ROWS, N), BF16), 4, 1, place=False)(pos, *parts)


def local(
    tokens,
    norm_gain,
    gate_proj,
    inner_proj,
    state_proj,
    conv_inner,
    conv_state,
    log_rate,
    rate_bias,
    skip_gain,
    gate_gain,
    out_proj,
):
    ci = lax.axis_index("chan")
    core = ci & 1
    pos = jnp.stack([ci >> 3, (ci >> 1) & 3, core, ci]).astype(jnp.int32)
    gain = norm_gain.reshape(32, N)

    small = jnp.pad(jnp.stack([rate_bias, -jnp.exp(log_rate), skip_gain]), ((0, 5), (0, N - HEADS)))

    away_tokens = swap(tokens)
    sem = (pltpu.SemaphoreType.DMA,)
    own_block = kernel(
        own_body, shape((HALF + 3 * N, N), BF16), 4, 1, sem, inputs=(pltpu.HBM,) * 3, last=pl.ANY
    )(pos, state_proj, gain, tokens)
    block = kernel(block_body, shape((BLOCK, N), BF16), 3, 1)(pos, own_block, away_tokens)

    n1, n3 = plane_move(block, 1, 0), plane_move(block, -1, 0)
    p0, m0 = plane_move(block, 1, 1), plane_move(block, -1, 1)
    p1, m3 = plane_move(n1, 1, 1), plane_move(n3, -1, 1)
    low = plane_move(n1[: BLOCK // 2], 1, 0)
    high = plane_move(n3[BLOCK // 2 :], -1, 0)
    m1 = plane_move(n1, -1, 1)
    n2 = jnp.concatenate([low, high], axis=0)
    a23 = jnp.stack([n2, n3])
    p23, m2 = plane_move(a23, 1, 1), plane_move(n2, -1, 1)
    c0 = plane_move(jnp.stack([p0, p1]), 1, 1)
    c1 = plane_move(jnp.stack([m2, m3]), -1, 1)
    mark1 = mark(p1)
    mark2 = mark(m2)
    early = (block, n1, a23, p0, p1, p23, m0, m1, m2, m3)

    keep = kernel(scale_body, shape((D, 2 * CH), BF16), 3)(gate_proj, inner_proj, gain)
    got = swap(keep)
    got_w = swap(out_proj)

    most_own = pick(*early, marks=(mark1, mark2))
    most_got = swap(most_own)
    acc, squares = most(pos, *early, keep, got)
    acc_st = state_most(pos, *early, most_own, most_got)
    w_all = kernel(stack_body, shape((2 * CH, D), BF16), 2)(out_proj, got_w)
    acc, squares = more(pos, c0, keep, got, acc, squares)
    last_own = pick(c0, c1)
    last_got = swap(last_own)
    own_gi, send_gi, scale = rest(pos, c1, keep, got, acc, squares)
    got_gi = swap(send_gi)
    own_st, send_st = state_rest(pos, a23, p23, m2, c0, c1, most_own, most_got, last_own, last_got, acc_st, scale)
    got_st = swap(send_st)

    edge = kernel(edge_body, shape((8, 2 * CH)), 5, 1)(pos, own_gi, got_gi, own_st, got_st)
    rim = later(edge, 1)

    values, head = values_of(pos, own_gi, got_gi, conv_inner)
    in_map, out_map, within, until, step, *fresh = rows_of_all(pos, own_st, got_st, values, conv_state, small)
    *new, entering, packet = scan(
        rim, within, until, step, *fresh, head, conv_inner, conv_state
    )
    p2, p1 = later(packet, 2), later(packet, 1)
    window = three(packet, p1, p2)
    e6, e3 = later(window, 6), later(window, 3)
    result, opened, out_all = inside(
        pos, own_gi, got_gi, values, in_map, out_map, within, step, *new, entering, small
    )
    own_g, send_g, energy = gated(pos, p1, p2, e3, e6, result, opened, out_all, until, gate_gain[None])

    got_g = swap(send_g)
    parts = (own_g, got_g, energy, w_all)
    far_low, far_high = spread(pos, ((2, (0, 1)), (2, (2, 3))), parts)
    t_plus, t_minus = plane_move(far_low, 1, 0), plane_move(far_high, -1, 0)
    near_plus, near_minus = spread(pos, ((1, (2, 3)), (3, (0, 1))), parts)
    d_plus, d_minus = plane_move(near_plus, 1, 0), plane_move(near_minus, -1, 0)
    keep_outs = (shape((4, 2 * HALF, N)), shape((8, N)))
    kept, tail = kernel(keep_body, keep_outs, 5, 1, (), 2 * HALF * 512 * 1024)(pos, *parts)
    (on_plus,) = spread(pos, ((1, (0, 1)),), parts, (t_plus,))
    u_plus = plane_move(on_plus, 1, 0)
    (on_minus,) = spread(pos, ((3, (2, 3)),), parts, (t_minus,))
    u_minus = plane_move(on_minus, -1, 0)
    q = half_sum(kept, tail, u_plus, d_minus, d_plus, u_minus)
    last = [q[0]] + [plane_move(q[t], t, 1) for t in (1, 2, 3)]
    got = swap(total(False, pos, *last))
    own = total(True, pos, *last)
    return finish(pos, tokens, own, got)


def solution(mesh):
    return jax.shard_map(
        local,
        mesh=mesh,
        in_specs=(
            P("seq", "chan"),
            P(),
            P(None, "chan"),
            P(None, "chan"),
            P("chan", None),
            P(None, "chan"),
            P(),
            P("chan"),
            P("chan"),
            P("chan"),
            P("chan"),
            P("chan", None),
        ),
        out_specs=P("seq", "chan"),
        check_vma=False,
    )
```

```python
import jax
import jax.numpy as jnp
from jax import lax
from jax.experimental import pallas as pl
from jax.experimental.pallas import tpu as pltpu
from jax.sharding import PartitionSpec as P


D = 4096
DI = 8192
N = 128
P_SIZE = 64
K = 4
Q = 256
ROWS = 1024
HALF = 512
CHUNKS = 4
HEADS = 4
CH = 256
EPS = 1e-05
F32 = jnp.float32
BF16 = jnp.bfloat16


def plane_move(value, steps, phase):
    pairs = []
    for y in range(4):
        for x in range(4):
            for c in range(2):
                dy, dx = (0, steps) if c == phase else (steps, 0)
                pairs.append(((y * 4 + x) * 2 + c, ((y + dy) % 4 * 4 + (x + dx) % 4) * 2 + c))
    return lax.ppermute(value, "chan", pairs)


def swap(value):
    return lax.ppermute(value, "chan", [(i, i ^ 1) for i in range(32)])


def later(value, steps):
    return lax.ppermute(value, "seq", [(i, i + steps) for i in range(8 - steps)])


def kernel(body, outs, n_in, smem=0, scratch=(), flops=0, place=True, inputs=None, last=pltpu.VMEM):
    inner = pl.pallas_call(
        body,
        out_shape=jax.tree.map(lambda o: pltpu.VMEM(o.shape, o.dtype), outs) if place else outs,
        in_specs=[pl.BlockSpec(memory_space=pltpu.SMEM)] * smem + [pl.BlockSpec(memory_space=pltpu.VMEM)] * (n_in - smem - 1)
        + [pl.BlockSpec(memory_space=last)],
        out_specs=jax.tree.map(lambda _: pl.BlockSpec(memory_space=pltpu.VMEM), outs),
        scratch_shapes=list(scratch),
        compiler_params=pltpu.CompilerParams(vmem_limit_bytes=16 * 1024 * 1024),
        cost_estimate=pl.CostEstimate(flops=flops, transcendentals=0, bytes_accessed=1 << 20),
    )

    def call(*args):
        spaces = inputs or (pltpu.VMEM,) * (n_in - smem)
        placed = [pltpu.with_memory_space_constraint(a, m) if m else a for a, m in zip(args[smem:], spaces)]
        return inner(*args[:smem], *placed)

    return call


def shape(dims, kind=F32):
    return jax.ShapeDtypeStruct(dims, kind)


def dot(a, b, precision=None):
    return jnp.dot(a, b, preferred_element_type=F32, precision=precision)


def eye(n):
    return lax.broadcasted_iota(jnp.int32, (n, n), 0) == lax.broadcasted_iota(jnp.int32, (n, n), 1)


def stand(row):
    return jnp.sum(jnp.where(eye(N), jnp.broadcast_to(row, (N, N)), 0.0), axis=1, keepdims=True)


def lay(column):
    return jnp.sum(jnp.where(eye(N), jnp.broadcast_to(column, (N, N)), 0.0), axis=0, keepdims=True)


def as_rows(column):
    return jnp.concatenate([lay(column[i * N : (i + 1) * N]) for i in range(4)], axis=0)


def as_column(rows):
    return jnp.concatenate([stand(rows[i : i + 1]) for i in range(4)], axis=0)


def half(index):
    return pl.ds(pl.multiple_of(index * HALF, HALF), HALF)


BLOCK = 2 * HALF + 3 * N


def own_body(pos, state_w, gain, tokens, out, sem):
    c, ci = pos[2], pos[3]
    copy = pltpu.make_async_copy(tokens.at[half(c)], out.at[:HALF], sem)
    copy.start()
    scaled = (state_w[...].astype(F32) * stand(gain[pl.ds(ci, 1)])).astype(BF16)
    for b in range(3):
        out[HALF + b * N : HALF + (b + 1) * N] = scaled[:, b * N : (b + 1) * N]
    copy.wait()


def block_body(pos, own, away, out):
    c = pos[2]
    out[half(c)] = own[:HALF]
    out[half(1 - c)] = away[half(c)]
    out[2 * HALF :] = own[HALF:]


def scale_body(gate, inner, gain, out):
    def step(i, _):
        rows = pl.ds(pl.multiple_of(i * N, N), N)
        column = stand(gain[pl.ds(i, 1)])
        out[rows, :CH] = (gate[rows].astype(F32) * column).astype(BF16)
        out[rows, CH:] = (inner[rows].astype(F32) * column).astype(BF16)
        return 0

    lax.fori_loop(0, 2 * 16, step, 0, unroll=4)


def mark_body(ref, out):
    out[...] = ref[:16]


def mark(piece):
    return kernel(mark_body, shape((16, N), BF16), 1)(piece)


def blocks_of(refs):
    found = []
    for ref in refs:
        found += [ref] if len(ref.shape) == 2 else [ref.at[0], ref.at[1]]
    return found


def pick_body(count):
    def body(*refs):
        for i, ref in enumerate(blocks_of(refs[:count])):
            refs[-1][i] = ref[2 * HALF :]

    return body


def pick(*pieces, marks=()):
    blocks = sum(1 if p.ndim == 2 else 2 for p in pieces)
    out = shape((blocks, 3 * N, N), BF16)
    return kernel(pick_body(len(pieces)), out, len(pieces) + len(marks))(*pieces, *marks)


def owner(pos, s, t):
    first = pos[2] == 0
    dy = jnp.where(first, s, t)
    dx = jnp.where(first, t, s)
    return ((pos[0] - dy) & 3) * 4 + ((pos[1] - dx) & 3)


STEP = 256


def add_slots(pos, slots, keep, got, acc, squares, fresh):
    def rows_of(r, _):
        rows = pl.ds(pl.multiple_of(r * STEP, STEP), STEP)
        low = pl.ds(pl.multiple_of(r * STEP, STEP), STEP)
        high = pl.ds(pl.multiple_of(HALF + r * STEP, STEP), STEP)
        square = None if fresh else squares[rows]
        for n, (s, blocks) in enumerate(slots):
            parts = []
            for ref in blocks:
                parts += [ref[low], ref[high]]
            for v in parts:
                v = v.astype(F32)
                square = v * v if square is None else square + v * v
            lhs = jnp.concatenate(parts, axis=1)
            ids = [pl.ds(pl.multiple_of(owner(pos, s, t) * 2 * N, 2 * N), 2 * N) for t in range(4)]
            for w, ref in enumerate((keep, got)):
                for b in range(2):
                    cols = slice(w * 2 * CH + b * CH, w * 2 * CH + (b + 1) * CH)
                    rhs = jnp.concatenate([ref[i, b * CH : (b + 1) * CH] for i in ids], axis=0)
                    part = dot(lhs, rhs)
                    if fresh and n == 0:
                        acc[rows, cols] = part
                    else:
                        acc[rows, cols] += part
        squares[rows] = square
        return 0

    lax.fori_loop(0, HALF // STEP, rows_of, 0)


def most_body(pos, *refs):
    blocks, (keep, got, acc, squares) = blocks_of(refs[:-4]), refs[-4:]
    slots = ((0, blocks[:4]), (1, blocks[4:8]), (3, blocks[8:]))
    add_slots(pos, slots, keep, got, acc, squares, True)


def most(pos, *parts):
    outs = (shape((HALF, 4 * CH)), shape((HALF, N)))
    return kernel(most_body, outs, len(parts) + 1, 1, (), 2 * HALF * 3072 * 1024)(pos, *parts)


def more_body(pos, c0, keep, got, acc_in, squares_in, acc, squares):
    blocks = blocks_of((c0,))

    def rows_of(r, _):
        rows = pl.ds(pl.multiple_of(r * STEP, STEP), STEP)
        high = pl.ds(pl.multiple_of(HALF + r * STEP, STEP), STEP)
        parts = []
        for ref in blocks:
            parts += [ref[rows], ref[high]]
        square = squares_in[rows]
        for v in parts:
            v = v.astype(F32)
            square = square + v * v
        squares[rows] = square
        lhs = jnp.concatenate(parts, axis=1)
        ids = [pl.ds(pl.multiple_of(owner(pos, 2, t) * 2 * N, 2 * N), 2 * N) for t in (0, 1)]
        for w, ref in enumerate((keep, got)):
            for b in range(2):
                cols = slice(w * 2 * CH + b * CH, w * 2 * CH + (b + 1) * CH)
                rhs = jnp.concatenate([ref[i, b * CH : (b + 1) * CH] for i in ids], axis=0)
                acc[rows, cols] = acc_in[rows, cols] + dot(lhs, rhs)
        return 0

    lax.fori_loop(0, HALF // STEP, rows_of, 0)


def more(pos, *parts):
    outs = (shape((HALF, 4 * CH)), shape((HALF, N)))
    return kernel(more_body, outs, 6, 1, (), 2 * HALF * 512 * 1024)(pos, *parts)


def rest_body(pos, c1, keep, got, acc, squares, own, send, scale):
    blocks = blocks_of((c1,))

    def rows_of(r, _):
        rows = pl.ds(pl.multiple_of(r * STEP, STEP), STEP)
        high = pl.ds(pl.multiple_of(HALF + r * STEP, STEP), STEP)
        square = squares[rows]
        parts = []
        for ref in blocks:
            parts += [ref[rows], ref[high]]
        for v in parts:
            v = v.astype(F32)
            square = square + v * v
        inverse = lax.rsqrt(jnp.sum(square, axis=1, keepdims=True) / D + EPS)
        scale[rows] = jnp.broadcast_to(inverse, (STEP, N))
        lhs = jnp.concatenate(parts, axis=1)
        ids = [pl.ds(pl.multiple_of(owner(pos, 2, t) * 2 * N, 2 * N), 2 * N) for t in (2, 3)]
        for w, (ref, out) in enumerate(((keep, own), (got, send))):
            for b in range(2):
                cols = slice(b * CH, (b + 1) * CH)
                rhs = jnp.concatenate([ref[i, cols] for i in ids], axis=0)
                part = acc[rows, w * 2 * CH + b * CH : w * 2 * CH + (b + 1) * CH] + dot(lhs, rhs)
                out[rows, cols] = (part * inverse).astype(BF16)
        return 0

    lax.fori_loop(0, HALF // STEP, rows_of, 0)


def rest(pos, *parts):
    outs = (shape((HALF, 2 * CH), BF16), shape((HALF, 2 * CH), BF16), shape((HALF, N)))
    return kernel(rest_body, outs, 6, 1, (), 2 * HALF * 512 * 1024)(pos, *parts)


ORDER = (0, 1, 3, 2)


def state_sum(pos, blocks, most_own, most_got, last_own, last_got, slots, finish):
    c = pos[2]

    def rows_of(r, _):
        mine = pl.ds(pl.multiple_of(c * HALF + r * STEP, STEP), STEP)
        other = pl.ds(pl.multiple_of((1 - c) * HALF + r * STEP, STEP), STEP)
        lhs, w = [], [[], [], []]
        for g, k in slots:
            i = 4 * g + k
            lhs += [blocks[i][mine], blocks[i][other]]
            j = 4 * ORDER.index(k) + ORDER[g]
            for b in range(3):
                cut = slice(b * N, (b + 1) * N)
                w[b].append(most_own[i, cut] if i < 12 else last_own[i - 12, cut])
                w[b].append(most_got[j, cut] if j < 12 else last_got[j - 12, cut])
        lhs = jnp.concatenate(lhs, axis=1)
        w = [jnp.concatenate(v, axis=0) for v in w]
        finish(r, dot(lhs, jnp.concatenate(w[:2], axis=1)), dot(lhs, w[2]))
        return 0

    lax.fori_loop(0, HALF // STEP, rows_of, 0)


EARLY = [(g, k) for g in range(3) for k in (0, 1, 3)]
LATE = [(g, 2) for g in range(3)] + [(3, k) for k in range(4)]


def state_most_body(pos, *refs):
    blocks, (most_own, most_got, out) = blocks_of(refs[:-3]), refs[-3:]

    def finish(r, left, right):
        rows = pl.ds(pl.multiple_of(r * STEP, STEP), STEP)
        out[rows, : 2 * N] = left
        out[rows, 2 * N :] = right

    state_sum(pos, blocks, most_own, most_got, None, None, EARLY, finish)


def state_most(pos, *parts):
    call = kernel(state_most_body, shape((HALF, 3 * N)), len(parts) + 1, 1, (), 2 * HALF * 2304 * 384)
    return call(pos, *parts)


def state_body(pos, n2, p2, m2, c0, c1, most_own, most_got, last_own, last_got, acc, scale, out, send):
    ci = pos[3]

    def finish(r, left, right):
        rows = pl.ds(pl.multiple_of(r * STEP, STEP), STEP)
        inverse = scale[rows]
        out[rows, :N] = (acc[rows, :N] + left[:, :N]) * inverse
        out[rows, N : 2 * N] = (acc[rows, N : 2 * N] + left[:, N:]) * inverse
        rates = (acc[rows, 2 * N :] + right) * inverse
        lane = lax.broadcasted_iota(jnp.int32, (STEP, N), 1)
        out[rows, 2 * N :] = pltpu.roll(rates, (N - ci * HEADS) & (N - 1), 1)
        send[rows, : 2 * N] = out[rows, : 2 * N].astype(BF16)
        left = pltpu.roll(rates, (N - (ci ^ 1) * HEADS) & (N - 1), 1)
        packed = jnp.zeros((STEP, N), F32)
        for k in range(3):
            piece = left.astype(BF16).astype(F32)
            left = left - piece
            packed = jnp.where(lane // HEADS == k, pltpu.roll(piece, k * HEADS, 1), packed)
        send[rows, 2 * N :] = packed.astype(BF16)

    late = [None] * 12 + blocks_of((c0, c1))
    late[2], late[6], late[10] = n2, p2, m2
    state_sum(pos, late, most_own, most_got, last_own, last_got, LATE, finish)


def state_rest(pos, *parts):
    outs = (shape((HALF, 3 * N)), shape((HALF, 3 * N), BF16))
    return kernel(state_body, outs, 12, 1, (), 2 * HALF * 1792 * 384)(pos, *parts)


def silu(v):
    h = 0.5 * v
    return h + h * jnp.tanh(h)


def widen(columns, rows):
    return jnp.concatenate(
        [jnp.broadcast_to(columns[:, h : h + 1], (rows, P_SIZE)) for h in range(HEADS)], axis=1
    )


def convolve(window, taps):
    total = jnp.zeros((Q, CH), F32)
    for k in range(K):
        total = total + taps[k : k + 1] * window[5 + k : 5 + k + Q]
    return silu(total)


def fresh_state(values, b, w, step):
    scaled = (values * widen(jnp.exp(w[Q - 1 : Q] - w) * step, Q)).astype(BF16)
    return lax.dot_general(b, scaled, (((0,), (0,)), ((), ())), preferred_element_type=F32)


def values_body(pos, own_gi, got_gi, taps, values, head, pad):
    c = pos[2]
    for which, gi in ((c, own_gi), (1 - c, got_gi)):
        pad[pl.ds(pl.multiple_of(8 + which * HALF, 8), HALF)] = gi[:, CH:].astype(F32)

    def chunk(i, _):
        rows = pl.ds(pl.multiple_of(i * Q, Q), Q)
        values[rows] = convolve(pad[pl.ds(pl.multiple_of(i * Q, Q), Q + 8)], taps)
        return 0

    lax.fori_loop(1, CHUNKS, chunk, 0)
    head[...] = pad[8 : 8 + Q]


def values_of(pos, *parts):
    scratch = (pltpu.VMEM((ROWS + 8, CH), F32),)
    return kernel(values_body, (shape((ROWS, CH)), shape((Q, CH))), 4, 1, scratch)(pos, *parts)


def rows_body(
    pos, own_st, got_st, values, conv_state, small,
    in_map, out_map, within, until, step, fresh, head, pad, rate, passed,
):
    c = pos[2]
    for which, st in ((c, own_st), (1 - c, got_st)):
        pad[pl.ds(pl.multiple_of(8 + which * HALF, 8), HALF)] = st[:, : 2 * N].astype(F32)
        tail = st[:, 2 * N :].astype(F32)
        if st is got_st:
            tail = tail + (pltpu.roll(tail, N - HEADS, 1) + pltpu.roll(tail, N - 2 * HEADS, 1))
        rate[half(which)] = tail
    lane = lax.broadcasted_iota(jnp.int32, (Q, N), 1)
    lower = (
        lax.broadcasted_iota(jnp.int32, (Q, Q), 0) >= lax.broadcasted_iota(jnp.int32, (Q, Q), 1)
    ).astype(BF16)
    passed[...] = jnp.zeros((8, N), F32)

    def rates(i, _):
        rows = pl.ds(pl.multiple_of(i * Q, Q), Q)
        v = rate[rows] + small[0:1]
        soft = jnp.maximum(v, 0.0) + jnp.log1p(jnp.exp(-jnp.abs(v)))
        steps = jnp.where(lane < HEADS, soft, 0.0)
        step[rows] = steps
        left = steps * small[1:2]
        w = jnp.zeros((Q, N), F32)
        for _ in range(3):
            piece = left.astype(BF16)
            left = left - piece.astype(F32)
            w = w + dot(lower, piece)
        within[rows] = w
        before = passed[:1]
        until[rows] = w + before
        passed[:1] = before + w[Q - 1 : Q]
        return 0

    lax.fori_loop(0, CHUNKS, rates, 0)

    def chunk(i, _):
        rows = pl.ds(pl.multiple_of(i * Q, Q), Q)
        vs = convolve(pad[pl.ds(pl.multiple_of(i * Q, Q), Q + 8)], conv_state)
        b = vs[:, :N].astype(BF16)
        in_map[rows] = b
        out_map[rows] = vs[:, N:].astype(BF16)
        fresh[i] = fresh_state(values[rows], b, within[rows], step[rows])
        return 0

    lax.fori_loop(1, CHUNKS, chunk, 0)
    head[...] = pad[8 : 8 + Q]


def rows_of_all(pos, *parts):
    outs = (
        shape((ROWS, N), BF16),
        shape((ROWS, N), BF16),
        shape((ROWS, N)),
        shape((ROWS, N)),
        shape((ROWS, N)),
        shape((CHUNKS, N, CH)),
        shape((Q, CH)),
    )
    scratch = (pltpu.VMEM((ROWS + 8, CH), F32), pltpu.VMEM((ROWS, N), F32), pltpu.VMEM((8, N), F32))
    return kernel(rows_body, outs, 6, 1, scratch)(pos, *parts)


def write_packet(packet, state, log):
    high = log.astype(BF16)
    low = (log - high.astype(F32)).astype(BF16)
    packet[:N] = state.astype(BF16)
    packet[N:] = jnp.concatenate([high, low, jnp.zeros((14, CH), BF16)], axis=0)


def read_packets(packets):
    state = jnp.zeros((N, CH), F32)
    log = jnp.zeros((1, CH), F32)
    for p in packets:
        state = state + jnp.exp(log) * p[:N].astype(F32)
        tail = p[N:].astype(F32)
        log = log + (tail[0:1] + tail[1:2])
    return state, log


def three_body(own, p1, p2, out):
    write_packet(out, *read_packets((own, p1, p2)))


def three(*packets):
    return kernel(three_body, shape((N + 16, CH), BF16), 3)(*packets)


def scan_body(
    rim, within, until, step, fresh, head_s, head_i, conv_inner, conv_state,
    new_values, new_in, new_out, entering, packet,
):
    vi = convolve(jnp.concatenate([rim[:, :CH], head_i[...]], axis=0), conv_inner)
    vs = convolve(jnp.concatenate([rim[:, CH:], head_s[...]], axis=0), conv_state)
    b = vs[:, :N].astype(BF16)
    new_values[...] = vi
    new_in[...] = b
    new_out[...] = vs[:, N:].astype(BF16)
    carry = fresh_state(vi, b, within[:Q], step[:Q])
    entering[0] = jnp.zeros((N, CH), BF16)
    for i in range(1, CHUNKS):
        entering[i] = carry.astype(BF16)
        end = (i + 1) * Q
        carry = widen(jnp.exp(within[end - 1 : end]), 1) * carry + fresh[i]
    total = widen(until[ROWS - 1 : ROWS], 1)
    write_packet(packet, carry, total)


def scan(*parts):
    outs = (
        shape((Q, CH)),
        shape((Q, N), BF16),
        shape((Q, N), BF16),
        shape((CHUNKS, N, CH), BF16),
        shape((N + 16, CH), BF16),
    )
    return kernel(scan_body, outs, 9)(*parts)


def inside_body(
    pos, own_gi, got_gi, values, in_map, out_map, within, step, new_values, new_in, new_out, entering, small,
    result, opened, out_all, gate,
):
    c = pos[2]
    skip = widen(small[2:3], 1)
    gate[half(c)] = own_gi[:, :CH]
    gate[half(1 - c)] = got_gi[:, :CH]
    lower = lax.broadcasted_iota(jnp.int32, (Q, Q), 0) >= lax.broadcasted_iota(jnp.int32, (Q, Q), 1)

    def chunk(i, _):
        rows = pl.ds(pl.multiple_of(i * Q, Q), Q)
        opened[rows] = silu(gate[rows].astype(F32))
        head = i == 0
        vi = jnp.where(head, new_values[...], values[rows])
        b = jnp.where(head, new_in[...].astype(F32), in_map[rows].astype(F32)).astype(BF16)
        out = jnp.where(head, new_out[...].astype(F32), out_map[rows].astype(F32)).astype(BF16)
        out_all[rows] = out
        w = within[rows]
        scores = lax.dot_general(out, b, (((1,), (1,)), ((), ())), preferred_element_type=F32)
        flat = w.T
        stepped = (vi * widen(step[rows], Q)).astype(BF16)
        parts = []
        for h in range(HEADS):
            gap = w[:, h : h + 1] - flat[h : h + 1]
            mixing = (scores * jnp.exp(jnp.where(lower, gap, -jnp.inf))).astype(BF16)
            parts.append(dot(mixing, stepped[:, h * P_SIZE : (h + 1) * P_SIZE]))
        local = jnp.concatenate(parts, axis=1)
        local = local + dot(out, entering[i]) * widen(jnp.exp(w), Q)
        result[rows] = local + skip * vi
        return 0

    lax.fori_loop(0, CHUNKS, chunk, 0)


def inside(pos, *parts):
    outs = (shape((ROWS, CH)), shape((ROWS, CH)), shape((ROWS, N), BF16))
    return kernel(inside_body, outs, 13, 1, (pltpu.VMEM((ROWS, CH), BF16),))(pos, *parts)


def edge_body(pos, own_gi, got_gi, own_st, got_st, out):
    second = pos[2] == 1
    last = slice(HALF - 16, HALF)
    inner = jnp.where(second, own_gi[last, CH:].astype(F32), got_gi[last, CH:].astype(F32))
    out[:, :CH] = inner[8:]
    state = jnp.where(second, own_st[last, : 2 * N], got_st[last, : 2 * N].astype(F32))
    out[:, CH:] = state[8:]


def split(energy):
    high = energy.astype(BF16)
    return high, (energy - high.astype(F32)).astype(BF16)


def gated_body(pos, p1, p2, e3, e6, local, opened, out_map, until, gate_gain, own, send, energy):
    c = pos[2]
    carried = read_packets((p1, p2, e3, e6))[0].astype(BF16)
    for which, to in ((1 - c, send), (c, own)):
        rows = half(which)
        out = local[rows] + dot(out_map[rows], carried) * widen(jnp.exp(until[rows]), HALF)
        out = out * opened[rows]
        to[:HALF] = (out * gate_gain[...]).astype(BF16)
        e = as_rows(jnp.sum(out * out, axis=1, keepdims=True))
        if to is own:
            energy[...] = jnp.concatenate([e, jnp.zeros((4, N), F32)], axis=0)
        else:
            e = jnp.concatenate(split(e), axis=1)
            to[HALF:] = jnp.concatenate([e, jnp.zeros((12, CH), BF16)], axis=0)


def gated(pos, *parts):
    outs = (shape((HALF, CH), BF16), shape((HALF + 16, CH), BF16), shape((8, N)))
    return kernel(gated_body, outs, 10, 1)(pos, *parts)


TALL = 2 * HALF + 16


def energy_rows(energy):
    return jnp.concatenate([*split(energy), jnp.zeros((8, N), BF16)], axis=0)


def stack_body(own, got, out):
    out[:CH] = own[...]
    out[CH:] = got[...]


def pair_energy(got, energy):
    tail = got[HALF:].astype(F32)
    return energy[:4] + (tail[:4, :N] + tail[:4, N:])


def product(pos, own, got, weights, s, t):
    first = pos[2] == 0
    dy = jnp.where(first, t, s)
    dx = jnp.where(first, s, t)
    chip = ((pos[0] + dy) & 3) * 4 + ((pos[1] + dx) & 3)
    cols = pl.ds(pl.multiple_of(chip * 2 * N, 2 * N), 2 * N)
    return dot(jnp.concatenate([own[...], got[:HALF]], axis=1), weights[:, cols])


def spread_body(specs, adds):
    def body(pos, own, got, energy, weights, *refs):
        extra, outs = refs[:adds], refs[adds:]
        for n, (s, pair) in enumerate(specs):
            tail = pair_energy(got, energy)
            if adds:
                rows = extra[n][0, 2 * HALF :].astype(F32)
                tail = tail + (rows[:4] + rows[4:8])
            tail = energy_rows(tail)
            for k, t in enumerate(pair):
                part = product(pos, own, got, weights, s, t)
                for side in range(2):
                    rows = slice(side * HALF, (side + 1) * HALF)
                    value = part[:, side * N : (side + 1) * N]
                    if adds:
                        value = value + extra[n][k, rows].astype(F32)
                    outs[n][k, rows] = value.astype(BF16)
                outs[n][k, 2 * HALF :] = tail

    return body


def spread(pos, specs, parts, extra=()):
    outs = tuple(shape((2, TALL, N), BF16) for _ in specs)
    count = len(extra)
    flops = 2 * HALF * 512 * 512 * len(specs)
    return kernel(spread_body(specs, count), outs, 5 + count, 1, (), flops)(pos, *parts, *extra)


def keep_body(pos, own, got, energy, weights, out, tail):
    for t in range(4):
        part = product(pos, own, got, weights, 0, t)
        out[t, :HALF] = part[:, :N]
        out[t, HALF:] = part[:, N:]
    tail[...] = jnp.concatenate([pair_energy(got, energy), jnp.zeros((4, N), F32)], axis=0)


def half_sum_body(own, tail, u_plus, d_minus, d_plus, u_minus, q0, q1, q2, q3):
    for t, q in enumerate((q0, q1, q2, q3)):
        x, y = ((u_plus, d_minus), (d_plus, u_minus))[t // 2]
        k = t % 2
        value = own[t] + x[k, : 2 * HALF].astype(F32) + y[k, : 2 * HALF].astype(F32)
        q[: 2 * HALF] = value.astype(q.dtype)
        e = x[k, 2 * HALF :].astype(F32) + y[k, 2 * HALF :].astype(F32)
        e = tail[:4] + (e[:4] + e[4:8])
        if q.dtype == BF16:
            q[2 * HALF :] = energy_rows(e)
        else:
            q[2 * HALF :] = jnp.concatenate([e, jnp.zeros((12, N), F32)], axis=0)


def half_sum(*parts):
    outs = (shape((TALL, N)),) + (shape((TALL, N), BF16),) * 3
    return kernel(half_sum_body, outs, 6)(*parts)


def total_body(mine):
    def body(pos, v0, v1, v2, v3, out):
        parts = (v0, v1, v2, v3)
        e = sum(v[2 * HALF :].astype(F32) for v in parts)
        scale = lax.rsqrt(as_column(e[:4] + e[4:8]) / DI + EPS)
        rows = half(pos[2] if mine else 1 - pos[2])
        out[...] = sum(v[rows].astype(F32) for v in parts) * scale

    return body


def total(mine, pos, *parts):
    return kernel(total_body(mine), shape((HALF, N)), 5, 1)(pos, *parts)


def finish_body(pos, tokens, own, got, out):
    c = pos[2]
    for which, part in ((c, own), (1 - c, got)):
        rows = half(which)
        out[rows] = (tokens[rows].astype(F32) + part[...]).astype(BF16)


def finish(pos, *parts):
    return kernel(finish_body, shape((ROWS, N), BF16), 4, 1, place=False)(pos, *parts)


def local(
    tokens,
    norm_gain,
    gate_proj,
    inner_proj,
    state_proj,
    conv_inner,
    conv_state,
    log_rate,
    rate_bias,
    skip_gain,
    gate_gain,
    out_proj,
):
    ci = lax.axis_index("chan")
    core = ci & 1
    pos = jnp.stack([ci >> 3, (ci >> 1) & 3, core, ci]).astype(jnp.int32)
    gain = norm_gain.reshape(32, N)

    small = jnp.pad(jnp.stack([rate_bias, -jnp.exp(log_rate), skip_gain]), ((0, 5), (0, N - HEADS)))

    away_tokens = swap(tokens)
    sem = (pltpu.SemaphoreType.DMA,)
    own_block = kernel(
        own_body, shape((HALF + 3 * N, N), BF16), 4, 1, sem, inputs=(pltpu.HBM,) * 3, last=pl.ANY
    )(pos, state_proj, gain, tokens)
    block = kernel(block_body, shape((BLOCK, N), BF16), 3, 1)(pos, own_block, away_tokens)

    n1, n3 = plane_move(block, 1, 0), plane_move(block, -1, 0)
    p0, m0 = plane_move(block, 1, 1), plane_move(block, -1, 1)
    p1, m3 = plane_move(n1, 1, 1), plane_move(n3, -1, 1)
    low = plane_move(n1[: BLOCK // 2], 1, 0)
    high = plane_move(n3[BLOCK // 2 :], -1, 0)
    p3, m1 = plane_move(n3, 1, 1), plane_move(n1, -1, 1)
    n2 = jnp.concatenate([low, high], axis=0)
    p2, m2 = plane_move(n2, 1, 1), plane_move(n2, -1, 1)
    c0 = plane_move(jnp.stack([p0, p1]), 1, 1)
    c1 = plane_move(jnp.stack([m2, m3]), -1, 1)
    mark1 = mark(p1)
    mark2 = mark(m2)
    early = (block, n1, n2, n3, p0, p1, p2, p3, m0, m1, m2, m3)

    keep = kernel(scale_body, shape((D, 2 * CH), BF16), 3)(gate_proj, inner_proj, gain)
    got = swap(keep)
    got_w = swap(out_proj)

    most_own = pick(*early, marks=(mark1, mark2))
    most_got = swap(most_own)
    acc, squares = most(pos, *early, keep, got)
    acc_st = state_most(pos, *early, most_own, most_got)
    w_all = kernel(stack_body, shape((2 * CH, D), BF16), 2)(out_proj, got_w)
    acc, squares = more(pos, c0, keep, got, acc, squares)
    last_own = pick(c0, c1)
    last_got = swap(last_own)
    own_gi, send_gi, scale = rest(pos, c1, keep, got, acc, squares)
    got_gi = swap(send_gi)
    own_st, send_st = state_rest(pos, n2, p2, m2, c0, c1, most_own, most_got, last_own, last_got, acc_st, scale)
    got_st = swap(send_st)

    edge = kernel(edge_body, shape((8, 2 * CH)), 5, 1)(pos, own_gi, got_gi, own_st, got_st)
    rim = later(edge, 1)

    values, head = values_of(pos, own_gi, got_gi, conv_inner)
    in_map, out_map, within, until, step, *fresh = rows_of_all(pos, own_st, got_st, values, conv_state, small)
    *new, entering, packet = scan(
        rim, within, until, step, *fresh, head, conv_inner, conv_state
    )
    z2, z1 = later(packet, 2), later(packet, 1)
    window = three(packet, z1, z2)
    e6, e3 = later(window, 6), later(window, 3)
    result, opened, out_all = inside(
        pos, own_gi, got_gi, values, in_map, out_map, within, step, *new, entering, small
    )
    own_g, send_g, energy = gated(pos, z1, z2, e3, e6, result, opened, out_all, until, gate_gain[None])

    got_g = swap(send_g)
    parts = (own_g, got_g, energy, w_all)
    far_low, far_high = spread(pos, ((2, (0, 1)), (2, (2, 3))), parts)
    t_plus, t_minus = plane_move(far_low, 1, 0), plane_move(far_high, -1, 0)
    near_plus, near_minus = spread(pos, ((1, (2, 3)), (3, (0, 1))), parts)
    d_plus, d_minus = plane_move(near_plus, 1, 0), plane_move(near_minus, -1, 0)
    keep_outs = (shape((4, 2 * HALF, N)), shape((8, N)))
    kept, tail = kernel(keep_body, keep_outs, 5, 1, (), 2 * HALF * 512 * 1024)(pos, *parts)
    (on_plus,) = spread(pos, ((1, (0, 1)),), parts, (t_plus,))
    u_plus = plane_move(on_plus, 1, 0)
    (on_minus,) = spread(pos, ((3, (2, 3)),), parts, (t_minus,))
    u_minus = plane_move(on_minus, -1, 0)
    q = half_sum(kept, tail, u_plus, d_minus, d_plus, u_minus)
    last = [q[0]] + [plane_move(q[t], t, 1) for t in (1, 2, 3)]
    got = swap(total(False, pos, *last))
    own = total(True, pos, *last)
    return finish(pos, tokens, own, got)


def solution(mesh):
    return jax.shard_map(
        local,
        mesh=mesh,
        in_specs=(
            P("seq", "chan"),
            P(),
            P(None, "chan"),
            P(None, "chan"),
            P("chan", None),
            P(None, "chan"),
            P(),
            P("chan"),
            P("chan"),
            P("chan"),
            P("chan"),
            P("chan", None),
        ),
        out_specs=P("seq", "chan"),
        check_vma=False,
    )
```

```python
import jax
import jax.numpy as jnp
from jax import lax
from jax.experimental import pallas as pl
from jax.experimental.pallas import tpu as pltpu
from jax.sharding import PartitionSpec as P


D = 4096
DI = 8192
N = 128
P_SIZE = 64
K = 4
Q = 256
ROWS = 1024
HALF = 512
CHUNKS = 4
HEADS = 4
CH = 256
EPS = 1e-05
F32 = jnp.float32
BF16 = jnp.bfloat16


def plane_move(value, steps, phase):
    pairs = []
    for y in range(4):
        for x in range(4):
            for c in range(2):
                dy, dx = (0, steps) if c == phase else (steps, 0)
                pairs.append(((y * 4 + x) * 2 + c, ((y + dy) % 4 * 4 + (x + dx) % 4) * 2 + c))
    return lax.ppermute(value, "chan", pairs)


def swap(value):
    return lax.ppermute(value, "chan", [(i, i ^ 1) for i in range(32)])


def later(value, steps):
    return lax.ppermute(value, "seq", [(i, i + steps) for i in range(8 - steps)])


def kernel(body, outs, n_in, smem=0, scratch=(), flops=0, place=True, inputs=None, last=pltpu.VMEM):
    inner = pl.pallas_call(
        body,
        out_shape=jax.tree.map(lambda o: pltpu.VMEM(o.shape, o.dtype), outs) if place else outs,
        in_specs=[pl.BlockSpec(memory_space=pltpu.SMEM)] * smem + [pl.BlockSpec(memory_space=pltpu.VMEM)] * (n_in - smem - 1)
        + [pl.BlockSpec(memory_space=last)],
        out_specs=jax.tree.map(lambda _: pl.BlockSpec(memory_space=pltpu.VMEM), outs),
        scratch_shapes=list(scratch),
        compiler_params=pltpu.CompilerParams(vmem_limit_bytes=16 * 1024 * 1024),
        cost_estimate=pl.CostEstimate(flops=flops, transcendentals=0, bytes_accessed=1 << 20),
    )

    def call(*args):
        spaces = inputs or (pltpu.VMEM,) * (n_in - smem)
        placed = [pltpu.with_memory_space_constraint(a, m) if m else a for a, m in zip(args[smem:], spaces)]
        return inner(*args[:smem], *placed)

    return call


def shape(dims, kind=F32):
    return jax.ShapeDtypeStruct(dims, kind)


def dot(a, b, precision=None):
    return jnp.dot(a, b, preferred_element_type=F32, precision=precision)


def eye(n):
    return lax.broadcasted_iota(jnp.int32, (n, n), 0) == lax.broadcasted_iota(jnp.int32, (n, n), 1)


def stand(row):
    return jnp.sum(jnp.where(eye(N), jnp.broadcast_to(row, (N, N)), 0.0), axis=1, keepdims=True)


def lay(column):
    return jnp.sum(jnp.where(eye(N), jnp.broadcast_to(column, (N, N)), 0.0), axis=0, keepdims=True)


def as_rows(column):
    return jnp.concatenate([lay(column[i * N : (i + 1) * N]) for i in range(4)], axis=0)


def as_column(rows):
    return jnp.concatenate([stand(rows[i : i + 1]) for i in range(4)], axis=0)


def half(index):
    return pl.ds(pl.multiple_of(index * HALF, HALF), HALF)


BLOCK = 2 * HALF + 3 * N


def own_body(pos, state_w, gain, tokens, out, sem):
    c, ci = pos[2], pos[3]
    copy = pltpu.make_async_copy(tokens.at[half(c)], out.at[:HALF], sem)
    copy.start()
    scaled = (state_w[...].astype(F32) * stand(gain[pl.ds(ci, 1)])).astype(BF16)
    for b in range(3):
        out[HALF + b * N : HALF + (b + 1) * N] = scaled[:, b * N : (b + 1) * N]
    copy.wait()


def block_body(pos, own, away, out):
    c = pos[2]
    out[half(c)] = own[:HALF]
    out[half(1 - c)] = away[half(c)]
    out[2 * HALF :] = own[HALF:]


def scale_body(gate, inner, gain, out):
    def step(i, _):
        rows = pl.ds(pl.multiple_of(i * N, N), N)
        column = stand(gain[pl.ds(i, 1)])
        out[rows, :CH] = (gate[rows].astype(F32) * column).astype(BF16)
        out[rows, CH:] = (inner[rows].astype(F32) * column).astype(BF16)
        return 0

    lax.fori_loop(0, 2 * 16, step, 0, unroll=4)


def mark_body(ref, out):
    out[...] = ref[:16]


def mark(piece):
    return kernel(mark_body, shape((16, N), BF16), 1)(piece)


def blocks_of(refs):
    found = []
    for ref in refs:
        found += [ref] if len(ref.shape) == 2 else [ref.at[0], ref.at[1]]
    return found


def pick_body(count):
    def body(*refs):
        for i, ref in enumerate(blocks_of(refs[:count])):
            refs[-1][i] = ref[2 * HALF :]

    return body


def pick(*pieces, marks=()):
    blocks = sum(1 if p.ndim == 2 else 2 for p in pieces)
    out = shape((blocks, 3 * N, N), BF16)
    return kernel(pick_body(len(pieces)), out, len(pieces) + len(marks))(*pieces, *marks)


def owner(pos, s, t):
    first = pos[2] == 0
    dy = jnp.where(first, s, t)
    dx = jnp.where(first, t, s)
    return ((pos[0] - dy) & 3) * 4 + ((pos[1] - dx) & 3)


STEP = 256


def add_slots(pos, slots, keep, got, acc, squares, fresh):
    def rows_of(r, _):
        rows = pl.ds(pl.multiple_of(r * STEP, STEP), STEP)
        low = pl.ds(pl.multiple_of(r * STEP, STEP), STEP)
        high = pl.ds(pl.multiple_of(HALF + r * STEP, STEP), STEP)
        square = None if fresh else squares[rows]
        for n, (s, blocks) in enumerate(slots):
            parts = []
            for ref in blocks:
                parts += [ref[low], ref[high]]
            for v in parts:
                v = v.astype(F32)
                square = v * v if square is None else square + v * v
            lhs = jnp.concatenate(parts, axis=1)
            ids = [pl.ds(pl.multiple_of(owner(pos, s, t) * 2 * N, 2 * N), 2 * N) for t in range(4)]
            for w, ref in enumerate((keep, got)):
                for b in range(2):
                    cols = slice(w * 2 * CH + b * CH, w * 2 * CH + (b + 1) * CH)
                    rhs = jnp.concatenate([ref[i, b * CH : (b + 1) * CH] for i in ids], axis=0)
                    part = dot(lhs, rhs)
                    if fresh and n == 0:
                        acc[rows, cols] = part
                    else:
                        acc[rows, cols] += part
        squares[rows] = square
        return 0

    lax.fori_loop(0, HALF // STEP, rows_of, 0)


def most_body(pos, *refs):
    blocks, (keep, got, acc, squares) = blocks_of(refs[:-4]), refs[-4:]
    slots = ((0, blocks[:4]), (1, blocks[4:8]), (3, blocks[8:]))
    add_slots(pos, slots, keep, got, acc, squares, True)


def most(pos, *parts):
    outs = (shape((HALF, 4 * CH)), shape((HALF, N)))
    return kernel(most_body, outs, len(parts) + 1, 1, (), 2 * HALF * 3072 * 1024)(pos, *parts)


def more_body(pos, c0, keep, got, acc_in, squares_in, acc, squares):
    blocks = blocks_of((c0,))

    def rows_of(r, _):
        rows = pl.ds(pl.multiple_of(r * STEP, STEP), STEP)
        high = pl.ds(pl.multiple_of(HALF + r * STEP, STEP), STEP)
        parts = []
        for ref in blocks:
            parts += [ref[rows], ref[high]]
        square = squares_in[rows]
        for v in parts:
            v = v.astype(F32)
            square = square + v * v
        squares[rows] = square
        lhs = jnp.concatenate(parts, axis=1)
        ids = [pl.ds(pl.multiple_of(owner(pos, 2, t) * 2 * N, 2 * N), 2 * N) for t in (0, 1)]
        for w, ref in enumerate((keep, got)):
            for b in range(2):
                cols = slice(w * 2 * CH + b * CH, w * 2 * CH + (b + 1) * CH)
                rhs = jnp.concatenate([ref[i, b * CH : (b + 1) * CH] for i in ids], axis=0)
                acc[rows, cols] = acc_in[rows, cols] + dot(lhs, rhs)
        return 0

    lax.fori_loop(0, HALF // STEP, rows_of, 0)


def more(pos, *parts):
    outs = (shape((HALF, 4 * CH)), shape((HALF, N)))
    return kernel(more_body, outs, 6, 1, (), 2 * HALF * 512 * 1024)(pos, *parts)


def rest_body(pos, c1, keep, got, acc, squares, own, send, scale):
    blocks = blocks_of((c1,))

    def rows_of(r, _):
        rows = pl.ds(pl.multiple_of(r * STEP, STEP), STEP)
        high = pl.ds(pl.multiple_of(HALF + r * STEP, STEP), STEP)
        square = squares[rows]
        parts = []
        for ref in blocks:
            parts += [ref[rows], ref[high]]
        for v in parts:
            v = v.astype(F32)
            square = square + v * v
        inverse = lax.rsqrt(jnp.sum(square, axis=1, keepdims=True) / D + EPS)
        scale[rows] = jnp.broadcast_to(inverse, (STEP, N))
        lhs = jnp.concatenate(parts, axis=1)
        ids = [pl.ds(pl.multiple_of(owner(pos, 2, t) * 2 * N, 2 * N), 2 * N) for t in (2, 3)]
        for w, (ref, out) in enumerate(((keep, own), (got, send))):
            for b in range(2):
                cols = slice(b * CH, (b + 1) * CH)
                rhs = jnp.concatenate([ref[i, cols] for i in ids], axis=0)
                part = acc[rows, w * 2 * CH + b * CH : w * 2 * CH + (b + 1) * CH] + dot(lhs, rhs)
                out[rows, cols] = (part * inverse).astype(BF16)
        return 0

    lax.fori_loop(0, HALF // STEP, rows_of, 0)


def rest(pos, *parts):
    outs = (shape((HALF, 2 * CH), BF16), shape((HALF, 2 * CH), BF16), shape((HALF, N)))
    return kernel(rest_body, outs, 6, 1, (), 2 * HALF * 512 * 1024)(pos, *parts)


ORDER = (0, 1, 3, 2)


def state_sum(pos, blocks, most_own, most_got, last_own, last_got, slots, finish):
    c = pos[2]

    def rows_of(r, _):
        mine = pl.ds(pl.multiple_of(c * HALF + r * STEP, STEP), STEP)
        other = pl.ds(pl.multiple_of((1 - c) * HALF + r * STEP, STEP), STEP)
        lhs, w = [], [[], [], []]
        for g, k in slots:
            i = 4 * g + k
            lhs += [blocks[i][mine], blocks[i][other]]
            j = 4 * ORDER.index(k) + ORDER[g]
            for b in range(3):
                cut = slice(b * N, (b + 1) * N)
                w[b].append(most_own[i, cut] if i < 12 else last_own[i - 12, cut])
                w[b].append(most_got[j, cut] if j < 12 else last_got[j - 12, cut])
        lhs = jnp.concatenate(lhs, axis=1)
        w = [jnp.concatenate(v, axis=0) for v in w]
        finish(r, dot(lhs, jnp.concatenate(w[:2], axis=1)), dot(lhs, w[2]))
        return 0

    lax.fori_loop(0, HALF // STEP, rows_of, 0)


EARLY = [(g, k) for g in range(3) for k in (0, 1, 3)]
LATE = [(g, 2) for g in range(3)] + [(3, k) for k in range(4)]


def state_most_body(pos, *refs):
    blocks, (most_own, most_got, out) = blocks_of(refs[:-3]), refs[-3:]

    def finish(r, left, right):
        rows = pl.ds(pl.multiple_of(r * STEP, STEP), STEP)
        out[rows, : 2 * N] = left
        out[rows, 2 * N :] = right

    state_sum(pos, blocks, most_own, most_got, None, None, EARLY, finish)


def state_most(pos, *parts):
    call = kernel(state_most_body, shape((HALF, 3 * N)), len(parts) + 1, 1, (), 2 * HALF * 2304 * 384)
    return call(pos, *parts)


def state_body(pos, a23, p23, m2, c0, c1, most_own, most_got, last_own, last_got, acc, scale, out, send):
    ci = pos[3]

    def finish(r, left, right):
        rows = pl.ds(pl.multiple_of(r * STEP, STEP), STEP)
        inverse = scale[rows]
        out[rows, :N] = (acc[rows, :N] + left[:, :N]) * inverse
        out[rows, N : 2 * N] = (acc[rows, N : 2 * N] + left[:, N:]) * inverse
        rates = (acc[rows, 2 * N :] + right) * inverse
        lane = lax.broadcasted_iota(jnp.int32, (STEP, N), 1)
        out[rows, 2 * N :] = pltpu.roll(rates, (N - ci * HEADS) & (N - 1), 1)
        send[rows, : 2 * N] = out[rows, : 2 * N].astype(BF16)
        left = pltpu.roll(rates, (N - (ci ^ 1) * HEADS) & (N - 1), 1)
        packed = jnp.zeros((STEP, N), F32)
        for k in range(3):
            piece = left.astype(BF16).astype(F32)
            left = left - piece
            packed = jnp.where(lane // HEADS == k, pltpu.roll(piece, k * HEADS, 1), packed)
        send[rows, 2 * N :] = packed.astype(BF16)

    late = [None] * 12 + blocks_of((c0, c1))
    late[2], late[6], late[10] = a23.at[0], p23.at[0], m2
    state_sum(pos, late, most_own, most_got, last_own, last_got, LATE, finish)


def state_rest(pos, *parts):
    outs = (shape((HALF, 3 * N)), shape((HALF, 3 * N), BF16))
    return kernel(state_body, outs, 12, 1, (), 2 * HALF * 1792 * 384)(pos, *parts)


def silu(v):
    h = 0.5 * v
    return h + h * jnp.tanh(h)


def widen(columns, rows):
    return jnp.concatenate(
        [jnp.broadcast_to(columns[:, h : h + 1], (rows, P_SIZE)) for h in range(HEADS)], axis=1
    )


def convolve(window, taps):
    total = jnp.zeros((Q, CH), F32)
    for k in range(K):
        total = total + taps[k : k + 1] * window[5 + k : 5 + k + Q]
    return silu(total)


def fresh_state(values, b, w, step):
    scaled = (values * widen(jnp.exp(w[Q - 1 : Q] - w) * step, Q)).astype(BF16)
    return lax.dot_general(b, scaled, (((0,), (0,)), ((), ())), preferred_element_type=F32)


def values_body(pos, own_gi, got_gi, taps, values, head, pad):
    c = pos[2]
    for which, gi in ((c, own_gi), (1 - c, got_gi)):
        pad[pl.ds(pl.multiple_of(8 + which * HALF, 8), HALF)] = gi[:, CH:].astype(F32)

    def chunk(i, _):
        rows = pl.ds(pl.multiple_of(i * Q, Q), Q)
        values[rows] = convolve(pad[pl.ds(pl.multiple_of(i * Q, Q), Q + 8)], taps)
        return 0

    lax.fori_loop(1, CHUNKS, chunk, 0)
    head[...] = pad[8 : 8 + Q]


def values_of(pos, *parts):
    scratch = (pltpu.VMEM((ROWS + 8, CH), F32),)
    return kernel(values_body, (shape((ROWS, CH)), shape((Q, CH))), 4, 1, scratch)(pos, *parts)


def rows_body(
    pos, own_st, got_st, values, conv_state, small,
    in_map, out_map, within, until, step, fresh, head, pad, rate, passed,
):
    c = pos[2]
    for which, st in ((c, own_st), (1 - c, got_st)):
        pad[pl.ds(pl.multiple_of(8 + which * HALF, 8), HALF)] = st[:, : 2 * N].astype(F32)
        tail = st[:, 2 * N :].astype(F32)
        if st is got_st:
            tail = tail + (pltpu.roll(tail, N - HEADS, 1) + pltpu.roll(tail, N - 2 * HEADS, 1))
        rate[half(which)] = tail
    lane = lax.broadcasted_iota(jnp.int32, (Q, N), 1)
    lower = (
        lax.broadcasted_iota(jnp.int32, (Q, Q), 0) >= lax.broadcasted_iota(jnp.int32, (Q, Q), 1)
    ).astype(BF16)
    passed[...] = jnp.zeros((8, N), F32)

    def rates(i, _):
        rows = pl.ds(pl.multiple_of(i * Q, Q), Q)
        v = rate[rows] + small[0:1]
        soft = jnp.maximum(v, 0.0) + jnp.log1p(jnp.exp(-jnp.abs(v)))
        steps = jnp.where(lane < HEADS, soft, 0.0)
        step[rows] = steps
        left = steps * small[1:2]
        w = jnp.zeros((Q, N), F32)
        for _ in range(3):
            piece = left.astype(BF16)
            left = left - piece.astype(F32)
            w = w + dot(lower, piece)
        within[rows] = w
        before = passed[:1]
        until[rows] = w + before
        passed[:1] = before + w[Q - 1 : Q]
        return 0

    lax.fori_loop(0, CHUNKS, rates, 0)

    def chunk(i, _):
        rows = pl.ds(pl.multiple_of(i * Q, Q), Q)
        vs = convolve(pad[pl.ds(pl.multiple_of(i * Q, Q), Q + 8)], conv_state)
        b = vs[:, :N].astype(BF16)
        in_map[rows] = b
        out_map[rows] = vs[:, N:].astype(BF16)
        fresh[i] = fresh_state(values[rows], b, within[rows], step[rows])
        return 0

    lax.fori_loop(1, CHUNKS, chunk, 0)
    head[...] = pad[8 : 8 + Q]


def rows_of_all(pos, *parts):
    outs = (
        shape((ROWS, N), BF16),
        shape((ROWS, N), BF16),
        shape((ROWS, N)),
        shape((ROWS, N)),
        shape((ROWS, N)),
        shape((CHUNKS, N, CH)),
        shape((Q, CH)),
    )
    scratch = (pltpu.VMEM((ROWS + 8, CH), F32), pltpu.VMEM((ROWS, N), F32), pltpu.VMEM((8, N), F32))
    return kernel(rows_body, outs, 6, 1, scratch)(pos, *parts)


def write_packet(packet, state, log):
    high = log.astype(BF16)
    low = (log - high.astype(F32)).astype(BF16)
    packet[:N] = state.astype(BF16)
    packet[N:] = jnp.concatenate([high, low, jnp.zeros((14, CH), BF16)], axis=0)


def read_packets(packets):
    state = jnp.zeros((N, CH), F32)
    log = jnp.zeros((1, CH), F32)
    for p in packets:
        state = state + jnp.exp(log) * p[:N].astype(F32)
        tail = p[N:].astype(F32)
        log = log + (tail[0:1] + tail[1:2])
    return state, log


def three_body(own, p1, p2, out):
    write_packet(out, *read_packets((own, p1, p2)))


def three(*packets):
    return kernel(three_body, shape((N + 16, CH), BF16), 3)(*packets)


def scan_body(
    rim, within, until, step, fresh, head_s, head_i, conv_inner, conv_state,
    new_values, new_in, new_out, entering, packet,
):
    vi = convolve(jnp.concatenate([rim[:, :CH], head_i[...]], axis=0), conv_inner)
    vs = convolve(jnp.concatenate([rim[:, CH:], head_s[...]], axis=0), conv_state)
    b = vs[:, :N].astype(BF16)
    new_values[...] = vi
    new_in[...] = b
    new_out[...] = vs[:, N:].astype(BF16)
    carry = fresh_state(vi, b, within[:Q], step[:Q])
    entering[0] = jnp.zeros((N, CH), BF16)
    for i in range(1, CHUNKS):
        entering[i] = carry.astype(BF16)
        end = (i + 1) * Q
        carry = widen(jnp.exp(within[end - 1 : end]), 1) * carry + fresh[i]
    total = widen(until[ROWS - 1 : ROWS], 1)
    write_packet(packet, carry, total)


def scan(*parts):
    outs = (
        shape((Q, CH)),
        shape((Q, N), BF16),
        shape((Q, N), BF16),
        shape((CHUNKS, N, CH), BF16),
        shape((N + 16, CH), BF16),
    )
    return kernel(scan_body, outs, 9)(*parts)


def inside_body(
    pos, own_gi, got_gi, values, in_map, out_map, within, step, new_values, new_in, new_out, entering, small,
    result, opened, out_all, gate,
):
    c = pos[2]
    skip = widen(small[2:3], 1)
    gate[half(c)] = own_gi[:, :CH]
    gate[half(1 - c)] = got_gi[:, :CH]
    lower = lax.broadcasted_iota(jnp.int32, (Q, Q), 0) >= lax.broadcasted_iota(jnp.int32, (Q, Q), 1)

    def chunk(i, _):
        rows = pl.ds(pl.multiple_of(i * Q, Q), Q)
        opened[rows] = silu(gate[rows].astype(F32))
        head = i == 0
        vi = jnp.where(head, new_values[...], values[rows])
        b = jnp.where(head, new_in[...].astype(F32), in_map[rows].astype(F32)).astype(BF16)
        out = jnp.where(head, new_out[...].astype(F32), out_map[rows].astype(F32)).astype(BF16)
        out_all[rows] = out
        w = within[rows]
        scores = lax.dot_general(out, b, (((1,), (1,)), ((), ())), preferred_element_type=F32)
        flat = w.T
        stepped = (vi * widen(step[rows], Q)).astype(BF16)
        parts = []
        for h in range(HEADS):
            gap = w[:, h : h + 1] - flat[h : h + 1]
            mixing = (scores * jnp.exp(jnp.where(lower, gap, -jnp.inf))).astype(BF16)
            parts.append(dot(mixing, stepped[:, h * P_SIZE : (h + 1) * P_SIZE]))
        local = jnp.concatenate(parts, axis=1)
        local = local + dot(out, entering[i]) * widen(jnp.exp(w), Q)
        result[rows] = local + skip * vi
        return 0

    lax.fori_loop(0, CHUNKS, chunk, 0)


def inside(pos, *parts):
    outs = (shape((ROWS, CH)), shape((ROWS, CH)), shape((ROWS, N), BF16))
    return kernel(inside_body, outs, 13, 1, (pltpu.VMEM((ROWS, CH), BF16),))(pos, *parts)


def edge_body(pos, own_gi, got_gi, own_st, got_st, out):
    second = pos[2] == 1
    last = slice(HALF - 16, HALF)
    inner = jnp.where(second, own_gi[last, CH:].astype(F32), got_gi[last, CH:].astype(F32))
    out[:, :CH] = inner[8:]
    state = jnp.where(second, own_st[last, : 2 * N], got_st[last, : 2 * N].astype(F32))
    out[:, CH:] = state[8:]


def split(energy):
    high = energy.astype(BF16)
    return high, (energy - high.astype(F32)).astype(BF16)


def gated_body(pos, p1, p2, e3, e6, local, opened, out_map, until, gate_gain, own, send, energy):
    c = pos[2]
    carried = read_packets((p1, p2, e3, e6))[0].astype(BF16)
    for which, to in ((1 - c, send), (c, own)):
        rows = half(which)
        out = local[rows] + dot(out_map[rows], carried) * widen(jnp.exp(until[rows]), HALF)
        out = out * opened[rows]
        to[:HALF] = (out * gate_gain[...]).astype(BF16)
        e = as_rows(jnp.sum(out * out, axis=1, keepdims=True))
        if to is own:
            energy[...] = jnp.concatenate([e, jnp.zeros((4, N), F32)], axis=0)
        else:
            e = jnp.concatenate(split(e), axis=1)
            to[HALF:] = jnp.concatenate([e, jnp.zeros((12, CH), BF16)], axis=0)


def gated(pos, *parts):
    outs = (shape((HALF, CH), BF16), shape((HALF + 16, CH), BF16), shape((8, N)))
    return kernel(gated_body, outs, 10, 1)(pos, *parts)


TALL = 2 * HALF + 16


def energy_rows(energy):
    return jnp.concatenate([*split(energy), jnp.zeros((8, N), BF16)], axis=0)


def stack_body(own, got, out):
    out[:CH] = own[...]
    out[CH:] = got[...]


def pair_energy(got, energy):
    tail = got[HALF:].astype(F32)
    return energy[:4] + (tail[:4, :N] + tail[:4, N:])


def product(pos, own, got, weights, s, t):
    first = pos[2] == 0
    dy = jnp.where(first, t, s)
    dx = jnp.where(first, s, t)
    chip = ((pos[0] + dy) & 3) * 4 + ((pos[1] + dx) & 3)
    cols = pl.ds(pl.multiple_of(chip * 2 * N, 2 * N), 2 * N)
    return dot(jnp.concatenate([own[...], got[:HALF]], axis=1), weights[:, cols])


def spread_body(specs, adds):
    def body(pos, own, got, energy, weights, *refs):
        extra, outs = refs[:adds], refs[adds:]
        for n, (s, pair) in enumerate(specs):
            tail = pair_energy(got, energy)
            if adds:
                rows = extra[n][0, 2 * HALF :].astype(F32)
                tail = tail + (rows[:4] + rows[4:8])
            tail = energy_rows(tail)
            for k, t in enumerate(pair):
                part = product(pos, own, got, weights, s, t)
                for side in range(2):
                    rows = slice(side * HALF, (side + 1) * HALF)
                    value = part[:, side * N : (side + 1) * N]
                    if adds:
                        value = value + extra[n][k, rows].astype(F32)
                    outs[n][k, rows] = value.astype(BF16)
                outs[n][k, 2 * HALF :] = tail

    return body


def spread(pos, specs, parts, extra=()):
    outs = tuple(shape((2, TALL, N), BF16) for _ in specs)
    count = len(extra)
    flops = 2 * HALF * 512 * 512 * len(specs)
    return kernel(spread_body(specs, count), outs, 5 + count, 1, (), flops)(pos, *parts, *extra)


def keep_body(pos, own, got, energy, weights, out, tail):
    for t in range(4):
        part = product(pos, own, got, weights, 0, t)
        out[t, :HALF] = part[:, :N]
        out[t, HALF:] = part[:, N:]
    tail[...] = jnp.concatenate([pair_energy(got, energy), jnp.zeros((4, N), F32)], axis=0)


def half_sum_body(own, tail, u_plus, d_minus, d_plus, u_minus, q0, q1, q2, q3):
    for t, q in enumerate((q0, q1, q2, q3)):
        x, y = ((u_plus, d_minus), (d_plus, u_minus))[t // 2]
        k = t % 2
        value = own[t] + x[k, : 2 * HALF].astype(F32) + y[k, : 2 * HALF].astype(F32)
        q[: 2 * HALF] = value.astype(q.dtype)
        e = x[k, 2 * HALF :].astype(F32) + y[k, 2 * HALF :].astype(F32)
        e = tail[:4] + (e[:4] + e[4:8])
        if q.dtype == BF16:
            q[2 * HALF :] = energy_rows(e)
        else:
            q[2 * HALF :] = jnp.concatenate([e, jnp.zeros((12, N), F32)], axis=0)


def half_sum(*parts):
    outs = (shape((TALL, N)),) + (shape((TALL, N), BF16),) * 3
    return kernel(half_sum_body, outs, 6)(*parts)


def total_body(mine):
    def body(pos, v0, v1, v2, v3, out):
        parts = (v0, v1, v2, v3)
        e = sum(v[2 * HALF :].astype(F32) for v in parts)
        scale = lax.rsqrt(as_column(e[:4] + e[4:8]) / DI + EPS)
        rows = half(pos[2] if mine else 1 - pos[2])
        out[...] = sum(v[rows].astype(F32) for v in parts) * scale

    return body


def total(mine, pos, *parts):
    return kernel(total_body(mine), shape((HALF, N)), 5, 1)(pos, *parts)


def finish_body(pos, tokens, own, got, out):
    c = pos[2]
    for which, part in ((c, own), (1 - c, got)):
        rows = half(which)
        out[rows] = (tokens[rows].astype(F32) + part[...]).astype(BF16)


def finish(pos, *parts):
    return kernel(finish_body, shape((ROWS, N), BF16), 4, 1, place=False)(pos, *parts)


def local(
    tokens,
    norm_gain,
    gate_proj,
    inner_proj,
    state_proj,
    conv_inner,
    conv_state,
    log_rate,
    rate_bias,
    skip_gain,
    gate_gain,
    out_proj,
):
    ci = lax.axis_index("chan")
    core = ci & 1
    pos = jnp.stack([ci >> 3, (ci >> 1) & 3, core, ci]).astype(jnp.int32)
    gain = norm_gain.reshape(32, N)

    small = jnp.pad(jnp.stack([rate_bias, -jnp.exp(log_rate), skip_gain]), ((0, 5), (0, N - HEADS)))

    away_tokens = swap(tokens)
    sem = (pltpu.SemaphoreType.DMA,)
    own_block = kernel(
        own_body, shape((HALF + 3 * N, N), BF16), 4, 1, sem, inputs=(pltpu.HBM,) * 3, last=pl.ANY
    )(pos, state_proj, gain, tokens)
    block = kernel(block_body, shape((BLOCK, N), BF16), 3, 1)(pos, own_block, away_tokens)

    n1, n3 = plane_move(block, 1, 0), plane_move(block, -1, 0)
    p0, m0 = plane_move(block, 1, 1), plane_move(block, -1, 1)
    p1, m3 = plane_move(n1, 1, 1), plane_move(n3, -1, 1)
    low = plane_move(n1[: BLOCK // 2], 1, 0)
    high = plane_move(n3[BLOCK // 2 :], -1, 0)
    m1 = plane_move(n1, -1, 1)
    n2 = jnp.concatenate([low, high], axis=0)
    a23 = jnp.stack([n2, n3])
    p23, m2 = plane_move(a23, 1, 1), plane_move(n2, -1, 1)
    c0 = plane_move(jnp.stack([p0, p1]), 1, 1)
    c1 = plane_move(jnp.stack([m2, m3]), -1, 1)
    mark1 = mark(p1)
    mark2 = mark(m2)
    early = (block, n1, a23, p0, p1, p23, m0, m1, m2, m3)

    raw_g, raw_i = swap(gate_proj), swap(inner_proj)
    scale_weights = kernel(scale_body, shape((D, 2 * CH), BF16), 3)
    keep = scale_weights(gate_proj, inner_proj, gain)
    got = scale_weights(raw_g, raw_i, gain)
    got_w = swap(out_proj)

    most_own = pick(*early, marks=(mark1, mark2))
    most_got = swap(most_own)
    acc, squares = most(pos, *early, keep, got)
    acc_st = state_most(pos, *early, most_own, most_got)
    w_all = kernel(stack_body, shape((2 * CH, D), BF16), 2)(out_proj, got_w)
    acc, squares = more(pos, c0, keep, got, acc, squares)
    last_own = pick(c0, c1)
    last_got = swap(last_own)
    own_gi, send_gi, scale = rest(pos, c1, keep, got, acc, squares)
    got_gi = swap(send_gi)
    own_st, send_st = state_rest(pos, a23, p23, m2, c0, c1, most_own, most_got, last_own, last_got, acc_st, scale)
    got_st = swap(send_st)

    edge = kernel(edge_body, shape((8, 2 * CH)), 5, 1)(pos, own_gi, got_gi, own_st, got_st)
    rim = later(edge, 1)

    values, head = values_of(pos, own_gi, got_gi, conv_inner)
    in_map, out_map, within, until, step, *fresh = rows_of_all(pos, own_st, got_st, values, conv_state, small)
    *new, entering, packet = scan(
        rim, within, until, step, *fresh, head, conv_inner, conv_state
    )
    p2, p1 = later(packet, 2), later(packet, 1)
    window = three(packet, p1, p2)
    e6, e3 = later(window, 6), later(window, 3)
    result, opened, out_all = inside(
        pos, own_gi, got_gi, values, in_map, out_map, within, step, *new, entering, small
    )
    own_g, send_g, energy = gated(pos, p1, p2, e3, e6, result, opened, out_all, until, gate_gain[None])

    got_g = swap(send_g)
    parts = (own_g, got_g, energy, w_all)
    far_low, far_high = spread(pos, ((2, (0, 1)), (2, (2, 3))), parts)
    t_plus, t_minus = plane_move(far_low, 1, 0), plane_move(far_high, -1, 0)
    near_plus, near_minus = spread(pos, ((1, (2, 3)), (3, (0, 1))), parts)
    d_plus, d_minus = plane_move(near_plus, 1, 0), plane_move(near_minus, -1, 0)
    keep_outs = (shape((4, 2 * HALF, N)), shape((8, N)))
    kept, tail = kernel(keep_body, keep_outs, 5, 1, (), 2 * HALF * 512 * 1024)(pos, *parts)
    (on_plus,) = spread(pos, ((1, (0, 1)),), parts, (t_plus,))
    u_plus = plane_move(on_plus, 1, 0)
    (on_minus,) = spread(pos, ((3, (2, 3)),), parts, (t_minus,))
    u_minus = plane_move(on_minus, -1, 0)
    q = half_sum(kept, tail, u_plus, d_minus, d_plus, u_minus)
    last = [q[0]] + [plane_move(q[t], t, 1) for t in (1, 2, 3)]
    got = swap(total(False, pos, *last))
    own = total(True, pos, *last)
    return finish(pos, tokens, own, got)


def solution(mesh):
    return jax.shard_map(
        local,
        mesh=mesh,
        in_specs=(
            P("seq", "chan"),
            P(),
            P(None, "chan"),
            P(None, "chan"),
            P("chan", None),
            P(None, "chan"),
            P(),
            P("chan"),
            P("chan"),
            P("chan"),
            P("chan"),
            P("chan", None),
        ),
        out_specs=P("seq", "chan"),
        check_vma=False,
    )
```
